8 devices in a mesh: data: 1 (over z), dap: 8 (over y, x, core).
Axes of the slice: x: 2, y: 2, z: 1, core: 2. Of those that a mesh axis runs over, the one named last changes fastest.
Arguments:
- extra_msa: bfloat16 [3072, 256, 64], P('data', 'dap')
- extra_mask: int32 [3072, 256], P('data')
- main_msa: bfloat16 [256, 256, 256], P('data', 'dap')
- main_mask: int32 [256, 256], P('data')
- pair_act: float32 [256, 256, 128], P(('data', 'dap'))
- extra_ln_gamma: bfloat16 [64], replicated
- extra_ln_beta: bfloat16 [64], replicated
- extra_w_left: bfloat16 [64, 32], replicated
- extra_b_left: bfloat16 [32], replicated
- extra_w_right: bfloat16 [64, 32], replicated
- extra_b_right: bfloat16 [32], replicated
- extra_w_out: bfloat16 [1024, 128], replicated
- extra_b_out: bfloat16 [128], replicated
- main_ln_gamma: bfloat16 [256], replicated
- main_ln_beta: bfloat16 [256], replicated
- main_w_left: bfloat16 [256, 32], replicated
- main_b_left: bfloat16 [32], replicated
- main_w_right: bfloat16 [256, 32], replicated
- main_b_right: bfloat16 [32], replicated
- main_w_out: bfloat16 [1024, 128], replicated
- main_b_out: bfloat16 [128], replicated
Outputs:
- output 1: float32 [256, 256, 128], P(('data', 'dap'))
- output 2: bfloat16 [3072, 256, 64], P(('data', 'dap'))
- output 3: bfloat16 [256, 256, 256], P(('data', 'dap'))
All inputs are finite; a program needn't handle non-finite values.
Results may differ from the reference program's by a relative error of at most 0.00470469.
Values are sent between devices in bfloat16 or wider.
A program may use at most 1 GiB of HBM per device.

```python
import jax
import jax.numpy as jnp
from jax import lax

NUM_RES = 256
NUM_SEQ = 256
NUM_EXTRA = 3072
MSA_DIM = 256
EXTRA_DIM = 64
OPM_HIDDEN = 32
PAIR_DIM = 128

LN_EPS = 1e-5
NORM_EPS = 1e-3
ROW_BLOCK = min(NUM_RES, 16)


def draw_msa(rng_key, seq_count, msa_width):
    key_profile, key_noise = jax.random.split(rng_key)
    profile = jax.random.normal(key_profile, (1, NUM_RES, msa_width), jnp.float32)
    seq_noise = jax.random.normal(key_noise, (seq_count, NUM_RES, msa_width), jnp.float32)
    return (profile + 0.7 * seq_noise).astype(jnp.bfloat16)


def draw_mask(rng_key, seq_count):
    key_level, key_draw = jax.random.split(rng_key)
    col_level = jax.random.randint(key_level, (1, NUM_RES), 4, 17)
    raw_draws = jax.random.randint(key_draw, (seq_count, NUM_RES), 0, 16)
    kept_mask = (raw_draws < col_level).astype(jnp.int32)
    first_row = jnp.arange(seq_count)[:, None] == 0
    return jnp.where(first_row, 1, kept_mask).astype(jnp.int32)


def draw_weights(rng_key, prefix, msa_width, seq_count):
    weight_keys = jax.random.split(rng_key, 8)
    hidden_sq = OPM_HIDDEN * OPM_HIDDEN
    return {
        prefix + '_ln_gamma': (1.0 + 0.3 * jax.random.normal(weight_keys[0], (msa_width,), jnp.float32)).astype(jnp.bfloat16),
        prefix + '_ln_beta': (0.5 * jax.random.normal(weight_keys[1], (msa_width,), jnp.float32)).astype(jnp.bfloat16),
        prefix + '_w_left': (jax.random.normal(weight_keys[2], (msa_width, OPM_HIDDEN), jnp.float32) * msa_width ** -0.5).astype(jnp.bfloat16),
        prefix + '_b_left': (0.5 * jax.random.normal(weight_keys[3], (OPM_HIDDEN,), jnp.float32)).astype(jnp.bfloat16),
        prefix + '_w_right': (jax.random.normal(weight_keys[4], (msa_width, OPM_HIDDEN), jnp.float32) * msa_width ** -0.5).astype(jnp.bfloat16),
        prefix + '_b_right': (0.5 * jax.random.normal(weight_keys[5], (OPM_HIDDEN,), jnp.float32)).astype(jnp.bfloat16),
        prefix + '_w_out': (jax.random.normal(weight_keys[6], (hidden_sq, PAIR_DIM), jnp.float32) * hidden_sq ** -0.5).astype(jnp.bfloat16),
        prefix + '_b_out': (0.2 * seq_count * jax.random.normal(weight_keys[7], (PAIR_DIM,), jnp.float32)).astype(jnp.bfloat16),
    }


def setup_inputs(seed: int = 0, part: int = 0) -> dict:
    part_keys = jax.random.split(jax.random.fold_in(jax.random.key(seed), part), 5)
    shared_keys = jax.random.split(jax.random.key(seed + 1), 2)
    inputs = {
        'extra_msa': draw_msa(part_keys[0], NUM_EXTRA, EXTRA_DIM),
        'extra_mask': draw_mask(part_keys[1], NUM_EXTRA),
        'main_msa': draw_msa(part_keys[2], NUM_SEQ, MSA_DIM),
        'main_mask': draw_mask(part_keys[3], NUM_SEQ),
        'pair_act': jax.random.normal(part_keys[4], (NUM_RES, NUM_RES, PAIR_DIM), jnp.float32),
    }
    inputs.update(draw_weights(shared_keys[0], 'extra', EXTRA_DIM, NUM_EXTRA))
    inputs.update(draw_weights(shared_keys[1], 'main', MSA_DIM, NUM_SEQ))
    return inputs


def layer_norm(msa_values, ln_gamma, ln_beta):
    as_float = msa_values.astype(jnp.float32)
    row_mean = jnp.mean(as_float, axis=-1, keepdims=True)
    centered = as_float - row_mean
    row_var = jnp.mean(centered * centered, axis=-1, keepdims=True)
    scaled = centered * lax.rsqrt(row_var + LN_EPS)
    return (scaled * ln_gamma.astype(jnp.float32) + ln_beta.astype(jnp.float32)).astype(jnp.bfloat16)


def outer_product_mean(msa_values, mask_int, ln_gamma, ln_beta, w_left, b_left, w_right, b_right, w_out, b_out):
    seq_count, res_count, msa_width = msa_values.shape
    hidden = w_left.shape[1]
    mask_float = mask_int.astype(jnp.float32)
    normed = layer_norm(msa_values, ln_gamma, ln_beta).reshape(seq_count * res_count, msa_width)
    left_acc = jnp.dot(normed, w_left, preferred_element_type=jnp.float32) + b_left.astype(jnp.float32)
    right_acc = jnp.dot(normed, w_right, preferred_element_type=jnp.float32) + b_right.astype(jnp.float32)
    left_proj = (left_acc.reshape(seq_count, res_count, hidden) * mask_float[:, :, None]).astype(jnp.bfloat16)
    right_proj = (right_acc.reshape(seq_count, res_count, hidden) * mask_float[:, :, None]).astype(jnp.bfloat16)
    left_float = left_proj.astype(jnp.float32)
    right_float = right_proj.astype(jnp.float32)
    w_grid = w_out.astype(jnp.float32).reshape(hidden, hidden, -1)
    left_blocks = left_float.reshape(seq_count, res_count // ROW_BLOCK, ROW_BLOCK, hidden).transpose(1, 0, 2, 3)

    def block_term(left_block):
        outer_prod = jnp.einsum('sic,sjd->ijcd', left_block, right_float).astype(jnp.bfloat16).astype(jnp.float32)
        return jnp.einsum('ijcd,cdk->ijk', outer_prod, w_grid)

    pair_sum = lax.map(block_term, left_blocks).reshape(res_count, res_count, -1)
    counts = jnp.dot(mask_float.T, mask_float)
    return (pair_sum + b_out.astype(jnp.float32)) / (NORM_EPS + counts)[:, :, None]


def reference(extra_msa, extra_mask, main_msa, main_mask, pair_act, extra_ln_gamma, extra_ln_beta, extra_w_left, extra_b_left, extra_w_right, extra_b_right, extra_w_out, extra_b_out, main_ln_gamma, main_ln_beta, main_w_left, main_b_left, main_w_right, main_b_right, main_w_out, main_b_out):
    extra_term = outer_product_mean(extra_msa, extra_mask, extra_ln_gamma, extra_ln_beta, extra_w_left, extra_b_left, extra_w_right, extra_b_right, extra_w_out, extra_b_out)
    main_term = outer_product_mean(main_msa, main_mask, main_ln_gamma, main_ln_beta, main_w_left, main_b_left, main_w_right, main_b_right, main_w_out, main_b_out)
    pair_out = pair_act + extra_term + main_term
    return (pair_out, extra_msa, main_msa)
```

```python
import functools

import jax
import jax.numpy as jnp
from jax import lax
from jax.experimental import pallas as pl
from jax.experimental.pallas import tpu as pltpu
from jax.sharding import PartitionSpec as P

LN_EPS = 1e-5
NORM_EPS = 1e-3
BF = jnp.bfloat16
F32 = jnp.float32
GROUP = 16
QSTEP = 4
RSTEP = 8


def partner(me, k):
    core, cx, cy = me % 2, (me // 2) % 2, me // 4
    k0, k1, k2 = k % 2, (k // 2) % 2, k // 4
    return (core + k0) % 2 + 2 * ((cx + k1) % 2) + 4 * ((cy + k2) % 2)


def nt_dot(lhs, rhs):
    return lax.dot_general(lhs, rhs, (((1,), (1,)), ((), ())), preferred_element_type=F32)


def opm_kernel(
    xe, xm, mask_e, mask_m, pair,
    gam_e, bet_e, w_blk, bias_b, bias_a, wo_e, bo_e, cnt_e,
    gam_m, bet_m, w_m, bias_m, wo_m, bo_m, cnt_m,
    pair_out, e_out, m_out, rs_recv,
    a_all, b_all, a_send, xb, y_s, mask_i, mask_et, mask_mt, mask_mo, am, bm, rt,
    e_ssem, e_rsem, m_ssem, m_rsem, xa_ssem, xa_rsem, xb_ssem, xb_rsem,
    g_ssem, g_rsem, f_ssem, f_rsem, rs_ssem, rs_rsem, lsem,
):
    me = lax.axis_index('dap')
    core = me % 2
    chip = me // 2
    sib = partner(me, 1)
    seq = e_out.shape[2]
    mseq = m_out.shape[0]
    rows = xe.shape[0]
    res = e_out.shape[0]

    def dev(d):
        return {'dap': d}

    def lane(h):
        return pl.ds(pl.multiple_of(h * seq, 128), seq)

    def rblk(d, n=rows):
        return pl.ds(pl.multiple_of(d * n, n), n)

    barrier = pltpu.get_barrier_semaphore()
    for k in range(1, 8):
        pl.semaphore_signal(barrier, inc=1, device_id=dev(partner(me, k)), device_id_type=pl.DeviceIdType.MESH)
    pl.semaphore_wait(barrier, 7)

    def remote(src, dst, ssem, rsem, target):
        return pltpu.make_async_remote_copy(
            src_ref=src, dst_ref=dst, send_sem=ssem, recv_sem=rsem,
            device_id=dev(target), device_id_type=pl.DeviceIdType.MESH)

    def e_copy(k):
        to = partner(me, k)
        return remote(xe.at[:, :, lane(to)], e_out.at[rblk(me)], e_ssem.at[k], e_rsem.at[k], to)

    for k in (1, 2, 4, 3, 5, 6, 7):
        e_copy(k).start()

    def m_copy(k):
        to = partner(me, k)
        return remote(xm.at[rblk(to, mseq)], m_out.at[:, rblk(me), :], m_ssem.at[k], m_rsem.at[k], to)

    cp = pltpu.make_async_copy(mask_e.at[rblk(me, seq)], mask_i, lsem.at[0])
    cp.start()
    mask_mt[...] = mask_m[...].astype(F32).T
    mask_mo[...] = mask_mt[rblk(me), :].reshape(rows, 1, mask_m.shape[0])
    cp.wait()
    mask_et[...] = mask_i[...].astype(F32).T

    def main_proj(xc, xf, bf):
        cp = pltpu.make_async_copy(xm.at[rblk(me, mseq)], xc.at[pl.ds(0, mseq)], lsem.at[1])
        cp.start()
        cp.wait()
        cp = pltpu.make_async_copy(xc.at[pl.ds(0, mseq)], m_out.at[:, rblk(me), :], lsem.at[1])
        cp.start()
        cp.wait()
        step = xc.shape[0]
        for part in range(xm.shape[0] // step):
            cp = pltpu.make_async_copy(xm.at[pl.ds(part * step, step)], xc, lsem.at[2])
            cp.start()
            cp.wait()

            def widen(i, _):
                s = pl.ds(pl.multiple_of(i * 8, 8), 8)
                xf[s] = xc[s].astype(F32)
                return 0
            lax.fori_loop(0, step // 8, widen, 0)

            def one(r, _):
                x = xf[:, r, :]
                mean = jnp.mean(x, axis=1, keepdims=True)
                cen = x - mean
                var = jnp.mean(cen * cen, axis=1, keepdims=True)
                y = (cen * lax.rsqrt(var + LN_EPS) * gam_m[...] + bet_m[...]).astype(BF)
                proj = nt_dot(w_m[...], y) + bias_m[...]
                proj = proj * mask_mo[r, :, pl.ds(part * step, step)]
                am[pl.ds(pl.multiple_of(r * 32, 32), 32), pl.ds(part * step, step)] = proj[:32].astype(BF)
                bf[:, r, :] = proj[32:]
                return 0
            lax.fori_loop(0, rows, one, 0)
            bm[:, rblk(me), pl.ds(part * step, step)] = bf[...].astype(BF)

    pl.run_scoped(
        main_proj, pltpu.VMEM((128, rows, xm.shape[2]), BF), pltpu.VMEM((128, rows, xm.shape[2]), F32),
        pltpu.VMEM((32, rows, 128), F32))

    def xb_copy(src):
        ref = b_all.at[:, rblk(src), lane(core)]
        return remote(ref, ref, xb_ssem.at[src], xb_rsem.at[src], sib)

    def xb_wait(src):
        ref = b_all.at[:, rblk(src), lane(1 - core)]
        return remote(ref, ref, xb_ssem.at[src], xb_rsem.at[src], sib)

    def xa_copy(c):
        return remote(a_send.at[rblk(c, rows * 32)], a_all.at[rblk(c, rows * 32), lane(core)],
                      xa_ssem.at[c], xa_rsem.at[c], sib)

    def xa_wait(c):
        return remote(a_send.at[rblk(c, rows * 32)], a_all.at[rblk(c, rows * 32), lane(1 - core)],
                      xa_ssem.at[c], xa_rsem.at[c], sib)

    def block(k, _):
        src = partner(me, k)
        own_half = (src % 2 + core) % 2

        @pl.when(k == 0)
        def _():
            cp = pltpu.make_async_copy(xe.at[:, :, lane(me)], xb, lsem.at[0])
            cp.start()
            cp.wait()
            cp = pltpu.make_async_copy(xb, e_out.at[rblk(me)], lsem.at[0])
            cp.start()
            cp.wait()

        @pl.when(k > 0)
        def _():
            remote(xe.at[:, :, lane(src)], e_out.at[rblk(src)], e_ssem.at[k], e_rsem.at[k], src).wait_recv()
            cp = pltpu.make_async_copy(e_out.at[rblk(src)], xb, lsem.at[0])
            cp.start()
            cp.wait()

        def half(hh, _):
            def norm(i, _):
                for u in range(2):
                    r = i * 2 + u
                    x = xb[hh * GROUP + r].astype(F32)
                    mean = jnp.mean(x, axis=0, keepdims=True)
                    cen = x - mean
                    var = jnp.mean(cen * cen, axis=0, keepdims=True)
                    y = cen * lax.rsqrt(var + LN_EPS) * gam_e[...] + bet_e[...]
                    y_s[pl.ds(pl.multiple_of(r * 64, 64), 64), :] = y.astype(BF)
                return 0
            lax.fori_loop(0, GROUP // 2, norm, 0)
            r0 = pl.multiple_of(src * rows + hh * GROUP, GROUP)
            m16 = mask_et[pl.ds(r0, GROUP), :]
            right = jnp.dot(w_blk[:512], y_s[...], preferred_element_type=F32) + bias_b[...]
            right = right.reshape(32, GROUP, seq) * m16[None]
            b_all[:, pl.ds(r0, GROUP), lane(core)] = right.astype(BF)
            left = jnp.dot(w_blk[512:], y_s[...], preferred_element_type=F32)
            left = jnp.concatenate(
                [(left[r * 32:r * 32 + 32] + bias_a[...]) * m16[r:r + 1] for r in range(GROUP)], axis=0).astype(BF)
            at = pl.ds(pl.multiple_of(((src // 2) * rows + hh * GROUP) * 32, GROUP * 32), GROUP * 32)

            @pl.when(own_half == 0)
            def _():
                a_all[at, lane(core)] = left

            @pl.when(own_half == 1)
            def _():
                a_send[at, :] = left
            return 0
        lax.fori_loop(0, rows // GROUP, half, 0)
        xb_copy(src).start()

        @pl.when(own_half == 1)
        def _():
            xa_copy(src // 2).start()
        return 0
    lax.fori_loop(0, 8, block, 0)

    for k in range(1, 8):
        e_copy(k).wait_send()

    def g_copy(i):
        ref = bm.at[:, rblk(me), :]
        return remote(ref, ref, g_ssem.at[i], g_rsem.at[i], partner(me, (1, 2, 4, 6)[i]))

    def g_wait(i):
        to = partner(me, (1, 2, 4, 6)[i])
        ref = bm.at[:, rblk(to), :]
        return remote(ref, ref, g_ssem.at[i], g_rsem.at[i], to)

    def f_copy(i):
        ref = bm.at[:, rblk(partner(me, (2, 4, 6)[i])), :]
        return remote(ref, ref, f_ssem.at[i], f_rsem.at[i], sib)

    def f_wait(i):
        ref = bm.at[:, rblk(partner(me, (3, 5, 7)[i])), :]
        return remote(ref, ref, f_ssem.at[i], f_rsem.at[i], sib)

    for i in range(4):
        g_copy(i).start()
    for k in (1, 2, 4, 3, 5, 6, 7):
        m_copy(k).start()

    def xwait(s, _):
        xb_wait(s).wait_recv()
        return 0
    lax.fori_loop(0, 8, xwait, 0)

    def xwait_a(c, _):
        xa_wait(c).wait_recv()
        return 0
    lax.fori_loop(0, 4, xwait_a, 0)

    def rs_copy(t, ib):
        to = partner(me, 6 - 2 * t)
        at = pl.ds(pl.multiple_of(ib * GROUP, GROUP), GROUP)
        return remote(rt.at[t, at], rs_recv.at[t, at], rs_ssem.at[t * 2 + ib], rs_rsem.at[t * 2 + ib], to)

    def contract(o_s, tm):
        def outer(left, right_of):
            def qstep(qq, _):
                for u in range(QSTEP):
                    q = qq * QSTEP + u
                    o = nt_dot(left(), right_of(q))
                    o_s[:, pl.ds(pl.multiple_of(q * 32, 32), 32), :] = o.astype(BF).reshape(GROUP, 32, res)
                return 0
            lax.fori_loop(0, 32 // QSTEP, qstep, 0)

        def eblk(n, _):
            t, ib = n // 2, n % 2
            c = partner(me, 6 - 2 * t) // 2
            at = pl.ds(pl.multiple_of((c * rows + ib * GROUP) * 32, GROUP * 32), GROUP * 32)
            outer(lambda: a_all[at, :], lambda q: b_all[q])

            def rstep(ii, _):
                for u in range(RSTEP):
                    i = ii * RSTEP + u
                    rt[t, ib * GROUP + i] = jnp.dot(wo_e[...], o_s[i], preferred_element_type=F32).astype(BF)
                return 0
            lax.fori_loop(0, GROUP // RSTEP, rstep, 0)

            @pl.when(t < 3)
            def _():
                rs_copy(t, ib).start()
            return 0
        lax.fori_loop(0, 8, eblk, 0)

        for i in range(1, 4):
            g_wait(i).wait_recv()
            f_copy(i - 1).start()
        g_wait(0).wait_recv()
        for i in range(3):
            f_wait(i).wait_recv()

        def mblk(ib, _):
            at = pl.ds(pl.multiple_of(ib * GROUP * 32, GROUP * 32), GROUP * 32)
            outer(lambda: am[at, :], lambda q: bm[q])

            def rstep(ii, _):
                for u in range(RSTEP):
                    i = ii * RSTEP + u
                    row = ib * GROUP + i
                    r = jnp.dot(wo_m[...], o_s[i], preferred_element_type=F32)
                    tm[row] = (r + bo_m[...]) / (NORM_EPS + cnt_m[row])
                return 0
            lax.fori_loop(0, GROUP // RSTEP, rstep, 0)
            return 0
        lax.fori_loop(0, rows // GROUP, mblk, 0)

        def final(zb, rb):
            def z_copy(j):
                return pltpu.make_async_copy(pair.at[pl.ds(j * 8, 8)], zb.at[j % 2], lsem.at[3 + j % 2])

            def o_copy(j):
                return pltpu.make_async_copy(zb.at[j % 2], pair_out.at[pl.ds(j * 8, 8)], lsem.at[5 + j % 2])

            def r_copy(j):
                return pltpu.make_async_copy(rs_recv.at[:, pl.ds(j * 8, 8)], rb, lsem.at[7])

            z_copy(0).start()
            for j in range(rows // 8):
                if j % 2 == 0:
                    for t in range(3):
                        rs_copy(t, j // 2).wait_recv()
                r_copy(j).start()
                if j >= 1:
                    o_copy(j - 1).wait()
                if j + 1 < rows // 8:
                    z_copy(j + 1).start()
                z_copy(j).wait()
                r_copy(j).wait()

                def row(i, _):
                    n = j * 8 + i
                    tot = rt[3, n].astype(F32) + rb[0, i].astype(F32) + rb[1, i].astype(F32) + rb[2, i].astype(F32)
                    te = (tot + bo_e[...]) / (NORM_EPS + cnt_e[n])
                    zb[j % 2, i] = (zb[j % 2, i] + te.T) + tm[n].T
                    return 0
                lax.fori_loop(0, 8, row, 0)
                o_copy(j).start()
            o_copy(rows // 8 - 1).wait()

        pl.run_scoped(final, pltpu.VMEM((2, 8, res, 128), F32), pltpu.VMEM((3, 8, 128, res), BF))

    pl.run_scoped(contract, pltpu.VMEM((GROUP, 1024, res), BF), pltpu.VMEM((rows, 128, res), F32))

    for k in range(1, 8):
        m_copy(k).wait_send()
        to = partner(me, k)
        remote(xm.at[rblk(me, mseq)], m_out.at[:, rblk(to), :], m_ssem.at[k], m_rsem.at[k], to).wait_recv()

    def drain(s, _):
        xb_copy(s).wait_send()
        return 0
    lax.fori_loop(0, 8, drain, 0)

    def drain_a(c, _):
        xa_copy(c).wait_send()
        return 0
    lax.fori_loop(0, 4, drain_a, 0)
    for i in range(4):
        g_copy(i).wait_send()
    for i in range(3):
        f_copy(i).wait_send()
        for ib in range(2):
            rs_copy(i, ib).wait_send()


def pair_counts(mask_rows, mask_full):
    return jnp.einsum('si,sj->ij', mask_rows.astype(BF), mask_full.astype(BF), preferred_element_type=F32)


def column(v):
    return v.astype(F32)[:, None]


def solution(mesh):
    msa_spec = P('data', 'dap', None)
    mask_spec = P('data', None)
    row_spec = P(('data', 'dap'), None, None)

    def local_program(extra_block, extra_mask, main_block, main_mask, pair_rows,
                      e_gam, e_bet, e_wl, e_bl, e_wr, e_br, e_wo, e_bo,
                      m_gam, m_bet, m_wl, m_bl, m_wr, m_br, m_wo, m_bo):
        seqs, rows, ce = extra_block.shape
        mseqs, _, cm = main_block.shape
        res = extra_mask.shape[1]
        hid = e_wl.shape[1]
        nk = e_wo.shape[1]
        me = lax.axis_index('dap')
        seq = seqs // 8

        def counts(mask):
            return pair_counts(lax.dynamic_slice_in_dim(mask, me * rows, rows, axis=1), mask)[:, None, :]

        eye = jnp.eye(GROUP, dtype=BF)
        w_b = (e_wr.T[:, None, None, :] * eye[None, :, :, None]).reshape(hid * GROUP, GROUP * ce)
        w_a = (e_wl.T[None, :, None, :] * eye[:, None, :, None]).reshape(hid * GROUP, GROUP * ce)
        w_blk = jnp.concatenate([w_b, w_a], axis=0)
        bias_b = jnp.repeat(e_br.astype(F32), GROUP)[:, None]

        def w_out_t(w):
            return w.reshape(hid, hid, nk).transpose(2, 1, 0).reshape(nk, hid * hid)

        args = (
            jnp.transpose(extra_block, (1, 2, 0)), main_block, extra_mask, main_mask, pair_rows,
            column(e_gam), column(e_bet), w_blk, bias_b, column(e_bl), w_out_t(e_wo), column(e_bo), counts(extra_mask),
            m_gam.astype(F32)[None], m_bet.astype(F32)[None], jnp.concatenate([m_wl.T, m_wr.T], axis=0),
            column(jnp.concatenate([m_bl, m_br])), w_out_t(m_wo), column(m_bo), counts(main_mask))
        any_spec = pl.BlockSpec(memory_space=pl.ANY)
        vmem = pl.BlockSpec(memory_space=pltpu.VMEM)
        dma = pltpu.SemaphoreType.DMA
        pair_out, e_recv, m_recv, _ = pl.pallas_call(
            opm_kernel,
            out_shape=(
                jax.ShapeDtypeStruct((rows, res, nk), F32),
                jax.ShapeDtypeStruct((res, ce, seq), BF),
                jax.ShapeDtypeStruct((mseqs // 8, res, cm), BF),
                jax.ShapeDtypeStruct((3, rows, nk, res), BF)),
            in_specs=[any_spec, any_spec, any_spec, vmem, any_spec] + [vmem] * 15,
            out_specs=(any_spec,) * 4,
            scratch_shapes=[
                pltpu.VMEM((4 * rows * hid, 2 * seq), BF),
                pltpu.VMEM((hid, res, 2 * seq), BF),
                pltpu.VMEM((4 * rows * hid, seq), BF),
                pltpu.VMEM((rows, ce, seq), BF),
                pltpu.VMEM((GROUP * ce, seq), BF),
                pltpu.VMEM((seq, res), jnp.int32),
                pltpu.VMEM((res, seq), F32),
                pltpu.VMEM((res, mseqs), F32),
                pltpu.VMEM((rows, 1, mseqs), F32),
                pltpu.VMEM((rows * hid, mseqs), BF),
                pltpu.VMEM((hid, res, mseqs), BF),
                pltpu.VMEM((4, rows, nk, res), BF),
                dma((8,)), dma((8,)), dma((8,)), dma((8,)), dma((4,)), dma((4,)), dma((8,)), dma((8,)),
                dma((4,)), dma((4,)), dma((3,)), dma((3,)), dma((6,)), dma((6,)), dma((8,))],
            compiler_params=pltpu.CompilerParams(
                collective_id=0, has_side_effects=True, vmem_limit_bytes=67043328),
            name='opm',
        )(*args)
        return pair_out, jnp.transpose(e_recv, (2, 0, 1)), m_recv

    in_specs = (msa_spec, mask_spec, msa_spec, mask_spec, row_spec) + (P(),) * 16
    return jax.shard_map(local_program, mesh=mesh, in_specs=in_specs, out_specs=(row_spec,) * 3, check_vma=False)
```

```python
import functools

import jax
import jax.numpy as jnp
from jax import lax
from jax.experimental import pallas as pl
from jax.experimental.pallas import tpu as pltpu
from jax.sharding import PartitionSpec as P

LN_EPS = 1e-5
NORM_EPS = 1e-3
BF = jnp.bfloat16
F32 = jnp.float32
GROUP = 16
QSTEP = 4
RSTEP = 8


def partner(me, k):
    core, cx, cy = me % 2, (me // 2) % 2, me // 4
    k0, k1, k2 = k % 2, (k // 2) % 2, k // 4
    return (core + k0) % 2 + 2 * ((cx + k1) % 2) + 4 * ((cy + k2) % 2)


def nt_dot(lhs, rhs):
    return lax.dot_general(lhs, rhs, (((1,), (1,)), ((), ())), preferred_element_type=F32)


def column(row, n, repeat):
    m = row.shape[1]
    at = lax.broadcasted_iota(jnp.int32, (n, m), 0) // repeat
    return jnp.sum(jnp.where(at == lax.broadcasted_iota(jnp.int32, (n, m), 1), row, 0.0), axis=1, keepdims=True)


def opm_kernel(
    xe, xm, mask_e, mask_m, pair,
    e_gam, e_bet, e_wl, e_bl, e_wr, e_br, e_wo, e_bo,
    m_gam, m_bet, m_wl, m_bl, m_wr, m_br, m_wo, m_bo,
    pair_out, e_out, m_out, rs_recv,
    a_all, b_all, a_send, xb, y_s, mask_i, mask_et, mask_mo, am, bm, rt, rs_mid,
    w_blk, w_m, wo_e, wo_m, gam_e, bet_e, bias_b, bias_a, bo_e, bias_m, bo_m, cnt_e, cnt_m,
    e_ssem, e_rsem, m_ssem, m_rsem, xa_ssem, xa_rsem, xb_ssem, xb_rsem,
    g_ssem, g_rsem, f_ssem, f_rsem, rs_ssem, rs_rsem, lsem,
):
    me = lax.axis_index('dap')
    core = me % 2
    chip = me // 2
    sib = partner(me, 1)
    seq = e_out.shape[2]
    mseq = m_out.shape[0]
    rows = xe.shape[0]
    res = e_out.shape[0]

    def dev(d):
        return {'dap': d}

    def lane(h):
        return pl.ds(pl.multiple_of(h * seq, 128), seq)

    def rblk(d, n=rows):
        return pl.ds(pl.multiple_of(d * n, n), n)

    barrier = pltpu.get_barrier_semaphore()
    for k in range(1, 8):
        pl.semaphore_signal(barrier, inc=1, device_id=dev(partner(me, k)), device_id_type=pl.DeviceIdType.MESH)
    pl.semaphore_wait(barrier, 7)

    def remote(src, dst, ssem, rsem, target):
        return pltpu.make_async_remote_copy(
            src_ref=src, dst_ref=dst, send_sem=ssem, recv_sem=rsem,
            device_id=dev(target), device_id_type=pl.DeviceIdType.MESH)

    def e_copy(k):
        to = partner(me, k)
        return remote(xe.at[:, :, lane(to)], e_out.at[rblk(me)], e_ssem.at[k], e_rsem.at[k], to)

    for k in (1, 2, 4, 3, 5, 6, 7):
        e_copy(k).start()

    def m_copy(k):
        to = partner(me, k)
        return remote(xm.at[rblk(to, mseq)], m_out.at[:, rblk(me), :], m_ssem.at[k], m_rsem.at[k], to)

    def row_of(ref):
        v = ref[...].astype(F32)
        return v.reshape(1, v.shape[0])

    def weights(wf, wp):
        gam_e[...] = column(row_of(e_gam), 64, 1)
        bet_e[...] = column(row_of(e_bet), 64, 1)
        bias_b[...] = column(row_of(e_br), 32 * GROUP, GROUP)
        bias_a[...] = column(row_of(e_bl), 32, 1)
        bo_e[...] = column(row_of(e_bo), 128, 1)
        bo_m[...] = column(row_of(m_bo), 128, 1)
        bias_m[:32] = column(row_of(m_bl), 32, 1)
        bias_m[32:] = column(row_of(m_br), 32, 1)
        w_m[:32] = m_wl[...]
        w_m[32:] = m_wr[...]
        at_col = lax.broadcasted_iota(jnp.int32, (32 * GROUP, 64 * GROUP), 1) // 64
        at_row = lax.broadcasted_iota(jnp.int32, (32 * GROUP, 64 * GROUP), 0)

        def wide(ref):
            w = ref[...].astype(F32)
            return jnp.concatenate([jnp.concatenate([w, w], axis=1)] * (GROUP // 2), axis=1)

        rep = jnp.broadcast_to(wide(e_wr)[:, None, :], (32, GROUP, 64 * GROUP)).reshape(32 * GROUP, 64 * GROUP)
        w_blk[:32 * GROUP] = jnp.where(at_row % GROUP == at_col, rep, 0.0).astype(BF)
        rep = jnp.concatenate([wide(e_wl)] * GROUP, axis=0)
        w_blk[32 * GROUP:] = jnp.where(at_row // 32 == at_col, rep, 0.0).astype(BF)
        for src, dst in ((e_wo, wo_e), (m_wo, wo_m)):
            wf[...] = src[...].astype(F32)

            def pick(q, _):
                wp[pl.ds(pl.multiple_of(q * 32, 32), 32), :] = wf[pl.ds(q, 32, stride=32), :]
                return 0
            lax.fori_loop(0, 32, pick, 0)
            dst[...] = wp[...].T.astype(BF)

    pl.run_scoped(weights, pltpu.VMEM((1024, 128), F32), pltpu.VMEM((1024, 128), F32))

    def masks(mt, acc):
        mt[:, :mask_m.shape[0]] = mask_m[...].astype(F32).T
        own = mt[rblk(me), :mask_m.shape[0]]
        mask_mo[...] = own.reshape(rows, 1, mask_m.shape[0])
        cnt_m[...] = jnp.dot(own.astype(BF), mask_m[...].astype(F32).astype(BF),
                             preferred_element_type=F32).reshape(rows, 1, res)
        acc[...] = jnp.zeros_like(acc)

        def load(d):
            cp = pltpu.make_async_copy(mask_e.at[rblk(d, seq)], mask_i, lsem.at[0])
            cp.start()
            cp.wait()

        def count(d, _):
            load(d)
            m = mask_i[...].astype(F32)
            mt[...] = m.T
            acc[...] += jnp.dot(mt[rblk(me), :].astype(BF), m.astype(BF), preferred_element_type=F32)
            return 0
        lax.fori_loop(0, 8, count, 0)
        cnt_e[...] = acc[...].reshape(rows, 1, res)
        load(me)
        mask_et[...] = mask_i[...].astype(F32).T

    pl.run_scoped(masks, pltpu.VMEM((res, seq), F32), pltpu.VMEM((rows, res), F32))

    def main_proj(xc, xf, bf):
        cp = pltpu.make_async_copy(xm.at[rblk(me, mseq)], xc.at[pl.ds(0, mseq)], lsem.at[1])
        cp.start()
        cp.wait()
        cp = pltpu.make_async_copy(xc.at[pl.ds(0, mseq)], m_out.at[:, rblk(me), :], lsem.at[1])
        cp.start()
        cp.wait()
        step = xc.shape[0]
        gam_m, bet_m = row_of(m_gam), row_of(m_bet)
        for part in range(xm.shape[0] // step):
            cp = pltpu.make_async_copy(xm.at[pl.ds(part * step, step)], xc, lsem.at[2])
            cp.start()
            cp.wait()

            def widen(i, _):
                s = pl.ds(pl.multiple_of(i * 8, 8), 8)
                xf[s] = xc[s].astype(F32)
                return 0
            lax.fori_loop(0, step // 8, widen, 0)

            def one(r, _):
                x = xf[:, r, :]
                mean = jnp.mean(x, axis=1, keepdims=True)
                cen = x - mean
                var = jnp.mean(cen * cen, axis=1, keepdims=True)
                y = (cen * lax.rsqrt(var + LN_EPS) * gam_m + bet_m).astype(BF)
                proj = nt_dot(w_m[...], y) + bias_m[...]
                proj = proj * mask_mo[r, :, pl.ds(part * step, step)]
                am[pl.ds(pl.multiple_of(r * 32, 32), 32), pl.ds(part * step, step)] = proj[:32].astype(BF)
                bf[:, r, :] = proj[32:]
                return 0
            lax.fori_loop(0, rows, one, 0)
            bm[:, rblk(me), pl.ds(part * step, step)] = bf[...].astype(BF)

    pl.run_scoped(
        main_proj, pltpu.VMEM((128, rows, xm.shape[2]), BF), pltpu.VMEM((128, rows, xm.shape[2]), F32),
        pltpu.VMEM((32, rows, 128), F32))

    def xb_copy(src):
        ref = b_all.at[:, rblk(src), lane(core)]
        return remote(ref, ref, xb_ssem.at[src], xb_rsem.at[src], sib)

    def xb_wait(src):
        ref = b_all.at[:, rblk(src), lane(1 - core)]
        return remote(ref, ref, xb_ssem.at[src], xb_rsem.at[src], sib)

    def xa_copy(c):
        return remote(a_send.at[rblk(c, rows * 32)], a_all.at[rblk(c, rows * 32), lane(core)],
                      xa_ssem.at[c], xa_rsem.at[c], sib)

    def xa_wait(c):
        return remote(a_send.at[rblk(c, rows * 32)], a_all.at[rblk(c, rows * 32), lane(1 - core)],
                      xa_ssem.at[c], xa_rsem.at[c], sib)

    def block(k, _):
        src = partner(me, k)
        own_half = (src % 2 + core) % 2

        @pl.when(k == 0)
        def _():
            cp = pltpu.make_async_copy(xe.at[:, :, lane(me)], xb, lsem.at[0])
            cp.start()
            cp.wait()
            cp = pltpu.make_async_copy(xb, e_out.at[rblk(me)], lsem.at[0])
            cp.start()
            cp.wait()

        @pl.when(k > 0)
        def _():
            remote(xe.at[:, :, lane(src)], e_out.at[rblk(src)], e_ssem.at[k], e_rsem.at[k], src).wait_recv()
            cp = pltpu.make_async_copy(e_out.at[rblk(src)], xb, lsem.at[0])
            cp.start()
            cp.wait()

        def half(hh, _):
            def norm(i, _):
                for u in range(2):
                    r = i * 2 + u
                    x = xb[hh * GROUP + r].astype(F32)
                    mean = jnp.mean(x, axis=0, keepdims=True)
                    cen = x - mean
                    var = jnp.mean(cen * cen, axis=0, keepdims=True)
                    y = cen * lax.rsqrt(var + LN_EPS) * gam_e[...] + bet_e[...]
                    y_s[pl.ds(pl.multiple_of(r * 64, 64), 64), :] = y.astype(BF)
                return 0
            lax.fori_loop(0, GROUP // 2, norm, 0)
            r0 = pl.multiple_of(src * rows + hh * GROUP, GROUP)
            m16 = mask_et[pl.ds(r0, GROUP), :]
            right = jnp.dot(w_blk[:512], y_s[...], preferred_element_type=F32) + bias_b[...]
            right = right.reshape(32, GROUP, seq) * m16[None]
            b_all[:, pl.ds(r0, GROUP), lane(core)] = right.astype(BF)
            left = jnp.dot(w_blk[512:], y_s[...], preferred_element_type=F32)
            left = jnp.concatenate(
                [(left[r * 32:r * 32 + 32] + bias_a[...]) * m16[r:r + 1] for r in range(GROUP)], axis=0).astype(BF)
            at = pl.ds(pl.multiple_of(((src // 2) * rows + hh * GROUP) * 32, GROUP * 32), GROUP * 32)

            @pl.when(own_half == 0)
            def _():
                a_all[at, lane(core)] = left

            @pl.when(own_half == 1)
            def _():
                a_send[at, :] = left
            return 0
        lax.fori_loop(0, rows // GROUP, half, 0)
        xb_copy(src).start()

        @pl.when(own_half == 1)
        def _():
            xa_copy(src // 2).start()
        return 0
    lax.fori_loop(0, 8, block, 0)

    for k in range(1, 8):
        e_copy(k).wait_send()

    def g_copy(i):
        ref = bm.at[:, rblk(me), :]
        return remote(ref, ref, g_ssem.at[i], g_rsem.at[i], partner(me, (1, 2, 4, 6)[i]))

    def g_wait(i):
        to = partner(me, (1, 2, 4, 6)[i])
        ref = bm.at[:, rblk(to), :]
        return remote(ref, ref, g_ssem.at[i], g_rsem.at[i], to)

    def f_copy(i):
        ref = bm.at[:, rblk(partner(me, (2, 4, 6)[i])), :]
        return remote(ref, ref, f_ssem.at[i], f_rsem.at[i], sib)

    def f_wait(i):
        ref = bm.at[:, rblk(partner(me, (3, 5, 7)[i])), :]
        return remote(ref, ref, f_ssem.at[i], f_rsem.at[i], sib)

    for i in range(4):
        g_copy(i).start()
    m_copy(1).start()

    def xwait(s, _):
        xb_wait(s).wait_recv()
        return 0
    lax.fori_loop(0, 8, xwait, 0)

    def xwait_a(c, _):
        xa_wait(c).wait_recv()
        return 0
    lax.fori_loop(0, 4, xwait_a, 0)

    def rs_copy(n):
        t, ib, k = ((0, 0, 2), (0, 1, 4), (1, 0, 2), (2, 1, 4), (2, 0, 4), (1, 1, 2))[n]
        at = pl.ds(ib * GROUP, GROUP)
        dst = rs_mid.at[ib] if t == 0 else rs_recv.at[t - 1, at]
        return remote(rt.at[t, at], dst, rs_ssem.at[n], rs_rsem.at[n], partner(me, k))

    def contract(o_s, tm):
        def outer(left, right_of):
            def qstep(qq, _):
                for u in range(QSTEP):
                    q = qq * QSTEP + u
                    o = nt_dot(left(), right_of(q))
                    o_s[:, pl.ds(pl.multiple_of(q * 32, 32), 32), :] = o.astype(BF).reshape(GROUP, 32, res)
                return 0
            lax.fori_loop(0, 32 // QSTEP, qstep, 0)

        def eblk(n, _):
            t = ((n // 2 + 1) // 2) % 2 * (1 + (n // 2 + n + 1) % 2) + 3 * (n // 6)
            ib = n % 2
            c = partner(me, 2 * (1 - t // 2) + 4 * (1 - t % 2)) // 2
            at = pl.ds(pl.multiple_of((c * rows + ib * GROUP) * 32, GROUP * 32), GROUP * 32)
            outer(lambda: a_all[at, :], lambda q: b_all[q])

            def rstep(ii, _):
                for u in range(RSTEP):
                    i = ii * RSTEP + u
                    rt[t, ib * GROUP + i] = jnp.dot(wo_e[...], o_s[i], preferred_element_type=F32).astype(BF)
                return 0
            lax.fori_loop(0, GROUP // RSTEP, rstep, 0)

            for v in range(6):
                @pl.when(n == v)
                def _():
                    if v >= 4:
                        rs_copy(v - 4).wait_recv()

                        def add(i, _):
                            at = (t, ib * GROUP + i)
                            rt[at] = (rt[at].astype(F32) + rs_mid[v - 4, i].astype(F32)).astype(BF)
                            return 0
                        lax.fori_loop(0, GROUP, add, 0)
                    rs_copy(v).start()
                    if v == 1:
                        for k in (2, 4, 3, 5, 6, 7):
                            m_copy(k).start()
            return 0
        lax.fori_loop(0, 8, eblk, 0)

        for i in range(1, 4):
            g_wait(i).wait_recv()
            f_copy(i - 1).start()
        g_wait(0).wait_recv()
        for i in range(3):
            f_wait(i).wait_recv()

        def mblk(ib, _):
            at = pl.ds(pl.multiple_of(ib * GROUP * 32, GROUP * 32), GROUP * 32)
            outer(lambda: am[at, :], lambda q: bm[q])

            def rstep(ii, _):
                for u in range(RSTEP):
                    i = ii * RSTEP + u
                    row = ib * GROUP + i
                    r = jnp.dot(wo_m[...], o_s[i], preferred_element_type=F32)
                    tm[row] = (r + bo_m[...]) / (NORM_EPS + cnt_m[row])
                return 0
            lax.fori_loop(0, GROUP // RSTEP, rstep, 0)
            return 0
        lax.fori_loop(0, rows // GROUP, mblk, 0)

        def final(zb, rb):
            def z_copy(j):
                return pltpu.make_async_copy(pair.at[pl.ds(j * 8, 8)], zb.at[j % 2], lsem.at[3 + j % 2])

            def o_copy(j):
                return pltpu.make_async_copy(zb.at[j % 2], pair_out.at[pl.ds(j * 8, 8)], lsem.at[5 + j % 2])

            def r_copy(j):
                return pltpu.make_async_copy(rs_recv.at[:, pl.ds(j * 8, 8)], rb, lsem.at[7])

            z_copy(0).start()
            for j in range(rows // 8):
                if j % 2 == 0:
                    for n in ((2, 4), (3, 5))[j // 2]:
                        rs_copy(n).wait_recv()
                r_copy(j).start()
                if j >= 1:
                    o_copy(j - 1).wait()
                if j + 1 < rows // 8:
                    z_copy(j + 1).start()
                z_copy(j).wait()
                r_copy(j).wait()

                def row(i, _):
                    n = j * 8 + i
                    tot = rt[3, n].astype(F32) + rb[0, i].astype(F32) + rb[1, i].astype(F32)
                    te = (tot + bo_e[...]) / (NORM_EPS + cnt_e[n])
                    zb[j % 2, i] = (zb[j % 2, i] + te.T) + tm[n].T
                    return 0
                lax.fori_loop(0, 8, row, 0)
                o_copy(j).start()
            o_copy(rows // 8 - 1).wait()

        pl.run_scoped(final, pltpu.VMEM((2, 8, res, 128), F32), pltpu.VMEM((2, 8, 128, res), BF))

    pl.run_scoped(contract, pltpu.VMEM((GROUP, 1024, res), BF), pltpu.VMEM((rows, 128, res), F32))

    for k in range(1, 8):
        m_copy(k).wait_send()
        to = partner(me, k)
        remote(xm.at[rblk(me, mseq)], m_out.at[:, rblk(to), :], m_ssem.at[k], m_rsem.at[k], to).wait_recv()

    def drain(s, _):
        xb_copy(s).wait_send()
        return 0
    lax.fori_loop(0, 8, drain, 0)

    def drain_a(c, _):
        xa_copy(c).wait_send()
        return 0
    lax.fori_loop(0, 4, drain_a, 0)
    for i in range(4):
        g_copy(i).wait_send()
    for i in range(3):
        f_copy(i).wait_send()
    for n in range(6):
        rs_copy(n).wait_send()


def solution(mesh):
    msa_spec = P('data', 'dap', None)
    mask_spec = P('data', None)
    row_spec = P(('data', 'dap'), None, None)

    def local_program(extra_block, extra_mask, main_block, main_mask, pair_rows,
                      e_gam, e_bet, e_wl, e_bl, e_wr, e_br, e_wo, e_bo,
                      m_gam, m_bet, m_wl, m_bl, m_wr, m_br, m_wo, m_bo):
        seqs, rows, ce = extra_block.shape
        mseqs, _, cm = main_block.shape
        res = extra_mask.shape[1]
        hid = e_wl.shape[1]
        nk = e_wo.shape[1]
        seq = seqs // 8
        args = (
            jnp.transpose(extra_block, (1, 2, 0)), main_block, extra_mask, main_mask, pair_rows,
            e_gam, e_bet, e_wl.T, e_bl, e_wr.T, e_br, e_wo, e_bo, m_gam, m_bet, m_wl.T, m_bl, m_wr.T, m_br, m_wo, m_bo)
        any_spec = pl.BlockSpec(memory_space=pl.ANY)
        vmem = pl.BlockSpec(memory_space=pltpu.VMEM)
        dma = pltpu.SemaphoreType.DMA
        pair_out, e_recv, m_recv, _ = pl.pallas_call(
            opm_kernel,
            out_shape=(
                jax.ShapeDtypeStruct((rows, res, nk), F32),
                jax.ShapeDtypeStruct((res, ce, seq), BF),
                jax.ShapeDtypeStruct((mseqs // 8, res, cm), BF),
                jax.ShapeDtypeStruct((2, rows, nk, res), BF)),
            in_specs=[any_spec, any_spec, any_spec, vmem, any_spec] + [vmem] * 16,
            out_specs=(any_spec,) * 4,
            scratch_shapes=[
                pltpu.VMEM((4 * rows * hid, 2 * seq), BF),
                pltpu.VMEM((hid, res, 2 * seq), BF),
                pltpu.VMEM((4 * rows * hid, seq), BF),
                pltpu.VMEM((rows, ce, seq), BF),
                pltpu.VMEM((GROUP * ce, seq), BF),
                pltpu.VMEM((seq, res), jnp.int32),
                pltpu.VMEM((res, seq), F32),
                pltpu.VMEM((rows, 1, mseqs), F32),
                pltpu.VMEM((rows * hid, mseqs), BF),
                pltpu.VMEM((hid, res, mseqs), BF),
                pltpu.VMEM((4, rows, nk, res), BF),
                pltpu.VMEM((2, GROUP, nk, res), BF),
                pltpu.VMEM((2 * hid * GROUP, ce * GROUP), BF),
                pltpu.VMEM((2 * hid, cm), BF),
                pltpu.VMEM((nk, hid * hid), BF),
                pltpu.VMEM((nk, hid * hid), BF),
                pltpu.VMEM((ce, 1), F32),
                pltpu.VMEM((ce, 1), F32),
                pltpu.VMEM((hid * GROUP, 1), F32),
                pltpu.VMEM((hid, 1), F32),
                pltpu.VMEM((nk, 1), F32),
                pltpu.VMEM((2 * hid, 1), F32),
                pltpu.VMEM((nk, 1), F32),
                pltpu.VMEM((rows, 1, res), F32),
                pltpu.VMEM((rows, 1, res), F32),
                dma((8,)), dma((8,)), dma((8,)), dma((8,)), dma((4,)), dma((4,)), dma((8,)), dma((8,)),
                dma((4,)), dma((4,)), dma((3,)), dma((3,)), dma((6,)), dma((6,)), dma((8,))],
            compiler_params=pltpu.CompilerParams(
                collective_id=0, has_side_effects=True, vmem_limit_bytes=67043328),
            name='opm',
        )(*args)
        return pair_out, jnp.transpose(e_recv, (2, 0, 1)), m_recv

    in_specs = (msa_spec, mask_spec, msa_spec, mask_spec, row_spec) + (P(),) * 16
    return jax.shard_map(local_program, mesh=mesh, in_specs=in_specs, out_specs=(row_spec,) * 3, check_vma=False)
```

```python
import functools

import jax
import jax.numpy as jnp
from jax import lax
from jax.experimental import pallas as pl
from jax.experimental.pallas import tpu as pltpu
from jax.sharding import PartitionSpec as P

LN_EPS = 1e-5
NORM_EPS = 1e-3
BF = jnp.bfloat16
F32 = jnp.float32
GROUP = 16
QSTEP = 4
LSTEP = 4
MSTEP = 8
RG, LG = 8, 4
HID, CE, LANES, HALF = 32, 64, 128, 64
RSTEP = 8


def loop(n, body):
    def step(i, carry):
        body(i)
        return carry
    lax.fori_loop(0, n, step, 0)


def part(i, n):
    return pl.ds(pl.multiple_of(i * n, n), n)


def partner(me, k):
    core, cx, cy = me % 2, (me // 2) % 2, me // 4
    k0, k1, k2 = k % 2, (k // 2) % 2, k // 4
    return (core + k0) % 2 + 2 * ((cx + k1) % 2) + 4 * ((cy + k2) % 2)


def nt_dot(lhs, rhs):
    return lax.dot_general(lhs, rhs, (((1,), (1,)), ((), ())), preferred_element_type=F32)


def column(row, n, repeat):
    m = row.shape[1]
    at = lax.broadcasted_iota(jnp.int32, (n, m), 0) // repeat
    return jnp.sum(jnp.where(at == lax.broadcasted_iota(jnp.int32, (n, m), 1), row, 0.0), axis=1, keepdims=True)


def opm_kernel(
    xe, xm, mask_e, mask_m, pair,
    e_gam, e_bet, e_wl, e_bl, e_wr, e_br, e_wo, e_bo,
    m_gam, m_bet, m_wl, m_bl, m_wr, m_br, m_wo, m_bo,
    pair_out, e_out, m_out,
    a_all, b_all, a_send, xb, y_s, mask_i, mask_et, mask_mo, am, bm, rt, rs_mid, rs_recv, r_own,
    w_right, w_left, w_m, wo_e, wo_m, gam_e, bet_e, bias_b, bias_a, bo_e, bias_m, bo_m, cnt_e, cnt_m,
    e_ssem, e_rsem, m_ssem, m_rsem, xa_ssem, xa_rsem, xb_ssem, xb_rsem,
    g_ssem, g_rsem, f_ssem, f_rsem, rs_ssem, rs_rsem, ob_ssem, ob_rsem, ob_free, lsem,
):
    me = lax.axis_index('dap')
    core = me % 2
    chip = me // 2
    sib = partner(me, 1)
    seq = e_out.shape[2]
    mseq = m_out.shape[0]
    rows = xe.shape[0]
    res = e_out.shape[0]

    def dev(d):
        return {'dap': d}

    def lane(h):
        return pl.ds(pl.multiple_of(h * seq, LANES), seq)

    def rblk(d, n=rows):
        return part(d, n)

    barrier = pltpu.get_barrier_semaphore()
    for k in range(1, 8):
        pl.semaphore_signal(barrier, inc=1, device_id=dev(partner(me, k)), device_id_type=pl.DeviceIdType.MESH)
    pl.semaphore_wait(barrier, 7)

    def remote(src, dst, ssem, rsem, target):
        return pltpu.make_async_remote_copy(
            src_ref=src, dst_ref=dst, send_sem=ssem, recv_sem=rsem,
            device_id=dev(target), device_id_type=pl.DeviceIdType.MESH)

    def e_copy(k):
        to = partner(me, k)
        return remote(xe.at[:, :, lane(to)], e_out.at[rblk(me)], e_ssem.at[k], e_rsem.at[k], to)

    for k in (1, 2, 4, 3, 5, 6, 7):
        e_copy(k).start()

    def m_copy(k):
        to = partner(me, k)
        return remote(xm.at[rblk(to, mseq)], m_out.at[:, rblk(me), :], m_ssem.at[k], m_rsem.at[k], to)

    def row_of(ref):
        v = ref[:].astype(F32)
        return v.reshape(1, v.shape[0])

    def weights(wf, wp):
        gam_e[:] = column(row_of(e_gam), HALF, 1)
        bet_e[:] = column(row_of(e_bet), HALF, 1)
        bias_b[:] = column(row_of(e_br), HID * RG, RG)
        bias_a[:] = column(row_of(e_bl), HID, 1)
        bo_e[:] = column(row_of(e_bo), LANES, 1)
        bo_m[:] = column(row_of(m_bo), LANES, 1)
        bias_m[:HID] = column(row_of(m_bl), HID, 1)
        bias_m[HID:] = column(row_of(m_br), HID, 1)
        w_m[:HID] = m_wl[:]
        w_m[HID:] = m_wr[:]

        def wide(ref, n):
            w = ref[:].astype(F32)
            return jnp.concatenate([w] * n, axis=1)

        def place(dst, rep, residue):
            at = lax.broadcasted_iota(jnp.int32, dst.shape, 0)
            dst[:] = jnp.where(residue(at) == lax.broadcasted_iota(jnp.int32, dst.shape, 1) // CE, rep, 0.0).astype(BF)

        w = wide(e_wr, RG)
        place(w_right, jnp.broadcast_to(w[:, None, :], (HID, RG, RG * CE)).reshape(HID * RG, RG * CE), lambda at: at % RG)
        place(w_left, jnp.concatenate([wide(e_wl, LG)] * LG, axis=0), lambda at: at // HID)
        for src, dst in ((e_wo, wo_e), (m_wo, wo_m)):
            wf[:] = src[:].astype(F32)

            def pick(q):
                wp[part(q, HID), :] = wf[pl.ds(q, HID, stride=HID), :]
            loop(HID, pick)
            dst[:] = wp[:].T.astype(BF)

    pl.run_scoped(weights, pltpu.VMEM((1024, LANES), F32), pltpu.VMEM((1024, LANES), F32))

    def masks(mt):
        mt[:] = mask_m[:].astype(F32).T
        own = mt[rblk(me), :]
        mask_mo[:] = own.reshape(rows, 1, mask_m.shape[0])
        cnt_m[:] = jnp.dot(own.astype(BF), mask_m[:].astype(F32).astype(BF),
                             preferred_element_type=F32).reshape(rows, 1, res)

    pl.run_scoped(masks, pltpu.VMEM((res, mask_m.shape[0]), F32))

    def load_mask(d):
        cp = pltpu.make_async_copy(mask_e.at[rblk(d, seq)], mask_i, lsem.at[0])
        cp.start()
        cp.wait()

    def main_proj(xc, xf, bf):
        cp = pltpu.make_async_copy(xm.at[rblk(me, mseq)], xc.at[pl.ds(0, mseq)], lsem.at[1])
        cp.start()
        cp.wait()
        cp = pltpu.make_async_copy(xc.at[pl.ds(0, mseq)], m_out.at[:, rblk(me), :], lsem.at[1])
        cp.start()
        cp.wait()
        step = xc.shape[0]
        gam_m, bet_m = row_of(m_gam), row_of(m_bet)
        for piece in range(xm.shape[0] // step):
            cp = pltpu.make_async_copy(xm.at[pl.ds(piece * step, step)], xc, lsem.at[2])
            cp.start()
            cp.wait()

            def widen(i):
                s = part(i, 8)
                xf[s] = xc[s].astype(F32)
            loop(step // 8, widen)

            def one(r):
                x = xf[:, r, :]
                mean = jnp.mean(x, axis=1, keepdims=True)
                cen = x - mean
                var = jnp.mean(cen * cen, axis=1, keepdims=True)
                y = (cen * lax.rsqrt(var + LN_EPS) * gam_m + bet_m).astype(BF)
                proj = nt_dot(w_m[:], y) + bias_m[:]
                proj = proj * mask_mo[r, :, pl.ds(piece * step, step)]
                am[part(r, HID), pl.ds(piece * step, step)] = proj[:HID].astype(BF)
                bf[:, r, :] = proj[HID:]
            def some(i):
                for u in range(MSTEP):
                    one(i * MSTEP + u)

            loop(rows // MSTEP, some)
            bm[:, rblk(me), pl.ds(piece * step, step)] = bf[:].astype(BF)

    pl.run_scoped(
        main_proj, pltpu.VMEM((LANES, rows, xm.shape[2]), BF), pltpu.VMEM((LANES, rows, xm.shape[2]), F32),
        pltpu.VMEM((HID, rows, LANES), F32))

    def g_copy(i):
        ref = bm.at[:, rblk(me), :]
        return remote(ref, ref, g_ssem.at[i], g_rsem.at[i], partner(me, (1, 2, 4, 6)[i]))

    def g_wait(i):
        to = partner(me, (1, 2, 4, 6)[i])
        ref = bm.at[:, rblk(to), :]
        return remote(ref, ref, g_ssem.at[i], g_rsem.at[i], to)

    def f_copy(i):
        ref = bm.at[:, rblk(partner(me, (2, 4, 6)[i])), :]
        return remote(ref, ref, f_ssem.at[i], f_rsem.at[i], sib)

    def f_wait(i):
        ref = bm.at[:, rblk(partner(me, (3, 5, 7)[i])), :]
        return remote(ref, ref, f_ssem.at[i], f_rsem.at[i], sib)

    for i in range(4):
        g_copy(i).start()
    for k in (1, 2, 4):
        m_copy(k).start()

    def project(hh, m16):
        def norm(i):
            for u in range(LSTEP):
                r = i * LSTEP + u
                x = xb[hh * GROUP + r].astype(F32)
                mean = jnp.mean(x, axis=0, keepdims=True)
                cen = x - mean
                var = jnp.mean(cen * cen, axis=0, keepdims=True)
                y = cen * lax.rsqrt(var + LN_EPS) * gam_e[:] + bet_e[:]
                y_s[part(r, CE), :] = y.astype(BF)
        loop(GROUP // LSTEP, norm)

        def dot(w, g):
            return jnp.dot(w[:], y_s[pl.ds(g * w.shape[1], w.shape[1])], preferred_element_type=F32)

        right = jnp.concatenate(
            [(dot(w_right, g) + bias_b[:]).reshape(HID, RG, seq) for g in range(GROUP // RG)], axis=1)
        right = (right * m16[None]).astype(BF)
        left = []
        for g in range(GROUP // LG):
            d = dot(w_left, g)
            for r in range(LG):
                left.append((d[r * HID:r * HID + HID] + bias_a[:]) * m16[g * LG + r:g * LG + r + 1])
        left = jnp.concatenate(left, axis=0).astype(BF)
        return right, left

    lane_lo = lax.broadcasted_iota(jnp.int32, (LANES, LANES), 1) < HALF

    def ob_copy(d, e, h):
        ref = rt.at[d % 4, :, pl.ds(pl.multiple_of(e * HALF + h * rows, rows), rows), :]
        return remote(ref, ref, ob_ssem.at[d % 4 * 2 + e], ob_rsem.at[d % 4 * 2 + e], sib)

    def own_pairs(mt, cnt, a_own, acc, o_pair):
        cnt[:] = jnp.zeros_like(cnt)

        def zero(g):
            acc[g] = jnp.zeros(acc.shape[1:], F32)
        loop(acc.shape[0], zero)

        def chunk(d):
            xcp = pltpu.make_async_copy(xe.at[:, :, lane(d)], xb, lsem.at[1])
            xcp.start()
            load_mask(d)
            m = mask_i[:].astype(F32)
            mt[:] = m.T
            cnt[:] += jnp.dot(mt[rblk(me), :].astype(BF), m.astype(BF), preferred_element_type=F32)

            @pl.when(d >= 4)
            def _():
                for e in range(2):
                    ob_copy(d, e, core).wait_send()
            xcp.wait()

            def half(hh):
                right, left = project(hh, mt[pl.ds(pl.multiple_of(me * rows + hh * GROUP, GROUP), GROUP), :])
                right = right.reshape(16, 2, GROUP, seq)
                for e in range(2):
                    at = pl.ds(pl.multiple_of(e * HALF + core * rows + hh * GROUP, GROUP), GROUP)
                    rt[d % 4, :, at, :] = right[:, e]
                a_own[d % 2, part(hh, GROUP * HID), :] = left
            loop(rows // GROUP, half)

            @pl.when((d // 4) * ((d + 1) % 2) == 1)
            def _():
                pl.semaphore_wait(ob_free, 1)
            for e in range(2):
                ob_copy(d, e, core).start()

            @pl.when(d % 2 == 1)
            def _():
                for e in range(2):
                    ob_copy(d - 1, e, 1 - core).wait_recv()
                    ob_copy(d, e, 1 - core).wait_recv()

                def group(g):
                    at = part(g, 2)
                    acc[g] += (nt_dot(a_own[0], rt[(d - 1) % 4, at].reshape(256, seq))
                               + nt_dot(a_own[1], rt[d % 4, at].reshape(256, seq)))
                loop(acc.shape[0], group)

                @pl.when(d < 4)
                def _():
                    pl.semaphore_signal(ob_free, inc=1, device_id=dev(sib), device_id_type=pl.DeviceIdType.MESH)
        loop(8, chunk)
        cnt_e[:] = cnt[:].reshape(rows, 1, res)

        def pair_rows(n):
            for g in range(8):
                t = acc[g, part(n, HALF), :]
                for b in range(2):
                    u0, u1 = t[:HID, b * LANES:b * LANES + LANES], t[HID:, b * LANES:b * LANES + LANES]
                    q = g * 4 + b * 2
                    lo = lane_lo[:HID]
                    o_pair[q * HID:q * HID + HID, :] = jnp.where(lo, u0, pltpu.roll(u1, HALF, 1)).astype(BF)
                    o_pair[q * HID + HID:q * HID + HALF, :] = jnp.where(lo, pltpu.roll(u0, HALF, 1), u1).astype(BF)
            r_own[n] = jnp.dot(wo_e[:], o_pair[:], preferred_element_type=F32)
        loop(rows // 2, pair_rows)
        for d in range(4, 8):
            for e in range(2):
                ob_copy(d, e, core).wait_send()
        load_mask(me)
        mask_et[:] = mask_i[:].astype(F32).T

    pl.run_scoped(
        own_pairs, pltpu.VMEM((res, seq), F32), pltpu.VMEM((rows, res), F32),
        pltpu.VMEM((2, rows * HID, seq), BF), pltpu.VMEM((8, rows * HID, 256), F32), pltpu.VMEM((1024, LANES), BF))

    def xb_copy(src):
        ref = b_all.at[:, rblk(src), lane(core)]
        return remote(ref, ref, xb_ssem.at[src], xb_rsem.at[src], sib)

    def xb_wait(src):
        ref = b_all.at[:, rblk(src), lane(1 - core)]
        return remote(ref, ref, xb_ssem.at[src], xb_rsem.at[src], sib)

    def xa_copy(c):
        return remote(a_send.at[rblk(c, rows * HID)], a_all.at[rblk(c, rows * HID), lane(core)],
                      xa_ssem.at[c], xa_rsem.at[c], sib)

    def xa_wait(c):
        return remote(a_send.at[rblk(c, rows * HID)], a_all.at[rblk(c, rows * HID), lane(1 - core)],
                      xa_ssem.at[c], xa_rsem.at[c], sib)

    def block(k):
        src = partner(me, k)
        own_half = (src % 2 + core) % 2

        @pl.when(k == 0)
        def _():
            cp = pltpu.make_async_copy(xe.at[:, :, lane(me)], xb, lsem.at[0])
            cp.start()
            cp.wait()
            cp = pltpu.make_async_copy(xb, e_out.at[rblk(me)], lsem.at[0])
            cp.start()
            cp.wait()

        @pl.when(k > 0)
        def _():
            remote(xe.at[:, :, lane(src)], e_out.at[rblk(src)], e_ssem.at[k], e_rsem.at[k], src).wait_recv()
            cp = pltpu.make_async_copy(e_out.at[rblk(src)], xb, lsem.at[0])
            cp.start()
            cp.wait()

        def half(hh):
            r0 = pl.multiple_of(src * rows + hh * GROUP, GROUP)
            right, left = project(hh, mask_et[pl.ds(r0, GROUP), :])
            b_all[:, pl.ds(r0, GROUP), lane(core)] = right
            at = pl.ds(pl.multiple_of(((src // 2) * rows + hh * GROUP) * HID, GROUP * HID), GROUP * HID)

            @pl.when(own_half == 0)
            def _():
                a_all[at, lane(core)] = left

            @pl.when(own_half == 1)
            def _():
                a_send[at, :] = left
        loop(rows // GROUP, half)
        xb_copy(src).start()

        @pl.when(own_half == 1)
        def _():
            xa_copy(src // 2).start()
    loop(8, block)

    for k in range(1, 8):
        e_copy(k).wait_send()


    def xwait(s):
        xb_wait(s).wait_recv()
    loop(8, xwait)

    def xwait_a(c):
        xa_wait(c).wait_recv()
    loop(4, xwait_a)

    def rs_copy(n):
        t, ib, k = ((0, 0, 2), (0, 1, 4), (1, 0, 2), (2, 1, 4), (2, 0, 4), (1, 1, 2))[n]
        at = pl.ds(ib * GROUP // 2, GROUP // 2)
        dst = rs_mid.at[ib] if t == 0 else rs_recv.at[t - 1, at]
        return remote(rt.at[t, at], dst, rs_ssem.at[n], rs_rsem.at[n], partner(me, k))

    def contract(o_s, tm):
        def outer(left, right_of):
            def qstep(qq):
                for u in range(QSTEP):
                    q = qq * QSTEP + u
                    o = nt_dot(left(), right_of(q))
                    o_s[:, part(q, HID), :] = o.astype(BF).reshape(GROUP, HID, res)
            loop(HID // QSTEP, qstep)

        def eblk(n):
            t = ((n // 2 + 1) // 2) % 2 * (1 + (n // 2 + n + 1) % 2) + 3 * (n // 6)
            ib = n % 2
            c = partner(me, 2 * (1 - t // 2) + 4 * (1 - t % 2)) // 2
            at = pl.ds(pl.multiple_of((c * rows + ib * GROUP) * HID, GROUP * HID), GROUP * HID)
            outer(lambda: a_all[at, :], lambda q: b_all[q])

            hi0 = lax.broadcasted_iota(jnp.int32, (LANES, LANES), 0) * 0 + c // 2 == 0
            odd = lax.broadcasted_iota(jnp.int32, (LANES, LANES), 0) * 0 + c % 2 == 1

            def rstep(ii):
                for u in range(RSTEP // 2):
                    n2 = ii * (RSTEP // 2) + u
                    away, near = [], []
                    for v in range(2):
                        r = jnp.dot(wo_e[:], o_s[n2 * 2 + v], preferred_element_type=F32)
                        away.append(jnp.where(hi0, r[:, LANES:], r[:, :LANES]))
                        near.append(jnp.where(hi0, r[:, :LANES], r[:, LANES:]))
                    n0 = jnp.where(odd, near[0], pltpu.roll(near[0], HALF, 1))
                    n1 = jnp.where(odd, pltpu.roll(near[1], HALF, 1), near[1])
                    rt[t, ib * (GROUP // 2) + n2] = jnp.concatenate(
                        [away[0], away[1], jnp.where(lane_lo, n0, n1)], axis=1).astype(BF)
            loop(GROUP // RSTEP, rstep)

            for v in range(6):
                @pl.when(n == v)
                def _():
                    if v >= 4:
                        rs_copy(v - 4).wait_recv()

                        def add(i):
                            at = (t, ib * (GROUP // 2) + i)
                            rt[at] = (rt[at].astype(F32) + rs_mid[v - 4, i].astype(F32)).astype(BF)
                        loop(GROUP // 2, add)
                    rs_copy(v).start()
                    if v == 1:
                        for k in (3, 5, 6, 7):
                            m_copy(k).start()
        loop(8, eblk)

        for i in range(1, 4):
            g_wait(i).wait_recv()
            f_copy(i - 1).start()
        g_wait(0).wait_recv()
        for i in range(3):
            f_wait(i).wait_recv()

        def mblk(ib):
            at = part(ib, GROUP * HID)
            outer(lambda: am[at, :], lambda q: bm[q])

            def rstep(ii):
                for u in range(RSTEP):
                    i = ii * RSTEP + u
                    row = ib * GROUP + i
                    r = jnp.dot(wo_m[:], o_s[i], preferred_element_type=F32)
                    tm[row] = (r + bo_m[:]) / (NORM_EPS + cnt_m[row])
            loop(GROUP // RSTEP, rstep)
        loop(rows // GROUP, mblk)

        def final(zb):
            def z_copy(j):
                return pltpu.make_async_copy(pair.at[pl.ds(j * 8, 8)], zb.at[j % 2], lsem.at[3 + j % 2])

            def o_copy(j):
                return pltpu.make_async_copy(zb.at[j % 2], pair_out.at[pl.ds(j * 8, 8)], lsem.at[5 + j % 2])

            hi0 = lax.broadcasted_iota(jnp.int32, (LANES, LANES), 0) * 0 + chip // 2 == 0
            odd = lax.broadcasted_iota(jnp.int32, (LANES, LANES), 0) * 0 + chip % 2 == 1
            z_copy(0).start()
            for j in range(rows // 8):
                if j % 2 == 0:
                    for n in ((2, 4), (3, 5))[j // 2]:
                        rs_copy(n).wait_recv()
                if j >= 1:
                    o_copy(j - 1).wait()
                if j + 1 < rows // 8:
                    z_copy(j + 1).start()
                z_copy(j).wait()

                def row2(i):
                    n = j * 4 + i
                    tot = rt[3, n].astype(F32) + rs_recv[0, n].astype(F32) + rs_recv[1, n].astype(F32)
                    kept, own = tot[:, 256:], r_own[n]
                    rkept, rown = pltpu.roll(kept, HALF, 1), pltpu.roll(own, HALF, 1)
                    near0 = jnp.where(lane_lo, jnp.where(odd, kept, own), jnp.where(odd, rown, rkept))
                    near1 = jnp.where(lane_lo, jnp.where(odd, rkept, rown), jnp.where(odd, own, kept))
                    for v, near in ((0, near0), (1, near1)):
                        away = tot[:, v * LANES:v * LANES + LANES]
                        row = n * 2 + v
                        r = jnp.concatenate([jnp.where(hi0, near, away), jnp.where(hi0, away, near)], axis=1)
                        te = (r + bo_e[:]) / (NORM_EPS + cnt_e[row])
                        zb[j % 2, i * 2 + v] = (zb[j % 2, i * 2 + v] + te.T) + tm[row].T
                loop(4, row2)
                o_copy(j).start()
            o_copy(rows // 8 - 1).wait()

        pl.run_scoped(final, pltpu.VMEM((2, 8, res, LANES), F32))

    pl.run_scoped(contract, pltpu.VMEM((GROUP, 1024, res), BF), pltpu.VMEM((rows, LANES, res), F32))

    for k in range(1, 8):
        m_copy(k).wait_send()
        to = partner(me, k)
        remote(xm.at[rblk(me, mseq)], m_out.at[:, rblk(to), :], m_ssem.at[k], m_rsem.at[k], to).wait_recv()

    def drain(s):
        xb_copy(s).wait_send()
    loop(8, drain)

    def drain_a(c):
        xa_copy(c).wait_send()
    loop(4, drain_a)
    for i in range(4):
        g_copy(i).wait_send()
    for i in range(3):
        f_copy(i).wait_send()
    for n in range(6):
        rs_copy(n).wait_send()


def solution(mesh):
    msa_spec = P('data', 'dap', None)
    mask_spec = P('data', None)
    row_spec = P(('data', 'dap'), None, None)

    def local_program(extra_block, extra_mask, main_block, main_mask, pair_rows,
                      e_gam, e_bet, e_wl, e_bl, e_wr, e_br, e_wo, e_bo,
                      m_gam, m_bet, m_wl, m_bl, m_wr, m_br, m_wo, m_bo):
        seqs, rows, ce = extra_block.shape
        mseqs, _, cm = main_block.shape
        res = extra_mask.shape[1]
        hid = e_wl.shape[1]
        nk = e_wo.shape[1]
        seq = seqs // 8
        args = (
            jnp.transpose(extra_block, (1, 2, 0)), main_block, extra_mask, main_mask, pair_rows,
            e_gam, e_bet, e_wl.T, e_bl, e_wr.T, e_br, e_wo, e_bo, m_gam, m_bet, m_wl.T, m_bl, m_wr.T, m_br, m_wo, m_bo)
        any_spec = pl.BlockSpec(memory_space=pl.ANY)
        vmem = pl.BlockSpec(memory_space=pltpu.VMEM)
        dma = pltpu.SemaphoreType.DMA
        pair_out, e_recv, m_recv = pl.pallas_call(
            opm_kernel,
            out_shape=(
                jax.ShapeDtypeStruct((rows, res, nk), F32),
                jax.ShapeDtypeStruct((res, ce, seq), BF),
                jax.ShapeDtypeStruct((mseqs // 8, res, cm), BF)),
            in_specs=[any_spec, any_spec, any_spec, vmem, any_spec] + [vmem] * 16,
            out_specs=(any_spec,) * 3,
            scratch_shapes=[
                pltpu.VMEM((4 * rows * hid, 2 * seq), BF),
                pltpu.VMEM((hid, res, 2 * seq), BF),
                pltpu.VMEM((4 * rows * hid, seq), BF),
                pltpu.VMEM((rows, ce, seq), BF),
                pltpu.VMEM((GROUP * ce, seq), BF),
                pltpu.VMEM((seq, res), jnp.int32),
                pltpu.VMEM((res, seq), F32),
                pltpu.VMEM((rows, 1, mseqs), F32),
                pltpu.VMEM((rows * hid, mseqs), BF),
                pltpu.VMEM((hid, res, mseqs), BF),
                pltpu.VMEM((4, rows // 2, nk, res // 2 * 3), BF),
                pltpu.VMEM((2, GROUP // 2, nk, res // 2 * 3), BF),
                pltpu.VMEM((2, rows // 2, nk, res // 2 * 3), BF),
                pltpu.VMEM((rows // 2, nk, res // 2), F32),
                pltpu.VMEM((hid * RG, ce * RG), BF),
                pltpu.VMEM((hid * LG, ce * LG), BF),
                pltpu.VMEM((2 * hid, cm), BF),
                pltpu.VMEM((nk, hid * hid), BF),
                pltpu.VMEM((nk, hid * hid), BF),
                pltpu.VMEM((ce, 1), F32),
                pltpu.VMEM((ce, 1), F32),
                pltpu.VMEM((hid * RG, 1), F32),
                pltpu.VMEM((hid, 1), F32),
                pltpu.VMEM((nk, 1), F32),
                pltpu.VMEM((2 * hid, 1), F32),
                pltpu.VMEM((nk, 1), F32),
                pltpu.VMEM((rows, 1, res), F32),
                pltpu.VMEM((rows, 1, res), F32),
                dma((8,)), dma((8,)), dma((8,)), dma((8,)), dma((4,)), dma((4,)), dma((8,)), dma((8,)),
                dma((4,)), dma((4,)), dma((3,)), dma((3,)), dma((6,)), dma((6,)),
                dma((8,)), dma((8,)), pltpu.SemaphoreType.REGULAR, dma((8,))],
            compiler_params=pltpu.CompilerParams(
                collective_id=0, has_side_effects=True, vmem_limit_bytes=67043328),
            name='opm',
        )(*args)
        return pair_out, jnp.transpose(e_recv, (2, 0, 1)), m_recv

    in_specs = (msa_spec, mask_spec, msa_spec, mask_spec, row_spec) + (P(),) * 16
    return jax.shard_map(local_program, mesh=mesh, in_specs=in_specs, out_specs=(row_spec,) * 3, check_vma=False)
```

```python
import functools

import jax
import jax.numpy as jnp
from jax import lax
from jax.experimental import pallas as pl
from jax.experimental.pallas import tpu as pltpu
from jax.sharding import PartitionSpec as P

LN_EPS = 1e-5
NORM_EPS = 1e-3
BF = jnp.bfloat16
F32 = jnp.float32
GROUP = 16
VMEM_LIMIT = 58 * 2 ** 20
QSTEP = 4
LSTEP = 4
MSTEP = 8
RG, LG = 8, 4
HID, CE, LANES, HALF = 32, 64, 128, 64
RSTEP = 8


def loop(n, body):
    def step(i, carry):
        body(i)
        return carry
    lax.fori_loop(0, n, step, 0)


def part(i, n):
    return pl.ds(pl.multiple_of(i * n, n), n)


def partner(me, k):
    core, cx, cy = me % 2, (me // 2) % 2, me // 4
    k0, k1, k2 = k % 2, (k // 2) % 2, k // 4
    return (core + k0) % 2 + 2 * ((cx + k1) % 2) + 4 * ((cy + k2) % 2)


def nt_dot(lhs, rhs):
    return lax.dot_general(lhs, rhs, (((1,), (1,)), ((), ())), preferred_element_type=F32)


def column(row, n, repeat):
    m = row.shape[1]
    at = lax.broadcasted_iota(jnp.int32, (n, m), 0) // repeat
    return jnp.sum(jnp.where(at == lax.broadcasted_iota(jnp.int32, (n, m), 1), row, 0.0), axis=1, keepdims=True)


def opm_kernel(
    xe, xm, mask_e, mask_m, pair,
    e_gam, e_bet, e_wl, e_bl, e_wr, e_br, e_wo, e_bo,
    m_gam, m_bet, m_wl, m_bl, m_wr, m_br, m_wo, m_bo,
    pair_out, e_t, m_out, e_out,
    a_all, b_all, a_send, xb, y_s, mask_i, mask_et, mask_mo, am, bm, rt, rs_mid, rs_recv, r_own,
    w_right, w_left, w_m, wo_e, wo_m, gam_e, bet_e, bias_b, bias_a, bo_e, bias_m, bo_m, cnt_e, cnt_m,
    e_ssem, e_rsem, m_ssem, m_rsem, xa_ssem, xa_rsem, xb_ssem, xb_rsem,
    d_ssem, d_rsem, t_isem, t_osem, g_ssem, g_rsem, f_ssem, f_rsem, rs_ssem, rs_rsem, ob_ssem, ob_rsem, ob_free, lsem,
):
    me = lax.axis_index('dap')
    core = me % 2
    chip = me // 2
    sib = partner(me, 1)
    seq = e_out.shape[2]
    mseq = m_out.shape[0]
    rows = xe.shape[0]
    res = e_out.shape[0]

    def dev(d):
        return {'dap': d}

    def lane(h):
        return pl.ds(pl.multiple_of(h * seq, LANES), seq)

    def rblk(d, n=rows):
        return part(d, n)

    barrier = pltpu.get_barrier_semaphore()
    for k in range(1, 8):
        pl.semaphore_signal(barrier, inc=1, device_id=dev(partner(me, k)), device_id_type=pl.DeviceIdType.MESH)
    pl.semaphore_wait(barrier, 7)

    def remote(src, dst, ssem, rsem, target):
        return pltpu.make_async_remote_copy(
            src_ref=src, dst_ref=dst, send_sem=ssem, recv_sem=rsem,
            device_id=dev(target), device_id_type=pl.DeviceIdType.MESH)

    def e_copy(k):
        to = partner(me, k)
        return remote(xe.at[:, :, lane(to)], e_out.at[rblk(me)], e_ssem.at[k], e_rsem.at[k], to)

    for k in (1, 2, 4, 3, 5, 6, 7):
        e_copy(k).start()

    def m_copy(k):
        to = partner(me, k)
        return remote(xm.at[rblk(to, mseq)], m_out.at[:, rblk(me), :], m_ssem.at[k], m_rsem.at[k], to)

    def row_of(ref):
        v = ref[:].astype(F32)
        return v.reshape(1, v.shape[0])

    def weights(wf, wp):
        gam_e[:] = column(row_of(e_gam), HALF, 1)
        bet_e[:] = column(row_of(e_bet), HALF, 1)
        bias_b[:] = column(row_of(e_br), HID * RG, RG)
        bias_a[:] = column(row_of(e_bl), HID, 1)
        bo_e[:] = column(row_of(e_bo), LANES, 1)
        bo_m[:] = column(row_of(m_bo), LANES, 1)
        bias_m[:HID] = column(row_of(m_bl), HID, 1)
        bias_m[HID:] = column(row_of(m_br), HID, 1)
        w_m[:HID] = m_wl[:]
        w_m[HID:] = m_wr[:]

        def wide(ref, n):
            w = ref[:].astype(F32)
            return jnp.concatenate([w] * n, axis=1)

        def place(dst, rep, residue):
            at = lax.broadcasted_iota(jnp.int32, dst.shape, 0)
            dst[:] = jnp.where(residue(at) == lax.broadcasted_iota(jnp.int32, dst.shape, 1) // CE, rep, 0.0).astype(BF)

        w = wide(e_wr, RG)
        place(w_right, jnp.broadcast_to(w[:, None, :], (HID, RG, RG * CE)).reshape(HID * RG, RG * CE), lambda at: at % RG)
        place(w_left, jnp.concatenate([wide(e_wl, LG)] * LG, axis=0), lambda at: at // HID)
        for src, dst in ((e_wo, wo_e), (m_wo, wo_m)):
            wf[:] = src[:].astype(F32)

            def pick(q):
                wp[part(q, HID), :] = wf[pl.ds(q, HID, stride=HID), :]
            loop(HID, pick)
            dst[:] = wp[:].T.astype(BF)

    pl.run_scoped(weights, pltpu.VMEM((1024, LANES), F32), pltpu.VMEM((1024, LANES), F32))

    def masks(mt):
        mt[:] = mask_m[:].astype(F32).T
        own = mt[rblk(me), :]
        mask_mo[:] = own.reshape(rows, 1, mask_m.shape[0])
        cnt_m[:] = jnp.dot(own.astype(BF), mask_m[:].astype(F32).astype(BF),
                             preferred_element_type=F32).reshape(rows, 1, res)

    pl.run_scoped(masks, pltpu.VMEM((res, mask_m.shape[0]), F32))

    def load_mask(d):
        cp = pltpu.make_async_copy(mask_e.at[rblk(d, seq)], mask_i, lsem.at[0])
        cp.start()
        cp.wait()

    def main_proj(xc, xf, bf):
        cp = pltpu.make_async_copy(xm.at[rblk(me, mseq)], xc.at[pl.ds(0, mseq)], lsem.at[1])
        cp.start()
        cp.wait()
        cp = pltpu.make_async_copy(xc.at[pl.ds(0, mseq)], m_out.at[:, rblk(me), :], lsem.at[1])
        cp.start()
        cp.wait()
        step = xc.shape[0]
        gam_m, bet_m = row_of(m_gam), row_of(m_bet)
        for piece in range(xm.shape[0] // step):
            cp = pltpu.make_async_copy(xm.at[pl.ds(piece * step, step)], xc, lsem.at[2])
            cp.start()
            cp.wait()

            def widen(i):
                s = part(i, 8)
                xf[s] = xc[s].astype(F32)
            loop(step // 8, widen)

            def one(r):
                x = xf[:, r, :]
                mean = jnp.mean(x, axis=1, keepdims=True)
                cen = x - mean
                var = jnp.mean(cen * cen, axis=1, keepdims=True)
                y = (cen * lax.rsqrt(var + LN_EPS) * gam_m + bet_m).astype(BF)
                proj = nt_dot(w_m[:], y) + bias_m[:]
                proj = proj * mask_mo[r, :, pl.ds(piece * step, step)]
                am[part(r, HID), pl.ds(piece * step, step)] = proj[:HID].astype(BF)
                bf[:, r, :] = proj[HID:]
            def some(i):
                for u in range(MSTEP):
                    one(i * MSTEP + u)

            loop(rows // MSTEP, some)
            bm[:, rblk(me), pl.ds(piece * step, step)] = bf[:].astype(BF)

    pl.run_scoped(
        main_proj, pltpu.VMEM((LANES, rows, xm.shape[2]), BF), pltpu.VMEM((LANES, rows, xm.shape[2]), F32),
        pltpu.VMEM((HID, rows, LANES), F32))

    def g_copy(i):
        ref = bm.at[:, rblk(me), :]
        return remote(ref, ref, g_ssem.at[i], g_rsem.at[i], partner(me, (1, 2, 4)[i]))

    def g_wait(i):
        to = partner(me, (1, 2, 4)[i])
        ref = bm.at[:, rblk(to), :]
        return remote(ref, ref, g_ssem.at[i], g_rsem.at[i], to)

    def d_copy(i):
        ref = bm.at[part(i, HID // 2), rblk(partner(me, (2, 4)[i])), :]
        return remote(ref, ref, d_ssem.at[i], d_rsem.at[i], partner(me, (4, 2)[i]))

    def d_wait(i):
        ref = bm.at[part(i, HID // 2), rblk(partner(me, 6)), :]
        return remote(ref, ref, d_ssem.at[i], d_rsem.at[i], partner(me, (4, 2)[i]))

    def f_copy(i):
        ref = bm.at[:, rblk(partner(me, (2, 4, 6)[i])), :]
        return remote(ref, ref, f_ssem.at[i], f_rsem.at[i], sib)

    def f_wait(i):
        ref = bm.at[:, rblk(partner(me, (3, 5, 7)[i])), :]
        return remote(ref, ref, f_ssem.at[i], f_rsem.at[i], sib)

    for i in range(3):
        g_copy(i).start()
    for k in (1, 2, 4):
        m_copy(k).start()

    def project(hh, m16):
        def norm(i):
            for u in range(LSTEP):
                r = i * LSTEP + u
                x = xb[hh * GROUP + r].astype(F32)
                mean = jnp.mean(x, axis=0, keepdims=True)
                cen = x - mean
                var = jnp.mean(cen * cen, axis=0, keepdims=True)
                y = cen * lax.rsqrt(var + LN_EPS) * gam_e[:] + bet_e[:]
                y_s[part(r, CE), :] = y.astype(BF)
        loop(GROUP // LSTEP, norm)

        def dot(w, g):
            return jnp.dot(w[:], y_s[pl.ds(g * w.shape[1], w.shape[1])], preferred_element_type=F32)

        right = jnp.concatenate(
            [(dot(w_right, g) + bias_b[:]).reshape(HID, RG, seq) for g in range(GROUP // RG)], axis=1)
        right = (right * m16[None]).astype(BF)
        left = []
        for g in range(GROUP // LG):
            d = dot(w_left, g)
            for r in range(LG):
                left.append((d[r * HID:r * HID + HID] + bias_a[:]) * m16[g * LG + r:g * LG + r + 1])
        left = jnp.concatenate(left, axis=0).astype(BF)
        return right, left

    lane_lo = lax.broadcasted_iota(jnp.int32, (LANES, LANES), 1) < HALF

    def ob_copy(d, e, h):
        ref = rt.at[d % 4, :, pl.ds(pl.multiple_of(e * HALF + h * rows, rows), rows), :]
        return remote(ref, ref, ob_ssem.at[d % 4 * 2 + e], ob_rsem.at[d % 4 * 2 + e], sib)

    def own_pairs(mt, cnt, a_own, acc, o_pair):
        cnt[:] = jnp.zeros_like(cnt)

        def zero(g):
            acc[g] = jnp.zeros(acc.shape[1:], F32)
        loop(acc.shape[0], zero)

        def chunk(d):
            xcp = pltpu.make_async_copy(xe.at[:, :, lane(d)], xb, lsem.at[1])
            xcp.start()
            load_mask(d)
            m = mask_i[:].astype(F32)
            mt[:] = m.T
            cnt[:] += jnp.dot(mt[rblk(me), :].astype(BF), m.astype(BF), preferred_element_type=F32)

            @pl.when(d >= 4)
            def _():
                for e in range(2):
                    ob_copy(d, e, core).wait_send()
            xcp.wait()

            def half(hh):
                right, left = project(hh, mt[pl.ds(pl.multiple_of(me * rows + hh * GROUP, GROUP), GROUP), :])
                right = right.reshape(16, 2, GROUP, seq)
                for e in range(2):
                    at = pl.ds(pl.multiple_of(e * HALF + core * rows + hh * GROUP, GROUP), GROUP)
                    rt[d % 4, :, at, :] = right[:, e]
                a_own[d % 2, part(hh, GROUP * HID), :] = left
            loop(rows // GROUP, half)

            @pl.when((d // 4) * ((d + 1) % 2) == 1)
            def _():
                pl.semaphore_wait(ob_free, 1)
            for e in range(2):
                ob_copy(d, e, core).start()

            @pl.when(d % 2 == 1)
            def _():
                for e in range(2):
                    ob_copy(d - 1, e, 1 - core).wait_recv()
                    ob_copy(d, e, 1 - core).wait_recv()

                def group(g):
                    at = part(g, 2)
                    acc[g] += (nt_dot(a_own[0], rt[(d - 1) % 4, at].reshape(256, seq))
                               + nt_dot(a_own[1], rt[d % 4, at].reshape(256, seq)))
                loop(acc.shape[0], group)

                @pl.when(d < 4)
                def _():
                    pl.semaphore_signal(ob_free, inc=1, device_id=dev(sib), device_id_type=pl.DeviceIdType.MESH)
        loop(8, chunk)
        cnt_e[:] = cnt[:].reshape(rows, 1, res)

        def pair_rows(n):
            for g in range(8):
                t = acc[g, part(n, HALF), :]
                for b in range(2):
                    u0, u1 = t[:HID, b * LANES:b * LANES + LANES], t[HID:, b * LANES:b * LANES + LANES]
                    q = g * 4 + b * 2
                    lo = lane_lo[:HID]
                    o_pair[q * HID:q * HID + HID, :] = jnp.where(lo, u0, pltpu.roll(u1, HALF, 1)).astype(BF)
                    o_pair[q * HID + HID:q * HID + HALF, :] = jnp.where(lo, pltpu.roll(u0, HALF, 1), u1).astype(BF)
            r_own[n] = jnp.dot(wo_e[:], o_pair[:], preferred_element_type=F32)
        loop(rows // 2, pair_rows)
        for d in range(4, 8):
            for e in range(2):
                ob_copy(d, e, core).wait_send()
        load_mask(me)
        mask_et[:] = mask_i[:].astype(F32).T

    pl.run_scoped(
        own_pairs, pltpu.VMEM((res, seq), F32), pltpu.VMEM((rows, res), F32),
        pltpu.VMEM((2, rows * HID, seq), BF), pltpu.VMEM((8, rows * HID, 256), F32), pltpu.VMEM((1024, LANES), BF))

    def transpose(yh):
        def body(tin, tout, f_in, f_out):
            side = GROUP * 8

            def i_copy(u):
                return pltpu.make_async_copy(
                    e_out.at[part(yh, side), part(u % 4, GROUP), part(u // 4, side)], tin.at[u % 2], t_isem.at[u % 2])

            def o_copy(u):
                return pltpu.make_async_copy(
                    tout.at[u % 2], e_t.at[part(u // 4, side), part(u % 4, GROUP), part(yh, side)], t_osem.at[u % 2])

            i_copy(0).start()

            def unit(u):
                @pl.when(u < 11)
                def _():
                    i_copy(u + 1).start()
                i_copy(u).wait()

                def widen(i):
                    f_in[part(i, side)] = tin[u % 2, part(i, 8)].astype(F32).reshape(side, side)
                loop(GROUP, widen)

                def flip(i):
                    for v in range(4):
                        at = pl.ds(i * 4 + v, side, stride=GROUP)
                        f_out[at] = f_in[at].T
                loop(4, flip)

                @pl.when(u >= 2)
                def _():
                    o_copy(u).wait()

                def narrow(i):
                    tout[u % 2, part(i, 8)] = f_out[part(i, side)].astype(BF).reshape(8, GROUP, side)
                loop(GROUP, narrow)
                o_copy(u).start()
            loop(12, unit)
            o_copy(10).wait()
            o_copy(11).wait()

        pl.run_scoped(
            body, pltpu.VMEM((2, LANES, GROUP, LANES), BF), pltpu.VMEM((2, LANES, GROUP, LANES), BF),
            pltpu.VMEM((LANES * GROUP, LANES), F32), pltpu.VMEM((LANES * GROUP, LANES), F32))

    def xb_copy(src):
        ref = b_all.at[:, rblk(src), lane(core)]
        return remote(ref, ref, xb_ssem.at[src], xb_rsem.at[src], sib)

    def xb_wait(src):
        ref = b_all.at[:, rblk(src), lane(1 - core)]
        return remote(ref, ref, xb_ssem.at[src], xb_rsem.at[src], sib)

    def xa_copy(c):
        return remote(a_send.at[rblk(c, rows * HID)], a_all.at[rblk(c, rows * HID), lane(core)],
                      xa_ssem.at[c], xa_rsem.at[c], sib)

    def xa_wait(c):
        return remote(a_send.at[rblk(c, rows * HID)], a_all.at[rblk(c, rows * HID), lane(1 - core)],
                      xa_ssem.at[c], xa_rsem.at[c], sib)

    def block(k):
        src = partner(me, k)
        own_half = (src % 2 + core) % 2

        @pl.when(k == 0)
        def _():
            cp = pltpu.make_async_copy(xe.at[:, :, lane(me)], xb, lsem.at[0])
            cp.start()
            cp.wait()
            cp = pltpu.make_async_copy(xb, e_out.at[rblk(me)], lsem.at[0])
            cp.start()
            cp.wait()

        @pl.when(k > 0)
        def _():
            remote(xe.at[:, :, lane(src)], e_out.at[rblk(src)], e_ssem.at[k], e_rsem.at[k], src).wait_recv()
            cp = pltpu.make_async_copy(e_out.at[rblk(src)], xb, lsem.at[0])
            cp.start()
            cp.wait()

        def half(hh):
            r0 = pl.multiple_of(src * rows + hh * GROUP, GROUP)
            right, left = project(hh, mask_et[pl.ds(r0, GROUP), :])
            b_all[:, pl.ds(r0, GROUP), lane(core)] = right
            at = pl.ds(pl.multiple_of(((src // 2) * rows + hh * GROUP) * HID, GROUP * HID), GROUP * HID)

            @pl.when(own_half == 0)
            def _():
                a_all[at, lane(core)] = left

            @pl.when(own_half == 1)
            def _():
                a_send[at, :] = left
        loop(rows // GROUP, half)
        xb_copy(src).start()

        @pl.when(own_half == 1)
        def _():
            xa_copy(src // 2).start()

        @pl.when(k == 3)
        def _():
            transpose(me // 4)
    loop(8, block)

    for k in range(1, 8):
        e_copy(k).wait_send()


    def xwait(s):
        xb_wait(s).wait_recv()
    loop(8, xwait)

    def xwait_a(c):
        xa_wait(c).wait_recv()
    loop(4, xwait_a)

    def rs_copy(n):
        t, ib, k = ((0, 0, 2), (0, 1, 4), (1, 0, 2), (2, 1, 4), (2, 0, 4), (1, 1, 2))[n]
        at = pl.ds(ib * GROUP // 2, GROUP // 2)
        dst = rs_mid.at[ib] if t == 0 else rs_recv.at[t - 1, at]
        return remote(rt.at[t, at], dst, rs_ssem.at[n], rs_rsem.at[n], partner(me, k))

    def contract(o_s):
        def outer(left, right_of):
            def qstep(qq):
                for u in range(QSTEP):
                    q = qq * QSTEP + u
                    o = nt_dot(left(), right_of(q))
                    o_s[:, part(q, HID), :] = o.astype(BF).reshape(GROUP, HID, res)
            loop(HID // QSTEP, qstep)

        def eblk(n):
            t = ((n // 2 + 1) // 2) % 2 * (1 + (n // 2 + n + 1) % 2) + 3 * (n // 6)
            ib = n % 2
            c = partner(me, 2 * (1 - t // 2) + 4 * (1 - t % 2)) // 2
            at = pl.ds(pl.multiple_of((c * rows + ib * GROUP) * HID, GROUP * HID), GROUP * HID)
            outer(lambda: a_all[at, :], lambda q: b_all[q])

            hi0 = lax.broadcasted_iota(jnp.int32, (LANES, LANES), 0) * 0 + c // 2 == 0
            odd = lax.broadcasted_iota(jnp.int32, (LANES, LANES), 0) * 0 + c % 2 == 1

            def rstep(ii):
                for u in range(RSTEP // 2):
                    n2 = ii * (RSTEP // 2) + u
                    away, near = [], []
                    for v in range(2):
                        r = jnp.dot(wo_e[:], o_s[n2 * 2 + v], preferred_element_type=F32)
                        away.append(jnp.where(hi0, r[:, LANES:], r[:, :LANES]))
                        near.append(jnp.where(hi0, r[:, :LANES], r[:, LANES:]))
                    n0 = jnp.where(odd, near[0], pltpu.roll(near[0], HALF, 1))
                    n1 = jnp.where(odd, pltpu.roll(near[1], HALF, 1), near[1])
                    rt[t, ib * (GROUP // 2) + n2] = jnp.concatenate(
                        [away[0], away[1], jnp.where(lane_lo, n0, n1)], axis=1).astype(BF)
            loop(GROUP // RSTEP, rstep)

            for v in range(6):
                @pl.when(n == v)
                def _():
                    if v >= 4:
                        rs_copy(v - 4).wait_recv()

                        def add(i):
                            at = (t, ib * (GROUP // 2) + i)
                            rt[at] = (rt[at].astype(F32) + rs_mid[v - 4, i].astype(F32)).astype(BF)
                        loop(GROUP // 2, add)
                    rs_copy(v).start()
                    if v == 0:
                        for i in range(2):
                            g_wait(i + 1).wait_recv()
                            d_copy(i).start()
                            f_copy(i).start()
                    if v == 1:
                        for k in (3, 5, 6, 7):
                            m_copy(k).start()
        loop(8, eblk)

        for i in range(2):
            d_wait(i).wait_recv()
        f_copy(2).start()
        g_wait(0).wait_recv()
        for i in range(3):
            f_wait(i).wait_recv()

        def mblk(ib):
            at = part(ib, GROUP * HID)
            outer(lambda: am[at, :], lambda q: bm[q])

            def rstep(ii):
                for u in range(RSTEP):
                    i = ii * RSTEP + u
                    row = ib * GROUP + i
                    r = jnp.dot(wo_m[:], o_s[i], preferred_element_type=F32)
                    pair_out[row] = ((r + bo_m[:]) / (NORM_EPS + cnt_m[row])).T
            loop(GROUP // RSTEP, rstep)
        loop(rows // GROUP, mblk)

    pl.run_scoped(contract, pltpu.VMEM((GROUP, 1024, res), BF))
    transpose(1 - me // 4)

    def final(zb):
        def z_copy(j):
            return pltpu.make_async_copy(pair.at[part(j, 8)], zb.at[part(j, 8)], lsem.at[3 + j])

        steps = rows // 8
        for j in range(steps):
            z_copy(j).start()
        hi0 = lax.broadcasted_iota(jnp.int32, (LANES, LANES), 0) * 0 + chip // 2 == 0
        odd = lax.broadcasted_iota(jnp.int32, (LANES, LANES), 0) * 0 + chip % 2 == 1

        def row2(n):
            tot = rt[3, n].astype(F32) + rs_recv[0, n].astype(F32) + rs_recv[1, n].astype(F32)
            kept, own = tot[:, 256:], r_own[n]
            rkept, rown = pltpu.roll(kept, HALF, 1), pltpu.roll(own, HALF, 1)
            near0 = jnp.where(lane_lo, jnp.where(odd, kept, own), jnp.where(odd, rown, rkept))
            near1 = jnp.where(lane_lo, jnp.where(odd, rkept, rown), jnp.where(odd, own, kept))
            for v, near in ((0, near0), (1, near1)):
                away = tot[:, v * LANES:v * LANES + LANES]
                row = n * 2 + v
                r = jnp.concatenate([jnp.where(hi0, near, away), jnp.where(hi0, away, near)], axis=1)
                te = (r + bo_e[:]) / (NORM_EPS + cnt_e[row])
                pair_out[row] = (zb[row] + te.T) + pair_out[row]

        for j in range(steps):
            z_copy(j).wait()
        for h in range(2):
            for n in ((2, 4), (3, 5))[h]:
                rs_copy(n).wait_recv()
            loop(rows // 4, lambda i: row2(h * (rows // 4) + i))

    pl.run_scoped(final, pltpu.VMEM((rows, res, LANES), F32))

    for k in range(1, 8):
        m_copy(k).wait_send()
        to = partner(me, k)
        remote(xm.at[rblk(me, mseq)], m_out.at[:, rblk(to), :], m_ssem.at[k], m_rsem.at[k], to).wait_recv()

    def drain(s):
        xb_copy(s).wait_send()
    loop(8, drain)

    def drain_a(c):
        xa_copy(c).wait_send()
    loop(4, drain_a)
    for i in range(3):
        g_copy(i).wait_send()
    for i in range(2):
        d_copy(i).wait_send()
    for i in range(3):
        f_copy(i).wait_send()
    for n in range(6):
        rs_copy(n).wait_send()


def solution(mesh):
    msa_spec = P('data', 'dap', None)
    mask_spec = P('data', None)
    row_spec = P(('data', 'dap'), None, None)

    def local_program(extra_block, extra_mask, main_block, main_mask, pair_rows,
                      e_gam, e_bet, e_wl, e_bl, e_wr, e_br, e_wo, e_bo,
                      m_gam, m_bet, m_wl, m_bl, m_wr, m_br, m_wo, m_bo):
        seqs, rows, ce = extra_block.shape
        mseqs, _, cm = main_block.shape
        res = extra_mask.shape[1]
        hid = e_wl.shape[1]
        nk = e_wo.shape[1]
        seq = seqs // 8
        args = (
            jnp.transpose(extra_block, (1, 2, 0)), main_block, extra_mask, main_mask, pair_rows,
            e_gam, e_bet, e_wl.T, e_bl, e_wr.T, e_br, e_wo, e_bo, m_gam, m_bet, m_wl.T, m_bl, m_wr.T, m_br, m_wo, m_bo)
        any_spec = pl.BlockSpec(memory_space=pl.ANY)
        vmem = pl.BlockSpec(memory_space=pltpu.VMEM)
        dma = pltpu.SemaphoreType.DMA
        pair_out, e_seq, m_seq, _ = pl.pallas_call(
            opm_kernel,
            out_shape=(
                pltpu.VMEM((rows, res, nk), F32),
                jax.ShapeDtypeStruct((seq, ce, res), BF),
                jax.ShapeDtypeStruct((mseqs // 8, res, cm), BF),
                jax.ShapeDtypeStruct((res, ce, seq), BF)),
            in_specs=[any_spec, any_spec, any_spec, vmem, any_spec] + [vmem] * 16,
            out_specs=(vmem, any_spec, any_spec, any_spec),
            scratch_shapes=[
                pltpu.VMEM((4 * rows * hid, 2 * seq), BF),
                pltpu.VMEM((hid, res, 2 * seq), BF),
                pltpu.VMEM((4 * rows * hid, seq), BF),
                pltpu.VMEM((rows, ce, seq), BF),
                pltpu.VMEM((GROUP * ce, seq), BF),
                pltpu.VMEM((seq, res), jnp.int32),
                pltpu.VMEM((res, seq), F32),
                pltpu.VMEM((rows, 1, mseqs), F32),
                pltpu.VMEM((rows * hid, mseqs), BF),
                pltpu.VMEM((hid, res, mseqs), BF),
                pltpu.VMEM((4, rows // 2, nk, res // 2 * 3), BF),
                pltpu.VMEM((2, GROUP // 2, nk, res // 2 * 3), BF),
                pltpu.VMEM((2, rows // 2, nk, res // 2 * 3), BF),
                pltpu.VMEM((rows // 2, nk, res // 2), F32),
                pltpu.VMEM((hid * RG, ce * RG), BF),
                pltpu.VMEM((hid * LG, ce * LG), BF),
                pltpu.VMEM((2 * hid, cm), BF),
                pltpu.VMEM((nk, hid * hid), BF),
                pltpu.VMEM((nk, hid * hid), BF),
                pltpu.VMEM((ce, 1), F32),
                pltpu.VMEM((ce, 1), F32),
                pltpu.VMEM((hid * RG, 1), F32),
                pltpu.VMEM((hid, 1), F32),
                pltpu.VMEM((nk, 1), F32),
                pltpu.VMEM((2 * hid, 1), F32),
                pltpu.VMEM((nk, 1), F32),
                pltpu.VMEM((rows, 1, res), F32),
                pltpu.VMEM((rows, 1, res), F32),
                dma((8,)), dma((8,)), dma((8,)), dma((8,)), dma((4,)), dma((4,)), dma((8,)), dma((8,)),
                dma((2,)), dma((2,)), dma((2,)), dma((2,)),
                dma((3,)), dma((3,)), dma((3,)), dma((3,)), dma((6,)), dma((6,)),
                dma((8,)), dma((8,)), pltpu.SemaphoreType.REGULAR, dma((8,))],
            compiler_params=pltpu.CompilerParams(
                collective_id=0, has_side_effects=True, vmem_limit_bytes=VMEM_LIMIT),
            name='opm',
        )(*args)
        return pair_out, jnp.transpose(e_seq, (0, 2, 1)), m_seq

    in_specs = (msa_spec, mask_spec, msa_spec, mask_spec, row_spec) + (P(),) * 16
    return jax.shard_map(local_program, mesh=mesh, in_specs=in_specs, out_specs=(row_spec,) * 3, check_vma=False)
```

```python
import functools

import jax
import jax.numpy as jnp
from jax import lax
from jax.experimental import pallas as pl
from jax.experimental.pallas import tpu as pltpu
from jax.sharding import PartitionSpec as P

LN_EPS = 1e-5
NORM_EPS = 1e-3
BF = jnp.bfloat16
F32 = jnp.float32
GROUP = 16
VMEM_LIMIT = 55 * 2 ** 20
QSTEP = 4
LSTEP = 4
MSTEP = 8
RG, LG = 8, 4
HID, CE, LANES, HALF = 32, 64, 128, 64
RSTEP = 8


def loop(n, body):
    def step(i, carry):
        body(i)
        return carry
    lax.fori_loop(0, n, step, 0)


def part(i, n):
    return pl.ds(pl.multiple_of(i * n, n), n)


def partner(me, k):
    core, cx, cy = me % 2, (me // 2) % 2, me // 4
    k0, k1, k2 = k % 2, (k // 2) % 2, k // 4
    return (core + k0) % 2 + 2 * ((cx + k1) % 2) + 4 * ((cy + k2) % 2)


def nt_dot(lhs, rhs):
    return lax.dot_general(lhs, rhs, (((1,), (1,)), ((), ())), preferred_element_type=F32)


def column(row, n, repeat):
    m = row.shape[1]
    at = lax.broadcasted_iota(jnp.int32, (n, m), 0) // repeat
    return jnp.sum(jnp.where(at == lax.broadcasted_iota(jnp.int32, (n, m), 1), row, 0.0), axis=1, keepdims=True)


def opm_kernel(
    xe, xm, mask_e, mask_m, pair,
    e_gam, e_bet, e_wl, e_bl, e_wr, e_br, e_wo, e_bo,
    m_gam, m_bet, m_wl, m_bl, m_wr, m_br, m_wo, m_bo,
    pair_out, e_t, m_out, e_out,
    a_all, b_all, a_send, xb, y_s, mask_i, mask_et, mask_mo, am, bm, rt, rs_mid, rs_recv, r_own,
    w_right, w_left, w_m, wo_e, wo_m, gam_e, bet_e, bias_b, bias_a, bo_e, bias_m, bo_m, cnt_e, cnt_m,
    e_ssem, e_rsem, m_ssem, m_rsem, xa_ssem, xa_rsem, xb_ssem, xb_rsem,
    d_ssem, d_rsem, t_isem, t_osem, g_ssem, g_rsem, f_ssem, f_rsem, rs_ssem, rs_rsem, ob_ssem, ob_rsem, ob_free, lsem,
):
    me = lax.axis_index('dap')
    core = me % 2
    chip = me // 2
    sib = partner(me, 1)
    seq = e_out.shape[2]
    mseq = m_out.shape[0]
    rows = xe.shape[0]
    res = e_out.shape[0]

    def dev(d):
        return {'dap': d}

    def lane(h):
        return pl.ds(pl.multiple_of(h * seq, LANES), seq)

    def rblk(d, n=rows):
        return part(d, n)

    barrier = pltpu.get_barrier_semaphore()
    for k in range(1, 8):
        pl.semaphore_signal(barrier, inc=1, device_id=dev(partner(me, k)), device_id_type=pl.DeviceIdType.MESH)
    pl.semaphore_wait(barrier, 7)

    def remote(src, dst, ssem, rsem, target):
        return pltpu.make_async_remote_copy(
            src_ref=src, dst_ref=dst, send_sem=ssem, recv_sem=rsem,
            device_id=dev(target), device_id_type=pl.DeviceIdType.MESH)

    def e_copy(k):
        to = partner(me, k)
        return remote(xe.at[:, :, lane(to)], e_out.at[rblk(me)], e_ssem.at[k], e_rsem.at[k], to)

    for k in (1, 2, 4, 3, 5, 6, 7):
        e_copy(k).start()

    def m_copy(k):
        to = partner(me, k)
        return remote(xm.at[rblk(to, mseq)], m_out.at[:, rblk(me), :], m_ssem.at[k], m_rsem.at[k], to)

    def row_of(ref):
        v = ref[:].astype(F32)
        return v.reshape(1, v.shape[0])

    def weights(wf, wp):
        gam_e[:] = column(row_of(e_gam), HALF, 1)
        bet_e[:] = column(row_of(e_bet), HALF, 1)
        bias_b[:] = column(row_of(e_br), HID * RG, RG)
        bias_a[:] = column(row_of(e_bl), HID, 1)
        bo_e[:] = column(row_of(e_bo), LANES, 1)
        bo_m[:] = column(row_of(m_bo), LANES, 1)
        bias_m[:HID] = column(row_of(m_bl), HID, 1)
        bias_m[HID:] = column(row_of(m_br), HID, 1)
        w_m[:HID] = m_wl[:]
        w_m[HID:] = m_wr[:]

        def wide(ref, n):
            w = ref[:].astype(F32)
            return jnp.concatenate([w] * n, axis=1)

        def place(dst, rep, residue):
            at = lax.broadcasted_iota(jnp.int32, dst.shape, 0)
            dst[:] = jnp.where(residue(at) == lax.broadcasted_iota(jnp.int32, dst.shape, 1) // CE, rep, 0.0).astype(BF)

        w = wide(e_wr, RG)
        place(w_right, jnp.broadcast_to(w[:, None, :], (HID, RG, RG * CE)).reshape(HID * RG, RG * CE), lambda at: at % RG)
        place(w_left, jnp.concatenate([wide(e_wl, LG)] * LG, axis=0), lambda at: at // HID)
        for src, dst in ((e_wo, wo_e), (m_wo, wo_m)):
            wf[:] = src[:].astype(F32)

            def pick(q):
                wp[part(q, HID), :] = wf[pl.ds(q, HID, stride=HID), :]
            loop(HID, pick)
            dst[:] = wp[:].T.astype(BF)

    pl.run_scoped(weights, pltpu.VMEM((1024, LANES), F32), pltpu.VMEM((1024, LANES), F32))

    def masks(mt):
        mt[:] = mask_m[:].astype(F32).T
        own = mt[rblk(me), :]
        mask_mo[:] = own.reshape(rows, 1, mask_m.shape[0])
        cnt_m[:] = jnp.dot(own.astype(BF), mask_m[:].astype(F32).astype(BF),
                             preferred_element_type=F32).reshape(rows, 1, res)

    pl.run_scoped(masks, pltpu.VMEM((res, mask_m.shape[0]), F32))

    def load_mask(d):
        cp = pltpu.make_async_copy(mask_e.at[rblk(d, seq)], mask_i, lsem.at[0])
        cp.start()
        cp.wait()

    def main_proj(xc, xf, bf):
        cp = pltpu.make_async_copy(xm.at[rblk(me, mseq)], xc.at[pl.ds(0, mseq)], lsem.at[1])
        cp.start()
        cp.wait()
        m_out[:, rblk(me), :] = xc[pl.ds(0, mseq)]
        step = xc.shape[0]
        gam_m, bet_m = row_of(m_gam), row_of(m_bet)
        for piece in range(xm.shape[0] // step):
            cp = pltpu.make_async_copy(xm.at[pl.ds(piece * step, step)], xc, lsem.at[2])
            cp.start()
            cp.wait()

            def widen(i):
                s = part(i, 8)
                xf[s] = xc[s].astype(F32)
            loop(step // 8, widen)

            def one(r):
                x = xf[:, r, :]
                mean = jnp.mean(x, axis=1, keepdims=True)
                cen = x - mean
                var = jnp.mean(cen * cen, axis=1, keepdims=True)
                y = (cen * lax.rsqrt(var + LN_EPS) * gam_m + bet_m).astype(BF)
                proj = nt_dot(w_m[:], y) + bias_m[:]
                proj = proj * mask_mo[r, :, pl.ds(piece * step, step)]
                am[part(r, HID), pl.ds(piece * step, step)] = proj[:HID].astype(BF)
                bf[:, r, :] = proj[HID:]
            def some(i):
                for u in range(MSTEP):
                    one(i * MSTEP + u)

            loop(rows // MSTEP, some)
            bm[:, rblk(me), pl.ds(piece * step, step)] = bf[:].astype(BF)

    pl.run_scoped(
        main_proj, pltpu.VMEM((LANES, rows, xm.shape[2]), BF), pltpu.VMEM((LANES, rows, xm.shape[2]), F32),
        pltpu.VMEM((HID, rows, LANES), F32))

    def g_copy(i):
        ref = bm.at[:, rblk(me), :]
        return remote(ref, ref, g_ssem.at[i], g_rsem.at[i], partner(me, (1, 2, 4)[i]))

    def g_wait(i):
        to = partner(me, (1, 2, 4)[i])
        ref = bm.at[:, rblk(to), :]
        return remote(ref, ref, g_ssem.at[i], g_rsem.at[i], to)

    def d_copy(i):
        ref = bm.at[part(i, HID // 2), rblk(partner(me, (2, 4)[i])), :]
        return remote(ref, ref, d_ssem.at[i], d_rsem.at[i], partner(me, (4, 2)[i]))

    def d_wait(i):
        ref = bm.at[part(i, HID // 2), rblk(partner(me, 6)), :]
        return remote(ref, ref, d_ssem.at[i], d_rsem.at[i], partner(me, (4, 2)[i]))

    def f_copy(i):
        ref = bm.at[:, rblk(partner(me, (2, 4, 6)[i])), :]
        return remote(ref, ref, f_ssem.at[i], f_rsem.at[i], sib)

    def f_wait(i):
        ref = bm.at[:, rblk(partner(me, (3, 5, 7)[i])), :]
        return remote(ref, ref, f_ssem.at[i], f_rsem.at[i], sib)

    for i in range(3):
        g_copy(i).start()
    for k in (1, 2, 4):
        m_copy(k).start()

    def project(hh, m16):
        def norm(i):
            for u in range(LSTEP):
                r = i * LSTEP + u
                x = xb[hh * GROUP + r].astype(F32)
                mean = jnp.mean(x, axis=0, keepdims=True)
                cen = x - mean
                var = jnp.mean(cen * cen, axis=0, keepdims=True)
                y = cen * lax.rsqrt(var + LN_EPS) * gam_e[:] + bet_e[:]
                y_s[part(r, CE), :] = y.astype(BF)
        loop(GROUP // LSTEP, norm)

        def dot(w, g):
            return jnp.dot(w[:], y_s[pl.ds(g * w.shape[1], w.shape[1])], preferred_element_type=F32)

        right = jnp.concatenate(
            [(dot(w_right, g) + bias_b[:]).reshape(HID, RG, seq) for g in range(GROUP // RG)], axis=1)
        right = (right * m16[None]).astype(BF)
        left = []
        for g in range(GROUP // LG):
            d = dot(w_left, g)
            for r in range(LG):
                left.append((d[r * HID:r * HID + HID] + bias_a[:]) * m16[g * LG + r:g * LG + r + 1])
        left = jnp.concatenate(left, axis=0).astype(BF)
        return right, left

    lane_lo = lax.broadcasted_iota(jnp.int32, (LANES, LANES), 1) < HALF

    def ob_copy(d, e, h):
        ref = rt.at[d % 4, :, pl.ds(pl.multiple_of(e * HALF + h * rows, rows), rows), :]
        return remote(ref, ref, ob_ssem.at[d % 4 * 2 + e], ob_rsem.at[d % 4 * 2 + e], sib)

    def own_pairs(mt, cnt, a_own, acc, o_pair):
        cnt[:] = jnp.zeros_like(cnt)

        def zero(g):
            acc[g] = jnp.zeros(acc.shape[1:], F32)
        loop(acc.shape[0], zero)

        def chunk(d):
            xcp = pltpu.make_async_copy(xe.at[:, :, lane(d)], xb, lsem.at[1])
            xcp.start()
            load_mask(d)
            m = mask_i[:].astype(F32)
            mt[:] = m.T
            cnt[:] += jnp.dot(mt[rblk(me), :].astype(BF), m.astype(BF), preferred_element_type=F32)

            @pl.when(d >= 4)
            def _():
                for e in range(2):
                    ob_copy(d, e, core).wait_send()
            xcp.wait()

            def half(hh):
                right, left = project(hh, mt[pl.ds(pl.multiple_of(me * rows + hh * GROUP, GROUP), GROUP), :])
                right = right.reshape(16, 2, GROUP, seq)
                for e in range(2):
                    at = pl.ds(pl.multiple_of(e * HALF + core * rows + hh * GROUP, GROUP), GROUP)
                    rt[d % 4, :, at, :] = right[:, e]
                a_own[d % 2, part(hh, GROUP * HID), :] = left
            loop(rows // GROUP, half)

            @pl.when((d // 4) * ((d + 1) % 2) == 1)
            def _():
                pl.semaphore_wait(ob_free, 1)
            for e in range(2):
                ob_copy(d, e, core).start()

            @pl.when(d % 2 == 1)
            def _():
                for e in range(2):
                    ob_copy(d - 1, e, 1 - core).wait_recv()
                    ob_copy(d, e, 1 - core).wait_recv()

                def group(g):
                    at = part(g, 2)
                    acc[g] += (nt_dot(a_own[0], rt[(d - 1) % 4, at].reshape(256, seq))
                               + nt_dot(a_own[1], rt[d % 4, at].reshape(256, seq)))
                loop(acc.shape[0], group)

                @pl.when(d < 4)
                def _():
                    pl.semaphore_signal(ob_free, inc=1, device_id=dev(sib), device_id_type=pl.DeviceIdType.MESH)
        loop(8, chunk)
        cnt_e[:] = cnt[:].reshape(rows, 1, res)

        def pair_rows(n):
            for g in range(8):
                t = acc[g, part(n, HALF), :]
                for b in range(2):
                    u0, u1 = t[:HID, b * LANES:b * LANES + LANES], t[HID:, b * LANES:b * LANES + LANES]
                    q = g * 4 + b * 2
                    lo = lane_lo[:HID]
                    o_pair[q * HID:q * HID + HID, :] = jnp.where(lo, u0, pltpu.roll(u1, HALF, 1)).astype(BF)
                    o_pair[q * HID + HID:q * HID + HALF, :] = jnp.where(lo, pltpu.roll(u0, HALF, 1), u1).astype(BF)
            r_own[n] = jnp.dot(wo_e[:], o_pair[:], preferred_element_type=F32)
        loop(rows // 2, pair_rows)
        for d in range(4, 8):
            for e in range(2):
                ob_copy(d, e, core).wait_send()
        load_mask(me)
        mask_et[:] = mask_i[:].astype(F32).T

    pl.run_scoped(
        own_pairs, pltpu.VMEM((res, seq), F32), pltpu.VMEM((rows, res), F32),
        pltpu.VMEM((2, rows * HID, seq), BF), pltpu.VMEM((8, rows * HID, 256), F32), pltpu.VMEM((1024, LANES), BF))

    def transpose(yh):
        def body(tin, tout, f_in, f_out):
            side = GROUP * 8

            def i_copy(u):
                return pltpu.make_async_copy(
                    e_out.at[part(yh, side), part(u % 4, GROUP), part(u // 4, side)], tin.at[u % 2], t_isem.at[u % 2])

            def o_copy(u):
                return pltpu.make_async_copy(
                    tout.at[u % 2], e_t.at[part(u // 4, side), part(u % 4, GROUP), part(yh, side)], t_osem.at[u % 2])

            i_copy(0).start()

            def unit(u):
                @pl.when(u < 11)
                def _():
                    i_copy(u + 1).start()
                i_copy(u).wait()

                def widen(i):
                    f_in[part(i, side)] = tin[u % 2, part(i, 8)].astype(F32).reshape(side, side)
                loop(GROUP, widen)

                def flip(i):
                    for v in range(4):
                        at = pl.ds(i * 4 + v, side, stride=GROUP)
                        f_out[at] = f_in[at].T
                loop(4, flip)

                @pl.when(u >= 2)
                def _():
                    o_copy(u).wait()

                def narrow(i):
                    tout[u % 2, part(i, 8)] = f_out[part(i, side)].astype(BF).reshape(8, GROUP, side)
                loop(GROUP, narrow)
                o_copy(u).start()
            loop(12, unit)
            o_copy(10).wait()
            o_copy(11).wait()

        pl.run_scoped(
            body, pltpu.VMEM((2, LANES, GROUP, LANES), BF), pltpu.VMEM((2, LANES, GROUP, LANES), BF),
            pltpu.VMEM((LANES * GROUP, LANES), F32), pltpu.VMEM((LANES * GROUP, LANES), F32))

    def xb_copy(src):
        ref = b_all.at[:, rblk(src), lane(core)]
        return remote(ref, ref, xb_ssem.at[src], xb_rsem.at[src], sib)

    def xb_wait(src):
        ref = b_all.at[:, rblk(src), lane(1 - core)]
        return remote(ref, ref, xb_ssem.at[src], xb_rsem.at[src], sib)

    def xa_copy(c):
        return remote(a_send.at[rblk(c, rows * HID)], a_all.at[rblk(c, rows * HID), lane(core)],
                      xa_ssem.at[c], xa_rsem.at[c], sib)

    def xa_wait(c):
        return remote(a_send.at[rblk(c, rows * HID)], a_all.at[rblk(c, rows * HID), lane(1 - core)],
                      xa_ssem.at[c], xa_rsem.at[c], sib)

    def block(k):
        src = partner(me, k)
        own_half = (src % 2 + core) % 2

        @pl.when(k == 0)
        def _():
            cp = pltpu.make_async_copy(xe.at[:, :, lane(me)], xb, lsem.at[0])
            cp.start()
            cp.wait()
            cp = pltpu.make_async_copy(xb, e_out.at[rblk(me)], lsem.at[0])
            cp.start()
            cp.wait()

        @pl.when(k > 0)
        def _():
            remote(xe.at[:, :, lane(src)], e_out.at[rblk(src)], e_ssem.at[k], e_rsem.at[k], src).wait_recv()
            cp = pltpu.make_async_copy(e_out.at[rblk(src)], xb, lsem.at[0])
            cp.start()
            cp.wait()

        def half(hh):
            r0 = pl.multiple_of(src * rows + hh * GROUP, GROUP)
            right, left = project(hh, mask_et[pl.ds(r0, GROUP), :])
            b_all[:, pl.ds(r0, GROUP), lane(core)] = right
            at = pl.ds(pl.multiple_of(((src // 2) * rows + hh * GROUP) * HID, GROUP * HID), GROUP * HID)

            @pl.when(own_half == 0)
            def _():
                a_all[at, lane(core)] = left

            @pl.when(own_half == 1)
            def _():
                a_send[at, :] = left
        loop(rows // GROUP, half)
        xb_copy(src).start()

        @pl.when(own_half == 1)
        def _():
            xa_copy(src // 2).start()

        @pl.when(k == 3)
        def _():
            transpose(me // 4)
    loop(8, block)

    for k in range(1, 8):
        e_copy(k).wait_send()


    def xwait(s):
        xb_wait(s).wait_recv()
    loop(8, xwait)

    def xwait_a(c):
        xa_wait(c).wait_recv()
    loop(4, xwait_a)

    def rs_copy(n):
        t, ib, k = ((0, 0, 2), (0, 1, 4), (1, 0, 2), (2, 1, 4), (2, 0, 4), (1, 1, 2))[n]
        at = pl.ds(ib * GROUP // 2, GROUP // 2)
        dst = rs_mid.at[ib] if t == 0 else rs_recv.at[t - 1, at]
        return remote(rt.at[t, at], dst, rs_ssem.at[n], rs_rsem.at[n], partner(me, k))

    def contract_extra(o_s):
        pairs = GROUP // 2
        low = lax.broadcasted_iota(jnp.int32, (pairs * HID, LANES), 1) < HALF

        def eblk(n):
            t = ((n // 2 + 1) // 2) % 2 * (1 + (n // 2 + n + 1) % 2) + 3 * (n // 6)
            ib = n % 2
            c = partner(me, 2 * (1 - t // 2) + 4 * (1 - t % 2)) // 2
            at = pl.ds(pl.multiple_of((c * rows + ib * GROUP) * HID, GROUP * HID), GROUP * HID)
            away_at = part(1 - c // 2, LANES)
            near_at = part(c // 2 * 2 + 1 - c % 2, HALF)

            def qstep(qq):
                for h in range(2):
                    q = qq * QSTEP + h * 2
                    o = nt_dot(a_all[at, :], b_all[pl.ds(q, 2), away_at, :].reshape(256, 2 * seq))
                    o = o.astype(BF).reshape(pairs, 2, HID, 256)
                    for v in range(2):
                        for x in range(2):
                            o_s[:, part(q + x, HID), pl.ds(v * LANES, LANES)] = o[:, v, :, x * LANES:x * LANES + LANES]
                q = qq * QSTEP
                o = nt_dot(a_all[at, :], b_all[pl.ds(q, QSTEP), near_at, :].reshape(256, 2 * seq))
                o = o.reshape(pairs, 2, HID, 256)
                for x in range(2):
                    u0, u1 = (o[:, v, :, x * LANES:x * LANES + LANES].reshape(pairs * HID, LANES) for v in range(2))
                    for y, near in ((0, jnp.where(low, u0, pltpu.roll(u1, HALF, 1))),
                                    (1, jnp.where(low, pltpu.roll(u0, HALF, 1), u1))):
                        o_s[:, part(q + x * 2 + y, HID), pl.ds(2 * LANES, LANES)] = near.astype(BF).reshape(pairs, HID, LANES)
            loop(HID // QSTEP, qstep)

            def rstep(ii):
                for u in range(RSTEP // 2):
                    i = ii * (RSTEP // 2) + u
                    rt[t, ib * pairs + i] = jnp.dot(wo_e[:], o_s[i], preferred_element_type=F32).astype(BF)
            loop(GROUP // RSTEP, rstep)

            for v in range(6):
                @pl.when(n == v)
                def _():
                    if v >= 4:
                        rs_copy(v - 4).wait_recv()

                        def add(i):
                            at = (t, ib * (GROUP // 2) + i)
                            rt[at] = (rt[at].astype(F32) + rs_mid[v - 4, i].astype(F32)).astype(BF)
                        loop(GROUP // 2, add)
                    rs_copy(v).start()
                    if v == 0:
                        for i in range(2):
                            g_wait(i + 1).wait_recv()
                            d_copy(i).start()
                            f_copy(i).start()
                    if v == 1:
                        for k in (3, 5, 6, 7):
                            m_copy(k).start()
        loop(8, eblk)

        for i in range(2):
            d_wait(i).wait_recv()
        f_copy(2).start()
        g_wait(0).wait_recv()
        for i in range(3):
            f_wait(i).wait_recv()

    def contract_main(o_s):
        def mblk(ib):
            at = part(ib, GROUP * HID)

            def qstep(qq):
                for u in range(QSTEP):
                    q = qq * QSTEP + u
                    o_s[:, part(q, HID), :] = nt_dot(am[at, :], bm[q]).astype(BF).reshape(GROUP, HID, res)
            loop(HID // QSTEP, qstep)

            def rstep(ii):
                for u in range(RSTEP):
                    i = ii * RSTEP + u
                    row = ib * GROUP + i
                    r = jnp.dot(wo_m[:], o_s[i], preferred_element_type=F32)
                    pair_out[row] = ((r + bo_m[:]) / (NORM_EPS + cnt_m[row])).T
            loop(GROUP // RSTEP, rstep)
        loop(rows // GROUP, mblk)

    pl.run_scoped(contract_extra, pltpu.VMEM((GROUP // 2, 1024, 3 * LANES), BF))
    pl.run_scoped(contract_main, pltpu.VMEM((GROUP, 1024, res), BF))
    transpose(1 - me // 4)

    def final(zb):
        def z_copy(j):
            return pltpu.make_async_copy(pair.at[part(j, 8)], zb.at[part(j, 8)], lsem.at[3 + j])

        steps = rows // 8
        for j in range(steps):
            z_copy(j).start()
        hi0 = lax.broadcasted_iota(jnp.int32, (LANES, LANES), 0) * 0 + chip // 2 == 0
        odd = lax.broadcasted_iota(jnp.int32, (LANES, LANES), 0) * 0 + chip % 2 == 1

        def row2(n):
            tot = rt[3, n].astype(F32) + rs_recv[0, n].astype(F32) + rs_recv[1, n].astype(F32)
            kept, own = tot[:, 256:], r_own[n]
            rkept, rown = pltpu.roll(kept, HALF, 1), pltpu.roll(own, HALF, 1)
            near0 = jnp.where(lane_lo, jnp.where(odd, kept, own), jnp.where(odd, rown, rkept))
            near1 = jnp.where(lane_lo, jnp.where(odd, rkept, rown), jnp.where(odd, own, kept))
            for v, near in ((0, near0), (1, near1)):
                away = tot[:, v * LANES:v * LANES + LANES]
                row = n * 2 + v
                r = jnp.concatenate([jnp.where(hi0, near, away), jnp.where(hi0, away, near)], axis=1)
                te = (r + bo_e[:]) / (NORM_EPS + cnt_e[row])
                pair_out[row] = (zb[row] + te.T) + pair_out[row]

        for j in range(steps):
            z_copy(j).wait()
        for h in range(2):
            for n in ((2, 4), (3, 5))[h]:
                rs_copy(n).wait_recv()
            loop(rows // 4, lambda i: row2(h * (rows // 4) + i))

    pl.run_scoped(final, pltpu.VMEM((rows, res, LANES), F32))

    for k in range(1, 8):
        m_copy(k).wait_send()
        to = partner(me, k)
        remote(xm.at[rblk(me, mseq)], m_out.at[:, rblk(to), :], m_ssem.at[k], m_rsem.at[k], to).wait_recv()

    def drain(s):
        xb_copy(s).wait_send()
    loop(8, drain)

    def drain_a(c):
        xa_copy(c).wait_send()
    loop(4, drain_a)
    for i in range(3):
        g_copy(i).wait_send()
    for i in range(2):
        d_copy(i).wait_send()
    for i in range(3):
        f_copy(i).wait_send()
    for n in range(6):
        rs_copy(n).wait_send()


def solution(mesh):
    msa_spec = P('data', 'dap', None)
    mask_spec = P('data', None)
    row_spec = P(('data', 'dap'), None, None)

    def local_program(extra_block, extra_mask, main_block, main_mask, pair_rows,
                      e_gam, e_bet, e_wl, e_bl, e_wr, e_br, e_wo, e_bo,
                      m_gam, m_bet, m_wl, m_bl, m_wr, m_br, m_wo, m_bo):
        seqs, rows, ce = extra_block.shape
        mseqs, _, cm = main_block.shape
        res = extra_mask.shape[1]
        hid = e_wl.shape[1]
        nk = e_wo.shape[1]
        seq = seqs // 8
        args = (
            jnp.transpose(extra_block, (1, 2, 0)), main_block, extra_mask, main_mask, pair_rows,
            e_gam, e_bet, e_wl.T, e_bl, e_wr.T, e_br, e_wo, e_bo, m_gam, m_bet, m_wl.T, m_bl, m_wr.T, m_br, m_wo, m_bo)
        any_spec = pl.BlockSpec(memory_space=pl.ANY)
        vmem = pl.BlockSpec(memory_space=pltpu.VMEM)
        dma = pltpu.SemaphoreType.DMA
        pair_out, e_seq, m_seq, _ = pl.pallas_call(
            opm_kernel,
            out_shape=(
                pltpu.VMEM((rows, res, nk), F32),
                jax.ShapeDtypeStruct((seq, ce, res), BF),
                pltpu.VMEM((mseqs // 8, res, cm), BF),
                jax.ShapeDtypeStruct((res, ce, seq), BF)),
            in_specs=[any_spec, any_spec, any_spec, vmem, any_spec] + [vmem] * 16,
            out_specs=(vmem, any_spec, vmem, any_spec),
            scratch_shapes=[
                pltpu.VMEM((4 * rows * hid, 2 * seq), BF),
                pltpu.VMEM((hid, res, 2 * seq), BF),
                pltpu.VMEM((4 * rows * hid, seq), BF),
                pltpu.VMEM((rows, ce, seq), BF),
                pltpu.VMEM((GROUP * ce, seq), BF),
                pltpu.VMEM((seq, res), jnp.int32),
                pltpu.VMEM((res, seq), F32),
                pltpu.VMEM((rows, 1, mseqs), F32),
                pltpu.VMEM((rows * hid, mseqs), BF),
                pltpu.VMEM((hid, res, mseqs), BF),
                pltpu.VMEM((4, rows // 2, nk, res // 2 * 3), BF),
                pltpu.VMEM((2, GROUP // 2, nk, res // 2 * 3), BF),
                pltpu.VMEM((2, rows // 2, nk, res // 2 * 3), BF),
                pltpu.VMEM((rows // 2, nk, res // 2), F32),
                pltpu.VMEM((hid * RG, ce * RG), BF),
                pltpu.VMEM((hid * LG, ce * LG), BF),
                pltpu.VMEM((2 * hid, cm), BF),
                pltpu.VMEM((nk, hid * hid), BF),
                pltpu.VMEM((nk, hid * hid), BF),
                pltpu.VMEM((ce, 1), F32),
                pltpu.VMEM((ce, 1), F32),
                pltpu.VMEM((hid * RG, 1), F32),
                pltpu.VMEM((hid, 1), F32),
                pltpu.VMEM((nk, 1), F32),
                pltpu.VMEM((2 * hid, 1), F32),
                pltpu.VMEM((nk, 1), F32),
                pltpu.VMEM((rows, 1, res), F32),
                pltpu.VMEM((rows, 1, res), F32),
                dma((8,)), dma((8,)), dma((8,)), dma((8,)), dma((4,)), dma((4,)), dma((8,)), dma((8,)),
                dma((2,)), dma((2,)), dma((2,)), dma((2,)),
                dma((3,)), dma((3,)), dma((3,)), dma((3,)), dma((6,)), dma((6,)),
                dma((8,)), dma((8,)), pltpu.SemaphoreType.REGULAR, dma((8,))],
            compiler_params=pltpu.CompilerParams(
                collective_id=0, has_side_effects=True, vmem_limit_bytes=VMEM_LIMIT),
            name='opm',
        )(*args)
        return pair_out, jnp.transpose(e_seq, (0, 2, 1)), m_seq

    in_specs = (msa_spec, mask_spec, msa_spec, mask_spec, row_spec) + (P(),) * 16
    return jax.shard_map(local_program, mesh=mesh, in_specs=in_specs, out_specs=(row_spec,) * 3, check_vma=False)
```

```python
import functools

import jax
import jax.numpy as jnp
from jax import lax
from jax.experimental import pallas as pl
from jax.experimental.pallas import tpu as pltpu
from jax.sharding import PartitionSpec as P

LN_EPS = 1e-5
NORM_EPS = 1e-3
BF = jnp.bfloat16
F32 = jnp.float32
GROUP = 16
VMEM_LIMIT = 43 * 2 ** 20
QSTEP = 4
LSTEP = 4
MSTEP = 8
RG, LG = 8, 4
HID, CE, LANES, HALF = 32, 64, 128, 64
RSTEP = 8


def loop(n, body):
    def step(i, carry):
        body(i)
        return carry
    lax.fori_loop(0, n, step, 0)


def part(i, n):
    return pl.ds(pl.multiple_of(i * n, n), n)


def partner(me, k):
    core, cx, cy = me % 2, (me // 2) % 2, me // 4
    k0, k1, k2 = k % 2, (k // 2) % 2, k // 4
    return (core + k0) % 2 + 2 * ((cx + k1) % 2) + 4 * ((cy + k2) % 2)


def nt_dot(lhs, rhs):
    return lax.dot_general(lhs, rhs, (((1,), (1,)), ((), ())), preferred_element_type=F32)


def column(row, n, repeat):
    m = row.shape[1]
    at = lax.broadcasted_iota(jnp.int32, (n, m), 0) // repeat
    return jnp.sum(jnp.where(at == lax.broadcasted_iota(jnp.int32, (n, m), 1), row, 0.0), axis=1, keepdims=True)


def opm_kernel(
    xe, xm, mask_e, mask_m, pair,
    e_gam, e_bet, e_wl, e_bl, e_wr, e_br, e_wo, e_bo,
    m_gam, m_bet, m_wl, m_bl, m_wr, m_br, m_wo, m_bo,
    pair_out, e_t, m_out, e_out,
    a_all, a_send, xb, y_s, mask_i, mask_et, mask_mo, am, bm, rt, rs_mid, rs_recv, r_own,
    w_right, w_left, w_m, wo_e, wo_m, gam_e, bet_e, bias_b, bias_a, bo_e, bias_m, bo_m, cnt_e, cnt_m,
    e_ssem, e_rsem, m_ssem, m_rsem, xa_ssem, xa_rsem, xb_ssem, xb_rsem,
    d_ssem, d_rsem, t_isem, g_ssem, g_rsem, f_ssem, f_rsem, rs_ssem, rs_rsem, ob_ssem, ob_rsem, ob_free, lsem,
):
    me = lax.axis_index('dap')
    core = me % 2
    chip = me // 2
    sib = partner(me, 1)
    seq = e_out.shape[2]
    mseq = m_out.shape[0]
    rows = xe.shape[0]
    res = e_out.shape[0]

    def dev(d):
        return {'dap': d}

    def lane(h):
        return pl.ds(pl.multiple_of(h * seq, LANES), seq)

    def rblk(d, n=rows):
        return part(d, n)

    barrier = pltpu.get_barrier_semaphore()
    for k in range(1, 8):
        pl.semaphore_signal(barrier, inc=1, device_id=dev(partner(me, k)), device_id_type=pl.DeviceIdType.MESH)
    pl.semaphore_wait(barrier, 7)

    def remote(src, dst, ssem, rsem, target):
        return pltpu.make_async_remote_copy(
            src_ref=src, dst_ref=dst, send_sem=ssem, recv_sem=rsem,
            device_id=dev(target), device_id_type=pl.DeviceIdType.MESH)

    def e_copy(k):
        to = partner(me, k)
        return remote(xe.at[:, :, lane(to)], e_out.at[rblk(me)], e_ssem.at[k], e_rsem.at[k], to)

    for k in (1, 2, 4, 3, 5, 6, 7):
        e_copy(k).start()

    def m_copy(k):
        to = partner(me, k)
        return remote(xm.at[rblk(to, mseq)], m_out.at[:, rblk(me), :], m_ssem.at[k], m_rsem.at[k], to)

    def row_of(ref):
        v = ref[:].astype(F32)
        return v.reshape(1, v.shape[0])

    def weights(wf, wp):
        gam_e[:] = column(row_of(e_gam), HALF, 1)
        bet_e[:] = column(row_of(e_bet), HALF, 1)
        bias_b[:] = column(row_of(e_br), HID * RG, RG)
        bias_a[:] = column(row_of(e_bl), HID, 1)
        bo_e[:] = column(row_of(e_bo), LANES, 1)
        bo_m[:] = column(row_of(m_bo), LANES, 1)
        bias_m[:HID] = column(row_of(m_bl), HID, 1)
        bias_m[HID:] = column(row_of(m_br), HID, 1)
        w_m[:HID] = m_wl[:]
        w_m[HID:] = m_wr[:]

        def wide(ref, n):
            w = ref[:].astype(F32)
            return jnp.concatenate([w] * n, axis=1)

        def place(dst, rep, residue):
            at = lax.broadcasted_iota(jnp.int32, dst.shape, 0)
            dst[:] = jnp.where(residue(at) == lax.broadcasted_iota(jnp.int32, dst.shape, 1) // CE, rep, 0.0).astype(BF)

        w = wide(e_wr, RG)
        place(w_right, jnp.broadcast_to(w[:, None, :], (HID, RG, RG * CE)).reshape(HID * RG, RG * CE), lambda at: at % RG)
        place(w_left, jnp.concatenate([wide(e_wl, LG)] * LG, axis=0), lambda at: at // HID)
        for src, dst in ((e_wo, wo_e), (m_wo, wo_m)):
            wf[:] = src[:].astype(F32)

            def pick(q):
                wp[part(q, HID), :] = wf[pl.ds(q, HID, stride=HID), :]
            loop(HID, pick)
            dst[:] = wp[:].T.astype(BF)

    pl.run_scoped(weights, pltpu.VMEM((1024, LANES), F32), pltpu.VMEM((1024, LANES), F32))

    def masks(mt):
        mt[:] = mask_m[:].astype(F32).T
        own = mt[rblk(me), :]
        mask_mo[:] = own.reshape(rows, 1, mask_m.shape[0])
        cnt_m[:] = jnp.dot(own.astype(BF), mask_m[:].astype(F32).astype(BF),
                             preferred_element_type=F32).reshape(rows, 1, res)

    pl.run_scoped(masks, pltpu.VMEM((res, mask_m.shape[0]), F32))

    def load_mask(d):
        cp = pltpu.make_async_copy(mask_e.at[rblk(d, seq)], mask_i, lsem.at[0])
        cp.start()
        cp.wait()

    def main_proj(xc, xf, bf):
        cp = pltpu.make_async_copy(xm.at[rblk(me, mseq)], xc.at[pl.ds(0, mseq)], lsem.at[1])
        cp.start()
        cp.wait()
        m_out[:, rblk(me), :] = xc[pl.ds(0, mseq)]
        step = xc.shape[0]
        gam_m, bet_m = row_of(m_gam), row_of(m_bet)
        for piece in range(xm.shape[0] // step):
            cp = pltpu.make_async_copy(xm.at[pl.ds(piece * step, step)], xc, lsem.at[2])
            cp.start()
            cp.wait()

            def widen(i):
                s = part(i, 8)
                xf[s] = xc[s].astype(F32)
            loop(step // 8, widen)

            def one(r):
                x = xf[:, r, :]
                mean = jnp.mean(x, axis=1, keepdims=True)
                cen = x - mean
                var = jnp.mean(cen * cen, axis=1, keepdims=True)
                y = (cen * lax.rsqrt(var + LN_EPS) * gam_m + bet_m).astype(BF)
                proj = nt_dot(w_m[:], y) + bias_m[:]
                proj = proj * mask_mo[r, :, pl.ds(piece * step, step)]
                am[part(r, HID), pl.ds(piece * step, step)] = proj[:HID].astype(BF)
                bf[:, r, :] = proj[HID:]
            def some(i):
                for u in range(MSTEP):
                    one(i * MSTEP + u)

            loop(rows // MSTEP, some)
            bm[:, rblk(me), pl.ds(piece * step, step)] = bf[:].astype(BF)

    pl.run_scoped(
        main_proj, pltpu.VMEM((LANES, rows, xm.shape[2]), BF), pltpu.VMEM((LANES, rows, xm.shape[2]), F32),
        pltpu.VMEM((HID, rows, LANES), F32))

    def g_copy(i):
        ref = bm.at[:, rblk(me), :]
        return remote(ref, ref, g_ssem.at[i], g_rsem.at[i], partner(me, (1, 2, 4)[i]))

    def g_wait(i):
        to = partner(me, (1, 2, 4)[i])
        ref = bm.at[:, rblk(to), :]
        return remote(ref, ref, g_ssem.at[i], g_rsem.at[i], to)

    def d_copy(i):
        ref = bm.at[part(i, HID // 2), rblk(partner(me, (2, 4)[i])), :]
        return remote(ref, ref, d_ssem.at[i], d_rsem.at[i], partner(me, (4, 2)[i]))

    def d_wait(i):
        ref = bm.at[part(i, HID // 2), rblk(partner(me, 6)), :]
        return remote(ref, ref, d_ssem.at[i], d_rsem.at[i], partner(me, (4, 2)[i]))

    def f_copy(i):
        ref = bm.at[:, rblk(partner(me, (2, 4, 6)[i])), :]
        return remote(ref, ref, f_ssem.at[i], f_rsem.at[i], sib)

    def f_wait(i):
        ref = bm.at[:, rblk(partner(me, (3, 5, 7)[i])), :]
        return remote(ref, ref, f_ssem.at[i], f_rsem.at[i], sib)

    for i in range(3):
        g_copy(i).start()
    for k in (1, 2, 4):
        m_copy(k).start()

    def project(hh, m16):
        def norm(i):
            for u in range(LSTEP):
                r = i * LSTEP + u
                x = xb[hh * GROUP + r].astype(F32)
                mean = jnp.mean(x, axis=0, keepdims=True)
                cen = x - mean
                var = jnp.mean(cen * cen, axis=0, keepdims=True)
                y = cen * lax.rsqrt(var + LN_EPS) * gam_e[:] + bet_e[:]
                y_s[part(r, CE), :] = y.astype(BF)
        loop(GROUP // LSTEP, norm)

        def dot(w, g):
            return jnp.dot(w[:], y_s[pl.ds(g * w.shape[1], w.shape[1])], preferred_element_type=F32)

        right = jnp.concatenate(
            [(dot(w_right, g) + bias_b[:]).reshape(HID, RG, seq) for g in range(GROUP // RG)], axis=1)
        right = (right * m16[None]).astype(BF)
        left = []
        for g in range(GROUP // LG):
            d = dot(w_left, g)
            for r in range(LG):
                left.append((d[r * HID:r * HID + HID] + bias_a[:]) * m16[g * LG + r:g * LG + r + 1])
        left = jnp.concatenate(left, axis=0).astype(BF)
        return right, left

    lane_lo = lax.broadcasted_iota(jnp.int32, (LANES, LANES), 1) < HALF

    def ob_copy(d, e, h):
        ref = rt.at[d % 4, :, pl.ds(pl.multiple_of(e * HALF + h * rows, rows), rows), :]
        return remote(ref, ref, ob_ssem.at[d % 4 * 2 + e], ob_rsem.at[d % 4 * 2 + e], sib)

    def own_pairs(mt, cnt, a_own, acc, o_pair):
        cnt[:] = jnp.zeros_like(cnt)

        def zero(g):
            acc[g] = jnp.zeros(acc.shape[1:], F32)
        loop(acc.shape[0], zero)

        def chunk(d):
            xcp = pltpu.make_async_copy(xe.at[:, :, lane(d)], xb, lsem.at[1])
            xcp.start()
            load_mask(d)
            m = mask_i[:].astype(F32)
            mt[:] = m.T
            cnt[:] += jnp.dot(mt[rblk(me), :].astype(BF), m.astype(BF), preferred_element_type=F32)

            @pl.when(d >= 4)
            def _():
                for e in range(2):
                    ob_copy(d, e, core).wait_send()
            xcp.wait()

            def half(hh):
                right, left = project(hh, mt[pl.ds(pl.multiple_of(me * rows + hh * GROUP, GROUP), GROUP), :])
                right = right.reshape(16, 2, GROUP, seq)
                for e in range(2):
                    at = pl.ds(pl.multiple_of(e * HALF + core * rows + hh * GROUP, GROUP), GROUP)
                    rt[d % 4, :, at, :] = right[:, e]
                a_own[d % 2, part(hh, GROUP * HID), :] = left
            loop(rows // GROUP, half)

            @pl.when((d // 4) * ((d + 1) % 2) == 1)
            def _():
                pl.semaphore_wait(ob_free, 1)
            for e in range(2):
                ob_copy(d, e, core).start()

            @pl.when(d % 2 == 1)
            def _():
                for e in range(2):
                    ob_copy(d - 1, e, 1 - core).wait_recv()
                    ob_copy(d, e, 1 - core).wait_recv()

                def group(g):
                    at = part(g, 2)
                    acc[g] += (nt_dot(a_own[0], rt[(d - 1) % 4, at].reshape(256, seq))
                               + nt_dot(a_own[1], rt[d % 4, at].reshape(256, seq)))
                loop(acc.shape[0], group)

                @pl.when(d < 4)
                def _():
                    pl.semaphore_signal(ob_free, inc=1, device_id=dev(sib), device_id_type=pl.DeviceIdType.MESH)
        loop(8, chunk)
        cnt_e[:] = cnt[:].reshape(rows, 1, res)

        def pair_rows(n):
            for g in range(8):
                t = acc[g, part(n, HALF), :]
                for b in range(2):
                    u0, u1 = t[:HID, b * LANES:b * LANES + LANES], t[HID:, b * LANES:b * LANES + LANES]
                    q = g * 4 + b * 2
                    lo = lane_lo[:HID]
                    o_pair[q * HID:q * HID + HID, :] = jnp.where(lo, u0, pltpu.roll(u1, HALF, 1)).astype(BF)
                    o_pair[q * HID + HID:q * HID + HALF, :] = jnp.where(lo, pltpu.roll(u0, HALF, 1), u1).astype(BF)
            r_own[n] = jnp.dot(wo_e[:], o_pair[:], preferred_element_type=F32)
        loop(rows // 2, pair_rows)
        for d in range(4, 8):
            for e in range(2):
                ob_copy(d, e, core).wait_send()
        load_mask(me)
        mask_et[:] = mask_i[:].astype(F32).T

    pl.run_scoped(
        own_pairs, pltpu.VMEM((res, seq), F32), pltpu.VMEM((rows, res), F32),
        pltpu.VMEM((2, rows * HID, seq), BF), pltpu.VMEM((8, rows * HID, 256), F32), pltpu.VMEM((1024, LANES), BF))

    def transpose(tin, f_in, f_out):
        side = GROUP * 8
        units = 24

        def i_copy(u):
            return pltpu.make_async_copy(
                e_out.at[part(u // 12, side), part(u % 4, GROUP), part(u // 4 % 3, side)], tin.at[u % 2], t_isem.at[u % 2])

        i_copy(0).start()

        def unit(u):
            @pl.when(u < units - 1)
            def _():
                i_copy(u + 1).start()
            i_copy(u).wait()

            def widen(i):
                f_in[part(i, side)] = tin[u % 2, part(i, 8)].astype(F32).reshape(side, side)
            loop(GROUP, widen)

            def flip(i):
                for v in range(4):
                    at = pl.ds(i * 4 + v, side, stride=GROUP)
                    f_out[at] = f_in[at].T
            loop(4, flip)

            def narrow(i):
                e_t[part(u // 4 % 3 * GROUP + i, 8), part(u % 4, GROUP), part(u // 12, side)] = (
                    f_out[part(i, side)].astype(BF).reshape(8, GROUP, side))
            loop(GROUP, narrow)
        loop(units, unit)

    def b_rows(kk, c):
        return part(kk * 4 + c, HID)

    def k_lane(kk, h):
        return pl.ds(pl.multiple_of(kk * 256 + h * LANES, LANES), LANES)

    def xb_copy(src, kk, h):
        ref = e_t.at[b_rows(kk, src // 2), part(src % 2, rows), part(h, LANES)]
        return remote(ref, ref, xb_ssem.at[src, kk], xb_rsem.at[src, kk], sib)

    def xa_copy(c, kk, h):
        return remote(a_send.at[rblk(c, rows * HID), pl.ds(kk * LANES, LANES)], a_all.at[rblk(c, rows * HID), k_lane(kk, h)],
                      xa_ssem.at[c, kk], xa_rsem.at[c, kk], sib)

    def block(k):
        src = partner(me, k)
        own_half = (src % 2 + core) % 2

        @pl.when(k == 0)
        def _():
            cp = pltpu.make_async_copy(xe.at[:, :, lane(me)], xb, lsem.at[0])
            cp.start()
            cp.wait()
            cp = pltpu.make_async_copy(xb, e_out.at[rblk(me)], lsem.at[0])
            cp.start()
            cp.wait()

        @pl.when(k > 0)
        def _():
            remote(xe.at[:, :, lane(src)], e_out.at[rblk(src)], e_ssem.at[k], e_rsem.at[k], src).wait_recv()
            cp = pltpu.make_async_copy(e_out.at[rblk(src)], xb, lsem.at[0])
            cp.start()
            cp.wait()

        def half(hh):
            r0 = pl.multiple_of(src * rows + hh * GROUP, GROUP)
            right, left = project(hh, mask_et[pl.ds(r0, GROUP), :])
            for kk in range(3):
                r_at = pl.ds(pl.multiple_of(src % 2 * rows + hh * GROUP, GROUP), GROUP)
                e_t[b_rows(kk, src // 2), r_at, part(core, LANES)] = right[:, :, kk * LANES:kk * LANES + LANES]
            at = pl.ds(pl.multiple_of(((src // 2) * rows + hh * GROUP) * HID, GROUP * HID), GROUP * HID)

            @pl.when(own_half == 0)
            def _():
                for kk in range(3):
                    a_all[at, k_lane(kk, core)] = left[:, kk * LANES:kk * LANES + LANES]

            @pl.when(own_half == 1)
            def _():
                a_send[at, :] = left
        loop(rows // GROUP, half)
        for kk in range(3):
            xb_copy(src, kk, core).start()

        @pl.when(own_half == 1)
        def _():
            for kk in range(3):
                xa_copy(src // 2, kk, core).start()
    loop(8, block)

    for k in range(1, 8):
        e_copy(k).wait_send()


    def xwait(s):
        for kk in range(3):
            xb_copy(s, kk, 1 - core).wait_recv()
    loop(8, xwait)

    def xwait_a(c):
        for kk in range(3):
            xa_copy(c, kk, 1 - core).wait_recv()
    loop(4, xwait_a)

    def rs_copy(n):
        t, first, count, k = ((0, 0, 8, 2), (0, 8, 8, 4), (1, 0, 8, 2), (2, 8, 8, 4),
                              (2, 0, 4, 4), (1, 8, 4, 2), (2, 4, 4, 4), (1, 12, 4, 2))[n]
        at = pl.ds(first, count)
        dst = rs_mid.at[first // 8] if t == 0 else rs_recv.at[t - 1, at]
        return remote(rt.at[t, at], dst, rs_ssem.at[n], rs_rsem.at[n], partner(me, k))

    def contract_extra(o_s):
        pairs = GROUP // 2
        low = lax.broadcasted_iota(jnp.int32, (pairs * HID, LANES), 1) < HALF

        def eblk(n):
            t = ((n // 2 + 1) // 2) % 2 * (1 + (n // 2 + n + 1) % 2) + 3 * (n // 6)
            ib = n % 2
            c = partner(me, 2 * (1 - t // 2) + 4 * (1 - t % 2)) // 2
            at = pl.ds(pl.multiple_of((c * rows + ib * GROUP) * HID, GROUP * HID), GROUP * HID)
            away = (1 - c // 2) * 2
            near = c // 2 * 2 + 1 - c % 2

            def right(blocks):
                return jnp.concatenate([jnp.concatenate(
                    [e_t[(kk * 4 + chip_j) * HID + q] for q, chip_j in blocks], axis=0) for kk in range(3)], axis=1)

            def qstep(qq):
                for h in range(2):
                    q = qq * QSTEP + h * 2
                    o = nt_dot(a_all[at, :], right([(q + x, away + y) for x in range(2) for y in range(2)]))
                    o = o.astype(BF).reshape(pairs, 2, HID, 256)
                    for v in range(2):
                        for x in range(2):
                            o_s[:, part(q + x, HID), pl.ds(v * LANES, LANES)] = o[:, v, :, x * LANES:x * LANES + LANES]
                q = qq * QSTEP
                o = nt_dot(a_all[at, :], right([(q + x, near) for x in range(QSTEP)]))
                o = o.reshape(pairs, 2, HID, 256)
                for x in range(2):
                    u0, u1 = (o[:, v, :, x * LANES:x * LANES + LANES].reshape(pairs * HID, LANES) for v in range(2))
                    for y, both in ((0, jnp.where(low, u0, pltpu.roll(u1, HALF, 1))),
                                    (1, jnp.where(low, pltpu.roll(u0, HALF, 1), u1))):
                        o_s[:, part(q + x * 2 + y, HID), pl.ds(2 * LANES, LANES)] = both.astype(BF).reshape(pairs, HID, LANES)
            loop(HID // QSTEP, qstep)

            def rstep(ii):
                for u in range(RSTEP // 2):
                    i = ii * (RSTEP // 2) + u
                    rt[t, ib * pairs + i] = jnp.dot(wo_e[:], o_s[i], preferred_element_type=F32).astype(BF)
            loop(GROUP // RSTEP, rstep)

            for v in range(6):
                @pl.when(n == v)
                def _():
                    if v >= 4:
                        rs_copy(v - 4).wait_recv()
                        for h in range(2):
                            def add(i):
                                i = h * 4 + i
                                at = (t, ib * pairs + i)
                                rt[at] = (rt[at].astype(F32) + rs_mid[v - 4, i].astype(F32)).astype(BF)
                            loop(4, add)
                            rs_copy(v + h * 2).start()
                    else:
                        rs_copy(v).start()
                    if v == 0:
                        for i in range(2):
                            g_wait(i + 1).wait_recv()
                            d_copy(i).start()
                            f_copy(i).start()
                    if v == 1:
                        for k in (3, 5, 6, 7):
                            m_copy(k).start()
        loop(8, eblk)

        for i in range(2):
            d_wait(i).wait_recv()
        f_copy(2).start()
        g_wait(0).wait_recv()
        for i in range(3):
            f_wait(i).wait_recv()

    def contract_main(o_s):
        def mblk(ib):
            at = part(ib, GROUP * HID)

            def qstep(qq):
                for u in range(QSTEP):
                    q = qq * QSTEP + u
                    o_s[:, part(q, HID), :] = nt_dot(am[at, :], bm[q]).astype(BF).reshape(GROUP, HID, res)
            loop(HID // QSTEP, qstep)

            def rstep(ii):
                for u in range(RSTEP):
                    i = ii * RSTEP + u
                    row = ib * GROUP + i
                    r = jnp.dot(wo_m[:], o_s[i], preferred_element_type=F32)
                    pair_out[row] = ((r + bo_m[:]) / (NORM_EPS + cnt_m[row])).T
            loop(GROUP // RSTEP, rstep)
        loop(rows // GROUP, mblk)

    pl.run_scoped(contract_extra, pltpu.VMEM((GROUP // 2, 1024, 3 * LANES), BF))
    pl.run_scoped(contract_main, pltpu.VMEM((GROUP, 1024, res), BF))
    def drain(s):
        for kk in range(3):
            xb_copy(s, kk, core).wait_send()
    loop(8, drain)

    def drain_a(c):
        for kk in range(3):
            xa_copy(c, kk, core).wait_send()
    loop(4, drain_a)

    pl.run_scoped(
        transpose, pltpu.VMEM((2, LANES, GROUP, LANES), BF), pltpu.VMEM((LANES * GROUP, LANES), F32),
        pltpu.VMEM((LANES * GROUP, LANES), F32))

    def final(zb):
        def z_copy(j):
            return pltpu.make_async_copy(pair.at[part(j, 8)], zb.at[part(j, 8)], lsem.at[3 + j])

        steps = rows // 8
        for j in range(steps):
            z_copy(j).start()
        hi0 = lax.broadcasted_iota(jnp.int32, (LANES, LANES), 0) * 0 + chip // 2 == 0
        odd = lax.broadcasted_iota(jnp.int32, (LANES, LANES), 0) * 0 + chip % 2 == 1

        def row2(n):
            tot = rt[3, n].astype(F32) + rs_recv[0, n].astype(F32) + rs_recv[1, n].astype(F32)
            kept, own = tot[:, 256:], r_own[n]
            rkept, rown = pltpu.roll(kept, HALF, 1), pltpu.roll(own, HALF, 1)
            near0 = jnp.where(lane_lo, jnp.where(odd, kept, own), jnp.where(odd, rown, rkept))
            near1 = jnp.where(lane_lo, jnp.where(odd, rkept, rown), jnp.where(odd, own, kept))
            for v, near in ((0, near0), (1, near1)):
                away = tot[:, v * LANES:v * LANES + LANES]
                row = n * 2 + v
                r = jnp.concatenate([jnp.where(hi0, near, away), jnp.where(hi0, away, near)], axis=1)
                te = (r + bo_e[:]) / (NORM_EPS + cnt_e[row])
                pair_out[row] = (zb[row] + te.T) + pair_out[row]

        for j in range(steps):
            z_copy(j).wait()
        for first, parts in ((0, (2, 4)), (8, (3, 5)), (4, (6,)), (12, (7,))):
            for n in parts:
                rs_copy(n).wait_recv()
            loop(4, lambda i: row2(first + i))

    pl.run_scoped(final, pltpu.VMEM((rows, res, LANES), F32))

    for k in range(1, 8):
        m_copy(k).wait_send()
        to = partner(me, k)
        remote(xm.at[rblk(me, mseq)], m_out.at[:, rblk(to), :], m_ssem.at[k], m_rsem.at[k], to).wait_recv()

    for i in range(3):
        g_copy(i).wait_send()
    for i in range(2):
        d_copy(i).wait_send()
    for i in range(3):
        f_copy(i).wait_send()
    for n in range(8):
        rs_copy(n).wait_send()


def store_kernel(pair_in, e_in, m_in, pair_out, e_out, m_out, sem):
    copies = []
    for i, (src, dst) in enumerate(((pair_in, pair_out), (e_in, e_out), (m_in, m_out))):
        copies.append(pltpu.make_async_copy(src, dst, sem.at[i]))
    for copy in copies:
        copy.start()
    for copy in copies:
        copy.wait()


def solution(mesh):
    msa_spec = P('data', 'dap', None)
    mask_spec = P('data', None)
    row_spec = P(('data', 'dap'), None, None)

    def local_program(extra_block, extra_mask, main_block, main_mask, pair_rows,
                      e_gam, e_bet, e_wl, e_bl, e_wr, e_br, e_wo, e_bo,
                      m_gam, m_bet, m_wl, m_bl, m_wr, m_br, m_wo, m_bo):
        seqs, rows, ce = extra_block.shape
        mseqs, _, cm = main_block.shape
        res = extra_mask.shape[1]
        hid = e_wl.shape[1]
        nk = e_wo.shape[1]
        seq = seqs // 8
        args = (
            jnp.transpose(extra_block, (1, 2, 0)), main_block, extra_mask, main_mask, pair_rows,
            e_gam, e_bet, e_wl.T, e_bl, e_wr.T, e_br, e_wo, e_bo, m_gam, m_bet, m_wl.T, m_bl, m_wr.T, m_br, m_wo, m_bo)
        any_spec = pl.BlockSpec(memory_space=pl.ANY)
        vmem = pl.BlockSpec(memory_space=pltpu.VMEM)
        dma = pltpu.SemaphoreType.DMA
        pair_out, e_seq, m_seq, _ = pl.pallas_call(
            opm_kernel,
            out_shape=(
                pltpu.VMEM((rows, res, nk), F32),
                pltpu.VMEM((seq, ce, res), BF),
                pltpu.VMEM((mseqs // 8, res, cm), BF),
                jax.ShapeDtypeStruct((res, ce, seq), BF)),
            in_specs=[any_spec, any_spec, any_spec, vmem, any_spec] + [vmem] * 16,
            out_specs=(vmem, vmem, vmem, any_spec),
            scratch_shapes=[
                pltpu.VMEM((4 * rows * hid, 2 * seq), BF),
                pltpu.VMEM((4 * rows * hid, seq), BF),
                pltpu.VMEM((rows, ce, seq), BF),
                pltpu.VMEM((GROUP * ce, seq), BF),
                pltpu.VMEM((seq, res), jnp.int32),
                pltpu.VMEM((res, seq), F32),
                pltpu.VMEM((rows, 1, mseqs), F32),
                pltpu.VMEM((rows * hid, mseqs), BF),
                pltpu.VMEM((hid, res, mseqs), BF),
                pltpu.VMEM((4, rows // 2, nk, res // 2 * 3), BF),
                pltpu.VMEM((2, GROUP // 2, nk, res // 2 * 3), BF),
                pltpu.VMEM((2, rows // 2, nk, res // 2 * 3), BF),
                pltpu.VMEM((rows // 2, nk, res // 2), F32),
                pltpu.VMEM((hid * RG, ce * RG), BF),
                pltpu.VMEM((hid * LG, ce * LG), BF),
                pltpu.VMEM((2 * hid, cm), BF),
                pltpu.VMEM((nk, hid * hid), BF),
                pltpu.VMEM((nk, hid * hid), BF),
                pltpu.VMEM((ce, 1), F32),
                pltpu.VMEM((ce, 1), F32),
                pltpu.VMEM((hid * RG, 1), F32),
                pltpu.VMEM((hid, 1), F32),
                pltpu.VMEM((nk, 1), F32),
                pltpu.VMEM((2 * hid, 1), F32),
                pltpu.VMEM((nk, 1), F32),
                pltpu.VMEM((rows, 1, res), F32),
                pltpu.VMEM((rows, 1, res), F32),
                dma((8,)), dma((8,)), dma((8,)), dma((8,)), dma((4, 3)), dma((4, 3)), dma((8, 3)), dma((8, 3)),
                dma((2,)), dma((2,)), dma((2,)),
                dma((3,)), dma((3,)), dma((3,)), dma((3,)), dma((8,)), dma((8,)),
                dma((8,)), dma((8,)), pltpu.SemaphoreType.REGULAR, dma((8,))],
            compiler_params=pltpu.CompilerParams(
                collective_id=0, has_side_effects=True, vmem_limit_bytes=VMEM_LIMIT),
            name='opm',
        )(*args)
        pair_out, e_seq, m_seq = pl.pallas_call(
            store_kernel,
            out_shape=tuple(jax.ShapeDtypeStruct(x.shape, x.dtype) for x in (pair_out, e_seq, m_seq)),
            in_specs=[vmem] * 3,
            out_specs=(any_spec,) * 3,
            scratch_shapes=[dma((3,))],
            compiler_params=pltpu.CompilerParams(vmem_limit_bytes=2 ** 20),
            name='store',
        )(pair_out, e_seq, m_seq)
        return pair_out, jnp.transpose(e_seq, (0, 2, 1)), m_seq

    in_specs = (msa_spec, mask_spec, msa_spec, mask_spec, row_spec) + (P(),) * 16
    return jax.shard_map(local_program, mesh=mesh, in_specs=in_specs, out_specs=(row_spec,) * 3, check_vma=False)
```

```python
import functools

import jax
import jax.numpy as jnp
from jax import lax
from jax.experimental import pallas as pl
from jax.experimental.pallas import tpu as pltpu
from jax.sharding import PartitionSpec as P

LN_EPS = 1e-5
NORM_EPS = 1e-3
BF = jnp.bfloat16
F32 = jnp.float32
GROUP = 16
VMEM_LIMIT = 43 * 2 ** 20
QSTEP = 4
LSTEP = 4
MSTEP = 8
RG, LG = 8, 4
HID, CE, LANES, HALF = 32, 64, 128, 64
RSTEP = 8


def loop(n, body):
    def step(i, carry):
        body(i)
        return carry
    lax.fori_loop(0, n, step, 0)


def part(i, n):
    return pl.ds(pl.multiple_of(i * n, n), n)


def partner(me, k):
    core, cx, cy = me % 2, (me // 2) % 2, me // 4
    k0, k1, k2 = k % 2, (k // 2) % 2, k // 4
    return (core + k0) % 2 + 2 * ((cx + k1) % 2) + 4 * ((cy + k2) % 2)


def nt_dot(lhs, rhs):
    return lax.dot_general(lhs, rhs, (((1,), (1,)), ((), ())), preferred_element_type=F32)


def column(row, n, repeat):
    m = row.shape[1]
    at = lax.broadcasted_iota(jnp.int32, (n, m), 0) // repeat
    return jnp.sum(jnp.where(at == lax.broadcasted_iota(jnp.int32, (n, m), 1), row, 0.0), axis=1, keepdims=True)


def opm_kernel(
    xe, xm, mask_e, mask_m, pair,
    e_gam, e_bet, e_wl, e_bl, e_wr, e_br, e_wo, e_bo,
    m_gam, m_bet, m_wl, m_bl, m_wr, m_br, m_wo, m_bo,
    pair_out, e_t, m_out, e_out, e_half,
    a_all, a_send, xb, y_s, mask_i, mask_et, mask_mo, am, bm, rt, rs_mid, rs_recv, r_own,
    w_right, w_left, w_m, wo_e, wo_m, gam_e, bet_e, bias_b, bias_a, bo_e, bias_m, bo_m, cnt_e, cnt_m,
    e_ssem, e_rsem, m_ssem, m_rsem, xa_ssem, xa_rsem, xb_ssem, xb_rsem,
    d_ssem, d_rsem, t_isem, t_osem, g_ssem, g_rsem, f_ssem, f_rsem, rs_ssem, rs_rsem, ob_ssem, ob_rsem, ob_free, lsem,
):
    me = lax.axis_index('dap')
    core = me % 2
    chip = me // 2
    sib = partner(me, 1)
    seq = e_out.shape[2]
    mseq = m_out.shape[0]
    rows = xe.shape[0]
    res = e_out.shape[0]

    def dev(d):
        return {'dap': d}

    def lane(h):
        return pl.ds(pl.multiple_of(h * seq, LANES), seq)

    def rblk(d, n=rows):
        return part(d, n)

    barrier = pltpu.get_barrier_semaphore()
    for k in range(1, 8):
        pl.semaphore_signal(barrier, inc=1, device_id=dev(partner(me, k)), device_id_type=pl.DeviceIdType.MESH)
    pl.semaphore_wait(barrier, 7)

    def remote(src, dst, ssem, rsem, target):
        return pltpu.make_async_remote_copy(
            src_ref=src, dst_ref=dst, send_sem=ssem, recv_sem=rsem,
            device_id=dev(target), device_id_type=pl.DeviceIdType.MESH)

    def e_copy(k):
        to = partner(me, k)
        return remote(xe.at[:, :, lane(to)], e_out.at[rblk(me)], e_ssem.at[k], e_rsem.at[k], to)

    for k in (1, 2, 4, 3, 5, 6, 7):
        e_copy(k).start()

    def m_copy(k):
        to = partner(me, k)
        return remote(xm.at[rblk(to, mseq)], m_out.at[:, rblk(me), :], m_ssem.at[k], m_rsem.at[k], to)

    def row_of(ref):
        v = ref[:].astype(F32)
        return v.reshape(1, v.shape[0])

    def weights(wf, wp):
        gam_e[:] = column(row_of(e_gam), HALF, 1)
        bet_e[:] = column(row_of(e_bet), HALF, 1)
        bias_b[:] = column(row_of(e_br), HID * RG, RG)
        bias_a[:] = column(row_of(e_bl), HID, 1)
        bo_e[:] = column(row_of(e_bo), LANES, 1)
        bo_m[:] = column(row_of(m_bo), LANES, 1)
        bias_m[:HID] = column(row_of(m_bl), HID, 1)
        bias_m[HID:] = column(row_of(m_br), HID, 1)
        w_m[:HID] = m_wl[:]
        w_m[HID:] = m_wr[:]

        def wide(ref, n):
            w = ref[:].astype(F32)
            return jnp.concatenate([w] * n, axis=1)

        def place(dst, rep, residue):
            at = lax.broadcasted_iota(jnp.int32, dst.shape, 0)
            dst[:] = jnp.where(residue(at) == lax.broadcasted_iota(jnp.int32, dst.shape, 1) // CE, rep, 0.0).astype(BF)

        w = wide(e_wr, RG)
        place(w_right, jnp.broadcast_to(w[:, None, :], (HID, RG, RG * CE)).reshape(HID * RG, RG * CE), lambda at: at % RG)
        place(w_left, jnp.concatenate([wide(e_wl, LG)] * LG, axis=0), lambda at: at // HID)
        for src, dst in ((e_wo, wo_e), (m_wo, wo_m)):
            wf[:] = src[:].astype(F32)

            def pick(q):
                wp[part(q, HID), :] = wf[pl.ds(q, HID, stride=HID), :]
            loop(HID, pick)
            dst[:] = wp[:].T.astype(BF)

    pl.run_scoped(weights, pltpu.VMEM((1024, LANES), F32), pltpu.VMEM((1024, LANES), F32))

    def masks(mt):
        mt[:] = mask_m[:].astype(F32).T
        own = mt[rblk(me), :]
        mask_mo[:] = own.reshape(rows, 1, mask_m.shape[0])
        cnt_m[:] = jnp.dot(own.astype(BF), mask_m[:].astype(F32).astype(BF),
                             preferred_element_type=F32).reshape(rows, 1, res)

    pl.run_scoped(masks, pltpu.VMEM((res, mask_m.shape[0]), F32))

    def load_mask(d):
        cp = pltpu.make_async_copy(mask_e.at[rblk(d, seq)], mask_i, lsem.at[0])
        cp.start()
        cp.wait()

    def main_proj(xc, xf, bf):
        cp = pltpu.make_async_copy(xm.at[rblk(me, mseq)], xc.at[pl.ds(0, mseq)], lsem.at[1])
        cp.start()
        cp.wait()
        m_out[:, rblk(me), :] = xc[pl.ds(0, mseq)]
        step = xc.shape[0]
        gam_m, bet_m = row_of(m_gam), row_of(m_bet)
        for piece in range(xm.shape[0] // step):
            cp = pltpu.make_async_copy(xm.at[pl.ds(piece * step, step)], xc, lsem.at[2])
            cp.start()
            cp.wait()

            def widen(i):
                s = part(i, 8)
                xf[s] = xc[s].astype(F32)
            loop(step // 8, widen)

            def one(r):
                x = xf[:, r, :]
                mean = jnp.mean(x, axis=1, keepdims=True)
                cen = x - mean
                var = jnp.mean(cen * cen, axis=1, keepdims=True)
                y = (cen * lax.rsqrt(var + LN_EPS) * gam_m + bet_m).astype(BF)
                proj = nt_dot(w_m[:], y) + bias_m[:]
                proj = proj * mask_mo[r, :, pl.ds(piece * step, step)]
                am[part(r, HID), pl.ds(piece * step, step)] = proj[:HID].astype(BF)
                bf[:, r, :] = proj[HID:]
            def some(i):
                for u in range(MSTEP):
                    one(i * MSTEP + u)

            loop(rows // MSTEP, some)
            bm[:, rblk(me), pl.ds(piece * step, step)] = bf[:].astype(BF)

    pl.run_scoped(
        main_proj, pltpu.VMEM((LANES, rows, xm.shape[2]), BF), pltpu.VMEM((LANES, rows, xm.shape[2]), F32),
        pltpu.VMEM((HID, rows, LANES), F32))

    def g_copy(i):
        ref = bm.at[:, rblk(me), :]
        return remote(ref, ref, g_ssem.at[i], g_rsem.at[i], partner(me, (1, 2, 4)[i]))

    def g_wait(i):
        to = partner(me, (1, 2, 4)[i])
        ref = bm.at[:, rblk(to), :]
        return remote(ref, ref, g_ssem.at[i], g_rsem.at[i], to)

    def d_copy(i):
        ref = bm.at[part(i, HID // 2), rblk(partner(me, (2, 4)[i])), :]
        return remote(ref, ref, d_ssem.at[i], d_rsem.at[i], partner(me, (4, 2)[i]))

    def d_wait(i):
        ref = bm.at[part(i, HID // 2), rblk(partner(me, 6)), :]
        return remote(ref, ref, d_ssem.at[i], d_rsem.at[i], partner(me, (4, 2)[i]))

    def f_copy(i):
        ref = bm.at[:, rblk(partner(me, (2, 4, 6)[i])), :]
        return remote(ref, ref, f_ssem.at[i], f_rsem.at[i], sib)

    def f_wait(i):
        ref = bm.at[:, rblk(partner(me, (3, 5, 7)[i])), :]
        return remote(ref, ref, f_ssem.at[i], f_rsem.at[i], sib)

    for i in range(3):
        g_copy(i).start()
    for k in (1, 2, 4):
        m_copy(k).start()

    def project(hh, m16):
        def norm(i):
            for u in range(LSTEP):
                r = i * LSTEP + u
                x = xb[hh * GROUP + r].astype(F32)
                mean = jnp.mean(x, axis=0, keepdims=True)
                cen = x - mean
                var = jnp.mean(cen * cen, axis=0, keepdims=True)
                y = cen * lax.rsqrt(var + LN_EPS) * gam_e[:] + bet_e[:]
                y_s[part(r, CE), :] = y.astype(BF)
        loop(GROUP // LSTEP, norm)

        def dot(w, g):
            return jnp.dot(w[:], y_s[pl.ds(g * w.shape[1], w.shape[1])], preferred_element_type=F32)

        right = jnp.concatenate(
            [(dot(w_right, g) + bias_b[:]).reshape(HID, RG, seq) for g in range(GROUP // RG)], axis=1)
        right = (right * m16[None]).astype(BF)
        left = []
        for g in range(GROUP // LG):
            d = dot(w_left, g)
            for r in range(LG):
                left.append((d[r * HID:r * HID + HID] + bias_a[:]) * m16[g * LG + r:g * LG + r + 1])
        left = jnp.concatenate(left, axis=0).astype(BF)
        return right, left

    lane_lo = lax.broadcasted_iota(jnp.int32, (LANES, LANES), 1) < HALF

    def ob_copy(d, e, h):
        ref = rt.at[d % 4, :, pl.ds(pl.multiple_of(e * HALF + h * rows, rows), rows), :]
        return remote(ref, ref, ob_ssem.at[d % 4 * 2 + e], ob_rsem.at[d % 4 * 2 + e], sib)

    def own_pairs(mt, cnt, a_own, acc, o_pair):
        cnt[:] = jnp.zeros_like(cnt)

        def zero(g):
            acc[g] = jnp.zeros(acc.shape[1:], F32)
        loop(acc.shape[0], zero)

        def chunk(d):
            xcp = pltpu.make_async_copy(xe.at[:, :, lane(d)], xb, lsem.at[1])
            xcp.start()
            load_mask(d)
            m = mask_i[:].astype(F32)
            mt[:] = m.T
            cnt[:] += jnp.dot(mt[rblk(me), :].astype(BF), m.astype(BF), preferred_element_type=F32)

            @pl.when(d >= 4)
            def _():
                for e in range(2):
                    ob_copy(d, e, core).wait_send()
            xcp.wait()

            def half(hh):
                right, left = project(hh, mt[pl.ds(pl.multiple_of(me * rows + hh * GROUP, GROUP), GROUP), :])
                right = right.reshape(16, 2, GROUP, seq)
                for e in range(2):
                    at = pl.ds(pl.multiple_of(e * HALF + core * rows + hh * GROUP, GROUP), GROUP)
                    rt[d % 4, :, at, :] = right[:, e]
                a_own[d % 2, part(hh, GROUP * HID), :] = left
            loop(rows // GROUP, half)

            @pl.when((d // 4) * ((d + 1) % 2) == 1)
            def _():
                pl.semaphore_wait(ob_free, 1)
            for e in range(2):
                ob_copy(d, e, core).start()

            @pl.when(d % 2 == 1)
            def _():
                for e in range(2):
                    ob_copy(d - 1, e, 1 - core).wait_recv()
                    ob_copy(d, e, 1 - core).wait_recv()

                def group(g):
                    at = part(g, 2)
                    acc[g] += (nt_dot(a_own[0], rt[(d - 1) % 4, at].reshape(256, seq))
                               + nt_dot(a_own[1], rt[d % 4, at].reshape(256, seq)))
                loop(acc.shape[0], group)

                @pl.when(d < 4)
                def _():
                    pl.semaphore_signal(ob_free, inc=1, device_id=dev(sib), device_id_type=pl.DeviceIdType.MESH)
        loop(8, chunk)
        cnt_e[:] = cnt[:].reshape(rows, 1, res)

        def pair_rows(n):
            for g in range(8):
                t = acc[g, part(n, HALF), :]
                for b in range(2):
                    u0, u1 = t[:HID, b * LANES:b * LANES + LANES], t[HID:, b * LANES:b * LANES + LANES]
                    q = g * 4 + b * 2
                    lo = lane_lo[:HID]
                    o_pair[q * HID:q * HID + HID, :] = jnp.where(lo, u0, pltpu.roll(u1, HALF, 1)).astype(BF)
                    o_pair[q * HID + HID:q * HID + HALF, :] = jnp.where(lo, pltpu.roll(u0, HALF, 1), u1).astype(BF)
            r_own[n] = jnp.dot(wo_e[:], o_pair[:], preferred_element_type=F32)
        loop(rows // 2, pair_rows)
        for d in range(4, 8):
            for e in range(2):
                ob_copy(d, e, core).wait_send()
        load_mask(me)
        mask_et[:] = mask_i[:].astype(F32).T

    pl.run_scoped(
        own_pairs, pltpu.VMEM((res, seq), F32), pltpu.VMEM((rows, res), F32),
        pltpu.VMEM((2, rows * HID, seq), BF), pltpu.VMEM((8, rows * HID, 256), F32), pltpu.VMEM((1024, LANES), BF))

    side = GROUP * 8
    units = 12

    def transpose(yh, narrow, stored, tin, f_in, f_out):
        def i_copy(u):
            return pltpu.make_async_copy(
                e_out.at[part(yh, side), part(u % 4, GROUP), part(u // 4, side)], tin.at[u % 2], t_isem.at[u % 2])

        i_copy(0).start()

        def unit(u):
            @pl.when(u < units - 1)
            def _():
                i_copy(u + 1).start()
            i_copy(u).wait()

            def widen(i):
                f_in[part(i, side)] = tin[u % 2, part(i, 8)].astype(F32).reshape(side, side)
            loop(GROUP, widen)

            def flip(i):
                for v in range(4):
                    at = pl.ds(i * 4 + v, side, stride=GROUP)
                    f_out[at] = f_in[at].T
            loop(4, flip)
            stored(u)
            loop(GROUP, lambda i: narrow(u, i, f_out[part(i, side)].astype(BF).reshape(8, GROUP, side)))
        loop(units, unit)

    def early_half(tout, tin, f_in, f_out):
        def o_copy(u):
            return pltpu.make_async_copy(
                tout.at[u % 2], e_half.at[part(u // 4, side), part(u % 4, GROUP), :], t_osem.at[u % 2])

        def narrow(u, i, value):
            tout[u % 2, part(i, 8)] = value

            @pl.when(i == GROUP - 1)
            def _():
                o_copy(u).start()

        def stored(u):
            @pl.when(u >= 2)
            def _():
                o_copy(u).wait()

        transpose(me // 4, narrow, stored, tin, f_in, f_out)
        o_copy(units - 2).wait()
        o_copy(units - 1).wait()

    def late_half(tin, f_in, f_out):
        yh = 1 - me // 4

        def narrow(u, i, value):
            e_t[part(u // 4 * GROUP + i, 8), part(u % 4, GROUP), part(yh, side)] = value

        transpose(yh, narrow, lambda u: None, tin, f_in, f_out)

    tile = pltpu.VMEM((2, LANES, GROUP, LANES), BF)
    wide_tile = pltpu.VMEM((LANES * GROUP, LANES), F32)

    def b_rows(kk, c):
        return part(kk * 4 + c, HID)

    def k_lane(kk, h):
        return pl.ds(pl.multiple_of(kk * 256 + h * LANES, LANES), LANES)

    def xb_copy(src, kk, h):
        ref = e_t.at[b_rows(kk, src // 2), part(src % 2, rows), part(h, LANES)]
        return remote(ref, ref, xb_ssem.at[src, kk], xb_rsem.at[src, kk], sib)

    def xa_copy(c, kk, h):
        return remote(a_send.at[rblk(c, rows * HID), pl.ds(kk * LANES, LANES)], a_all.at[rblk(c, rows * HID), k_lane(kk, h)],
                      xa_ssem.at[c, kk], xa_rsem.at[c, kk], sib)

    def block(k):
        src = partner(me, k)
        own_half = (src % 2 + core) % 2

        @pl.when(k == 0)
        def _():
            cp = pltpu.make_async_copy(xe.at[:, :, lane(me)], xb, lsem.at[0])
            cp.start()
            cp.wait()
            cp = pltpu.make_async_copy(xb, e_out.at[rblk(me)], lsem.at[0])
            cp.start()
            cp.wait()

        @pl.when(k > 0)
        def _():
            remote(xe.at[:, :, lane(src)], e_out.at[rblk(src)], e_ssem.at[k], e_rsem.at[k], src).wait_recv()
            cp = pltpu.make_async_copy(e_out.at[rblk(src)], xb, lsem.at[0])
            cp.start()
            cp.wait()

        def half(hh):
            r0 = pl.multiple_of(src * rows + hh * GROUP, GROUP)
            right, left = project(hh, mask_et[pl.ds(r0, GROUP), :])
            for kk in range(3):
                r_at = pl.ds(pl.multiple_of(src % 2 * rows + hh * GROUP, GROUP), GROUP)
                e_t[b_rows(kk, src // 2), r_at, part(core, LANES)] = right[:, :, kk * LANES:kk * LANES + LANES]
            at = pl.ds(pl.multiple_of(((src // 2) * rows + hh * GROUP) * HID, GROUP * HID), GROUP * HID)

            @pl.when(own_half == 0)
            def _():
                for kk in range(3):
                    a_all[at, k_lane(kk, core)] = left[:, kk * LANES:kk * LANES + LANES]

            @pl.when(own_half == 1)
            def _():
                a_send[at, :] = left
        loop(rows // GROUP, half)
        for kk in range(3):
            xb_copy(src, kk, core).start()

        @pl.when(own_half == 1)
        def _():
            for kk in range(3):
                xa_copy(src // 2, kk, core).start()

        @pl.when(k == 3)
        def _():
            pl.run_scoped(early_half, tile, tile, wide_tile, wide_tile)
    loop(8, block)

    for k in range(1, 8):
        e_copy(k).wait_send()


    def xwait(s):
        for kk in range(3):
            xb_copy(s, kk, 1 - core).wait_recv()
    loop(8, xwait)

    def xwait_a(c):
        for kk in range(3):
            xa_copy(c, kk, 1 - core).wait_recv()
    loop(4, xwait_a)

    def rs_copy(n):
        t, first, count, k = ((0, 0, 8, 2), (0, 8, 8, 4), (1, 0, 8, 2), (2, 8, 8, 4),
                              (2, 0, 4, 4), (1, 8, 4, 2), (2, 4, 4, 4), (1, 12, 4, 2))[n]
        at = pl.ds(first, count)
        dst = rs_mid.at[first // 8] if t == 0 else rs_recv.at[t - 1, at]
        return remote(rt.at[t, at], dst, rs_ssem.at[n], rs_rsem.at[n], partner(me, k))

    def contract_extra(o_s):
        pairs = GROUP // 2
        low = lax.broadcasted_iota(jnp.int32, (pairs * HID, LANES), 1) < HALF

        def eblk(n):
            t = ((n // 2 + 1) // 2) % 2 * (1 + (n // 2 + n + 1) % 2) + 3 * (n // 6)
            ib = n % 2
            c = partner(me, 2 * (1 - t // 2) + 4 * (1 - t % 2)) // 2
            at = pl.ds(pl.multiple_of((c * rows + ib * GROUP) * HID, GROUP * HID), GROUP * HID)
            away = (1 - c // 2) * 2
            near = c // 2 * 2 + 1 - c % 2

            def right(blocks):
                return jnp.concatenate([jnp.concatenate(
                    [e_t[(kk * 4 + chip_j) * HID + q] for q, chip_j in blocks], axis=0) for kk in range(3)], axis=1)

            def qstep(qq):
                for h in range(2):
                    q = qq * QSTEP + h * 2
                    o = nt_dot(a_all[at, :], right([(q + x, away + y) for x in range(2) for y in range(2)]))
                    o = o.astype(BF).reshape(pairs, 2, HID, 256)
                    for v in range(2):
                        for x in range(2):
                            o_s[:, part(q + x, HID), pl.ds(v * LANES, LANES)] = o[:, v, :, x * LANES:x * LANES + LANES]
                q = qq * QSTEP
                o = nt_dot(a_all[at, :], right([(q + x, near) for x in range(QSTEP)]))
                o = o.reshape(pairs, 2, HID, 256)
                for x in range(2):
                    u0, u1 = (o[:, v, :, x * LANES:x * LANES + LANES].reshape(pairs * HID, LANES) for v in range(2))
                    for y, both in ((0, jnp.where(low, u0, pltpu.roll(u1, HALF, 1))),
                                    (1, jnp.where(low, pltpu.roll(u0, HALF, 1), u1))):
                        o_s[:, part(q + x * 2 + y, HID), pl.ds(2 * LANES, LANES)] = both.astype(BF).reshape(pairs, HID, LANES)
            loop(HID // QSTEP, qstep)

            def rstep(ii):
                for u in range(RSTEP // 2):
                    i = ii * (RSTEP // 2) + u
                    rt[t, ib * pairs + i] = jnp.dot(wo_e[:], o_s[i], preferred_element_type=F32).astype(BF)
            loop(GROUP // RSTEP, rstep)

            for v in range(6):
                @pl.when(n == v)
                def _():
                    if v >= 4:
                        rs_copy(v - 4).wait_recv()
                        for h in range(2):
                            def add(i):
                                i = h * 4 + i
                                at = (t, ib * pairs + i)
                                rt[at] = (rt[at].astype(F32) + rs_mid[v - 4, i].astype(F32)).astype(BF)
                            loop(4, add)
                            rs_copy(v + h * 2).start()
                    else:
                        rs_copy(v).start()
                    if v == 0:
                        for i in range(2):
                            g_wait(i + 1).wait_recv()
                            d_copy(i).start()
                            f_copy(i).start()
                    if v == 1:
                        for k in (3, 5, 6, 7):
                            m_copy(k).start()
        loop(8, eblk)

        for i in range(2):
            d_wait(i).wait_recv()
        f_copy(2).start()
        g_wait(0).wait_recv()
        for i in range(3):
            f_wait(i).wait_recv()

    def contract_main(o_s):
        def mblk(ib):
            at = part(ib, GROUP * HID)

            def qstep(qq):
                for u in range(QSTEP):
                    q = qq * QSTEP + u
                    o_s[:, part(q, HID), :] = nt_dot(am[at, :], bm[q]).astype(BF).reshape(GROUP, HID, res)
            loop(HID // QSTEP, qstep)

            def rstep(ii):
                for u in range(RSTEP):
                    i = ii * RSTEP + u
                    row = ib * GROUP + i
                    r = jnp.dot(wo_m[:], o_s[i], preferred_element_type=F32)
                    pair_out[row] = ((r + bo_m[:]) / (NORM_EPS + cnt_m[row])).T
            loop(GROUP // RSTEP, rstep)
        loop(rows // GROUP, mblk)

    pl.run_scoped(contract_extra, pltpu.VMEM((GROUP // 2, 1024, 3 * LANES), BF))
    def drain(s):
        for kk in range(3):
            xb_copy(s, kk, core).wait_send()
    loop(8, drain)

    def drain_a(c):
        for kk in range(3):
            xa_copy(c, kk, core).wait_send()
    loop(4, drain_a)
    half_copy = pltpu.make_async_copy(e_half, e_t.at[:, :, part(me // 4, side)], lsem.at[2])
    half_copy.start()
    pl.run_scoped(contract_main, pltpu.VMEM((GROUP, 1024, res), BF))
    pl.run_scoped(late_half, tile, wide_tile, wide_tile)
    half_copy.wait()

    def final(zb):
        def z_copy(j):
            return pltpu.make_async_copy(pair.at[part(j, 8)], zb.at[part(j, 8)], lsem.at[3 + j])

        steps = rows // 8
        for j in range(steps):
            z_copy(j).start()
        hi0 = lax.broadcasted_iota(jnp.int32, (LANES, LANES), 0) * 0 + chip // 2 == 0
        odd = lax.broadcasted_iota(jnp.int32, (LANES, LANES), 0) * 0 + chip % 2 == 1

        def row2(n):
            tot = rt[3, n].astype(F32) + rs_recv[0, n].astype(F32) + rs_recv[1, n].astype(F32)
            kept, own = tot[:, 256:], r_own[n]
            rkept, rown = pltpu.roll(kept, HALF, 1), pltpu.roll(own, HALF, 1)
            near0 = jnp.where(lane_lo, jnp.where(odd, kept, own), jnp.where(odd, rown, rkept))
            near1 = jnp.where(lane_lo, jnp.where(odd, rkept, rown), jnp.where(odd, own, kept))
            for v, near in ((0, near0), (1, near1)):
                away = tot[:, v * LANES:v * LANES + LANES]
                row = n * 2 + v
                r = jnp.concatenate([jnp.where(hi0, near, away), jnp.where(hi0, away, near)], axis=1)
                te = (r + bo_e[:]) / (NORM_EPS + cnt_e[row])
                pair_out[row] = (zb[row] + te.T) + pair_out[row]

        for j in range(steps):
            z_copy(j).wait()
        for first, parts in ((0, (2, 4)), (8, (3, 5)), (4, (6,)), (12, (7,))):
            for n in parts:
                rs_copy(n).wait_recv()
            loop(4, lambda i: row2(first + i))

    pl.run_scoped(final, pltpu.VMEM((rows, res, LANES), F32))

    for k in range(1, 8):
        m_copy(k).wait_send()
        to = partner(me, k)
        remote(xm.at[rblk(me, mseq)], m_out.at[:, rblk(to), :], m_ssem.at[k], m_rsem.at[k], to).wait_recv()

    for i in range(3):
        g_copy(i).wait_send()
    for i in range(2):
        d_copy(i).wait_send()
    for i in range(3):
        f_copy(i).wait_send()
    for n in range(8):
        rs_copy(n).wait_send()


def store_kernel(pair_in, e_in, m_in, pair_out, e_out, m_out, sem):
    copies = []
    for i, (src, dst) in enumerate(((pair_in, pair_out), (e_in, e_out), (m_in, m_out))):
        copies.append(pltpu.make_async_copy(src, dst, sem.at[i]))
    for copy in copies:
        copy.start()
    for copy in copies:
        copy.wait()


def solution(mesh):
    msa_spec = P('data', 'dap', None)
    mask_spec = P('data', None)
    row_spec = P(('data', 'dap'), None, None)

    def local_program(extra_block, extra_mask, main_block, main_mask, pair_rows,
                      e_gam, e_bet, e_wl, e_bl, e_wr, e_br, e_wo, e_bo,
                      m_gam, m_bet, m_wl, m_bl, m_wr, m_br, m_wo, m_bo):
        seqs, rows, ce = extra_block.shape
        mseqs, _, cm = main_block.shape
        res = extra_mask.shape[1]
        hid = e_wl.shape[1]
        nk = e_wo.shape[1]
        seq = seqs // 8
        args = (
            jnp.transpose(extra_block, (1, 2, 0)), main_block, extra_mask, main_mask, pair_rows,
            e_gam, e_bet, e_wl.T, e_bl, e_wr.T, e_br, e_wo, e_bo, m_gam, m_bet, m_wl.T, m_bl, m_wr.T, m_br, m_wo, m_bo)
        any_spec = pl.BlockSpec(memory_space=pl.ANY)
        vmem = pl.BlockSpec(memory_space=pltpu.VMEM)
        dma = pltpu.SemaphoreType.DMA
        pair_out, e_seq, m_seq, _, _ = pl.pallas_call(
            opm_kernel,
            out_shape=(
                pltpu.VMEM((rows, res, nk), F32),
                pltpu.VMEM((seq, ce, res), BF),
                pltpu.VMEM((mseqs // 8, res, cm), BF),
                jax.ShapeDtypeStruct((res, ce, seq), BF),
                jax.ShapeDtypeStruct((seq, ce, res // 2), BF)),
            in_specs=[any_spec, any_spec, any_spec, vmem, any_spec] + [vmem] * 16,
            out_specs=(vmem, vmem, vmem, any_spec, any_spec),
            scratch_shapes=[
                pltpu.VMEM((4 * rows * hid, 2 * seq), BF),
                pltpu.VMEM((4 * rows * hid, seq), BF),
                pltpu.VMEM((rows, ce, seq), BF),
                pltpu.VMEM((GROUP * ce, seq), BF),
                pltpu.VMEM((seq, res), jnp.int32),
                pltpu.VMEM((res, seq), F32),
                pltpu.VMEM((rows, 1, mseqs), F32),
                pltpu.VMEM((rows * hid, mseqs), BF),
                pltpu.VMEM((hid, res, mseqs), BF),
                pltpu.VMEM((4, rows // 2, nk, res // 2 * 3), BF),
                pltpu.VMEM((2, GROUP // 2, nk, res // 2 * 3), BF),
                pltpu.VMEM((2, rows // 2, nk, res // 2 * 3), BF),
                pltpu.VMEM((rows // 2, nk, res // 2), F32),
                pltpu.VMEM((hid * RG, ce * RG), BF),
                pltpu.VMEM((hid * LG, ce * LG), BF),
                pltpu.VMEM((2 * hid, cm), BF),
                pltpu.VMEM((nk, hid * hid), BF),
                pltpu.VMEM((nk, hid * hid), BF),
                pltpu.VMEM((ce, 1), F32),
                pltpu.VMEM((ce, 1), F32),
                pltpu.VMEM((hid * RG, 1), F32),
                pltpu.VMEM((hid, 1), F32),
                pltpu.VMEM((nk, 1), F32),
                pltpu.VMEM((2 * hid, 1), F32),
                pltpu.VMEM((nk, 1), F32),
                pltpu.VMEM((rows, 1, res), F32),
                pltpu.VMEM((rows, 1, res), F32),
                dma((8,)), dma((8,)), dma((8,)), dma((8,)), dma((4, 3)), dma((4, 3)), dma((8, 3)), dma((8, 3)),
                dma((2,)), dma((2,)), dma((2,)), dma((2,)),
                dma((3,)), dma((3,)), dma((3,)), dma((3,)), dma((8,)), dma((8,)),
                dma((8,)), dma((8,)), pltpu.SemaphoreType.REGULAR, dma((8,))],
            compiler_params=pltpu.CompilerParams(
                collective_id=0, has_side_effects=True, vmem_limit_bytes=VMEM_LIMIT),
            name='opm',
        )(*args)
        pair_out, e_seq, m_seq = pl.pallas_call(
            store_kernel,
            out_shape=tuple(jax.ShapeDtypeStruct(x.shape, x.dtype) for x in (pair_out, e_seq, m_seq)),
            in_specs=[vmem] * 3,
            out_specs=(any_spec,) * 3,
            scratch_shapes=[dma((3,))],
            compiler_params=pltpu.CompilerParams(vmem_limit_bytes=2 ** 20),
            name='store',
        )(pair_out, e_seq, m_seq)
        return pair_out, jnp.transpose(e_seq, (0, 2, 1)), m_seq

    in_specs = (msa_spec, mask_spec, msa_spec, mask_spec, row_spec) + (P(),) * 16
    return jax.shard_map(local_program, mesh=mesh, in_specs=in_specs, out_specs=(row_spec,) * 3, check_vma=False)
```

```python
import functools

import jax
import jax.numpy as jnp
from jax import lax
from jax.experimental import pallas as pl
from jax.experimental.pallas import tpu as pltpu
from jax.sharding import PartitionSpec as P

LN_EPS = 1e-5
NORM_EPS = 1e-3
BF = jnp.bfloat16
F32 = jnp.float32
SMALL = 17
GROUP = 16
VMEM_LIMIT = 43 * 2 ** 20
QSTEP = 4
LSTEP = 4
MSTEP = 8
RG, LG = 8, 4
HID, CE, LANES, HALF = 32, 64, 128, 64
RSTEP = 8


def loop(n, body):
    def step(i, carry):
        body(i)
        return carry
    lax.fori_loop(0, n, step, 0)


def part(i, n):
    return pl.ds(pl.multiple_of(i * n, n), n)


def partner(me, k):
    core, cx, cy = me % 2, (me // 2) % 2, me // 4
    k0, k1, k2 = k % 2, (k // 2) % 2, k // 4
    return (core + k0) % 2 + 2 * ((cx + k1) % 2) + 4 * ((cy + k2) % 2)


def nt_dot(lhs, rhs):
    return lax.dot_general(lhs, rhs, (((1,), (1,)), ((), ())), preferred_element_type=F32)


def column(row, n, repeat):
    m = row.shape[1]
    at = lax.broadcasted_iota(jnp.int32, (n, m), 0) // repeat
    return jnp.sum(jnp.where(at == lax.broadcasted_iota(jnp.int32, (n, m), 1), row, 0.0), axis=1, keepdims=True)


def opm_kernel(xe, xm, mask_e, pair, *refs):
    raw, outs, small, scratch = refs[:SMALL], refs[SMALL:SMALL + 5], refs[SMALL + 5:SMALL * 2 + 5], refs[SMALL * 2 + 5:]
    sems = scratch[-1]
    copies = [pltpu.make_async_copy(src, dst, sems.at[i]) for i, (src, dst) in enumerate(zip(raw, small))]
    opm_body(copies, xe, xm, mask_e, small[0], pair, *small[1:], *outs, *scratch[:-1])


def opm_body(
    copies, xe, xm, mask_e, mask_m, pair,
    e_gam, e_bet, e_wl, e_bl, e_wr, e_br, e_wo, e_bo,
    m_gam, m_bet, m_wl, m_bl, m_wr, m_br, m_wo, m_bo,
    pair_out, e_t, m_out, e_out, e_half,
    a_all, a_send, xb, y_s, mask_i, mask_et, mask_mo, am, bm, rt, rs_mid, rs_recv, r_own,
    w_right, w_left, w_m, wo_e, wo_m, gam_e, bet_e, bias_b, bias_a, bo_e, bias_m, bo_m, cnt_e, cnt_m,
    e_ssem, e_rsem, m_ssem, m_rsem, xa_ssem, xa_rsem, xb_ssem, xb_rsem,
    d_ssem, d_rsem, t_isem, t_osem, g_ssem, g_rsem, f_ssem, f_rsem, rs_ssem, rs_rsem, ob_ssem, ob_rsem, ob_free, lsem,
):
    me = lax.axis_index('dap')
    core = me % 2
    chip = me // 2
    sib = partner(me, 1)
    seq = e_out.shape[2]
    mseq = m_out.shape[0]
    rows = xe.shape[0]
    res = e_out.shape[0]

    def dev(d):
        return {'dap': d}

    def lane(h):
        return pl.ds(pl.multiple_of(h * seq, LANES), seq)

    def rblk(d, n=rows):
        return part(d, n)

    for copy in copies:
        copy.start()
    barrier = pltpu.get_barrier_semaphore()
    for k in range(1, 8):
        pl.semaphore_signal(barrier, inc=1, device_id=dev(partner(me, k)), device_id_type=pl.DeviceIdType.MESH)
    pl.semaphore_wait(barrier, 7)

    def remote(src, dst, ssem, rsem, target):
        return pltpu.make_async_remote_copy(
            src_ref=src, dst_ref=dst, send_sem=ssem, recv_sem=rsem,
            device_id=dev(target), device_id_type=pl.DeviceIdType.MESH)

    def e_copy(k):
        to = partner(me, k)
        return remote(xe.at[:, :, lane(to)], e_out.at[rblk(me)], e_ssem.at[k], e_rsem.at[k], to)

    for k in (1, 2, 4, 3, 5, 6, 7):
        e_copy(k).start()

    def m_copy(k):
        to = partner(me, k)
        return remote(xm.at[rblk(to, mseq)], m_out.at[:, rblk(me), :], m_ssem.at[k], m_rsem.at[k], to)

    def row_of(ref):
        v = ref[:].astype(F32)
        return v.reshape(1, v.shape[0])

    for copy in copies:
        copy.wait()

    def weights(wf, wp):
        gam_e[:] = column(row_of(e_gam), HALF, 1)
        bet_e[:] = column(row_of(e_bet), HALF, 1)
        bias_b[:] = column(row_of(e_br), HID * RG, RG)
        bias_a[:] = column(row_of(e_bl), HID, 1)
        bo_e[:] = column(row_of(e_bo), LANES, 1)
        bo_m[:] = column(row_of(m_bo), LANES, 1)
        bias_m[:HID] = column(row_of(m_bl), HID, 1)
        bias_m[HID:] = column(row_of(m_br), HID, 1)
        w_m[:HID] = m_wl[:]
        w_m[HID:] = m_wr[:]

        def wide(ref, n):
            w = ref[:].astype(F32)
            return jnp.concatenate([w] * n, axis=1)

        def place(dst, rep, residue):
            at = lax.broadcasted_iota(jnp.int32, dst.shape, 0)
            dst[:] = jnp.where(residue(at) == lax.broadcasted_iota(jnp.int32, dst.shape, 1) // CE, rep, 0.0).astype(BF)

        w = wide(e_wr, RG)
        place(w_right, jnp.broadcast_to(w[:, None, :], (HID, RG, RG * CE)).reshape(HID * RG, RG * CE), lambda at: at % RG)
        place(w_left, jnp.concatenate([wide(e_wl, LG)] * LG, axis=0), lambda at: at // HID)
        for src, dst in ((e_wo, wo_e), (m_wo, wo_m)):
            wf[:] = src[:].astype(F32)

            def pick(q):
                wp[part(q, HID), :] = wf[pl.ds(q, HID, stride=HID), :]
            loop(HID, pick)
            dst[:] = wp[:].T.astype(BF)

    pl.run_scoped(weights, pltpu.VMEM((1024, LANES), F32), pltpu.VMEM((1024, LANES), F32))

    def masks(mt):
        mt[:] = mask_m[:].astype(F32).T
        own = mt[rblk(me), :]
        mask_mo[:] = own.reshape(rows, 1, mask_m.shape[0])
        cnt_m[:] = jnp.dot(own.astype(BF), mask_m[:].astype(F32).astype(BF),
                             preferred_element_type=F32).reshape(rows, 1, res)

    pl.run_scoped(masks, pltpu.VMEM((res, mask_m.shape[0]), F32))

    def load_mask(d):
        cp = pltpu.make_async_copy(mask_e.at[rblk(d, seq)], mask_i, lsem.at[0])
        cp.start()
        cp.wait()

    def main_proj(xc, xf, bf):
        cp = pltpu.make_async_copy(xm.at[rblk(me, mseq)], xc.at[pl.ds(0, mseq)], lsem.at[1])
        cp.start()
        cp.wait()
        m_out[:, rblk(me), :] = xc[pl.ds(0, mseq)]
        step = xc.shape[0]
        gam_m, bet_m = row_of(m_gam), row_of(m_bet)
        for piece in range(xm.shape[0] // step):
            cp = pltpu.make_async_copy(xm.at[pl.ds(piece * step, step)], xc, lsem.at[2])
            cp.start()
            cp.wait()

            def widen(i):
                s = part(i, 8)
                xf[s] = xc[s].astype(F32)
            loop(step // 8, widen)

            def one(r):
                x = xf[:, r, :]
                mean = jnp.mean(x, axis=1, keepdims=True)
                cen = x - mean
                var = jnp.mean(cen * cen, axis=1, keepdims=True)
                y = (cen * lax.rsqrt(var + LN_EPS) * gam_m + bet_m).astype(BF)
                proj = nt_dot(w_m[:], y) + bias_m[:]
                proj = proj * mask_mo[r, :, pl.ds(piece * step, step)]
                am[part(r, HID), pl.ds(piece * step, step)] = proj[:HID].astype(BF)
                bf[:, r, :] = proj[HID:]
            def some(i):
                for u in range(MSTEP):
                    one(i * MSTEP + u)

            loop(rows // MSTEP, some)
            bm[:, rblk(me), pl.ds(piece * step, step)] = bf[:].astype(BF)

    pl.run_scoped(
        main_proj, pltpu.VMEM((LANES, rows, xm.shape[2]), BF), pltpu.VMEM((LANES, rows, xm.shape[2]), F32),
        pltpu.VMEM((HID, rows, LANES), F32))

    def g_copy(i):
        ref = bm.at[:, rblk(me), :]
        return remote(ref, ref, g_ssem.at[i], g_rsem.at[i], partner(me, (1, 2, 4)[i]))

    def g_wait(i):
        to = partner(me, (1, 2, 4)[i])
        ref = bm.at[:, rblk(to), :]
        return remote(ref, ref, g_ssem.at[i], g_rsem.at[i], to)

    def d_copy(i):
        ref = bm.at[part(i, HID // 2), rblk(partner(me, (2, 4)[i])), :]
        return remote(ref, ref, d_ssem.at[i], d_rsem.at[i], partner(me, (4, 2)[i]))

    def d_wait(i):
        ref = bm.at[part(i, HID // 2), rblk(partner(me, 6)), :]
        return remote(ref, ref, d_ssem.at[i], d_rsem.at[i], partner(me, (4, 2)[i]))

    def f_copy(i):
        ref = bm.at[:, rblk(partner(me, (2, 4, 6)[i])), :]
        return remote(ref, ref, f_ssem.at[i], f_rsem.at[i], sib)

    def f_wait(i):
        ref = bm.at[:, rblk(partner(me, (3, 5, 7)[i])), :]
        return remote(ref, ref, f_ssem.at[i], f_rsem.at[i], sib)

    for i in range(3):
        g_copy(i).start()
    for k in (1, 2, 4):
        m_copy(k).start()

    def project(hh, m16):
        def norm(i):
            for u in range(LSTEP):
                r = i * LSTEP + u
                x = xb[hh * GROUP + r].astype(F32)
                mean = jnp.mean(x, axis=0, keepdims=True)
                cen = x - mean
                var = jnp.mean(cen * cen, axis=0, keepdims=True)
                y = cen * lax.rsqrt(var + LN_EPS) * gam_e[:] + bet_e[:]
                y_s[part(r, CE), :] = y.astype(BF)
        loop(GROUP // LSTEP, norm)

        def dot(w, g):
            return jnp.dot(w[:], y_s[pl.ds(g * w.shape[1], w.shape[1])], preferred_element_type=F32)

        right = jnp.concatenate(
            [(dot(w_right, g) + bias_b[:]).reshape(HID, RG, seq) for g in range(GROUP // RG)], axis=1)
        right = (right * m16[None]).astype(BF)
        left = []
        for g in range(GROUP // LG):
            d = dot(w_left, g)
            for r in range(LG):
                left.append((d[r * HID:r * HID + HID] + bias_a[:]) * m16[g * LG + r:g * LG + r + 1])
        left = jnp.concatenate(left, axis=0).astype(BF)
        return right, left

    lane_lo = lax.broadcasted_iota(jnp.int32, (LANES, LANES), 1) < HALF

    def ob_copy(d, e, h):
        ref = rt.at[d % 4, :, pl.ds(pl.multiple_of(e * HALF + h * rows, rows), rows), :]
        return remote(ref, ref, ob_ssem.at[d % 4 * 2 + e], ob_rsem.at[d % 4 * 2 + e], sib)

    def own_pairs(mt, cnt, a_own, acc, o_pair):
        cnt[:] = jnp.zeros_like(cnt)

        def zero(g):
            acc[g] = jnp.zeros(acc.shape[1:], F32)
        loop(acc.shape[0], zero)

        def chunk(d):
            xcp = pltpu.make_async_copy(xe.at[:, :, lane(d)], xb, lsem.at[1])
            xcp.start()
            load_mask(d)
            m = mask_i[:].astype(F32)
            mt[:] = m.T
            cnt[:] += jnp.dot(mt[rblk(me), :].astype(BF), m.astype(BF), preferred_element_type=F32)

            @pl.when(d >= 4)
            def _():
                for e in range(2):
                    ob_copy(d, e, core).wait_send()
            xcp.wait()

            def half(hh):
                right, left = project(hh, mt[pl.ds(pl.multiple_of(me * rows + hh * GROUP, GROUP), GROUP), :])
                right = right.reshape(16, 2, GROUP, seq)
                for e in range(2):
                    at = pl.ds(pl.multiple_of(e * HALF + core * rows + hh * GROUP, GROUP), GROUP)
                    rt[d % 4, :, at, :] = right[:, e]
                a_own[d % 2, part(hh, GROUP * HID), :] = left
            loop(rows // GROUP, half)

            @pl.when((d // 4) * ((d + 1) % 2) == 1)
            def _():
                pl.semaphore_wait(ob_free, 1)
            for e in range(2):
                ob_copy(d, e, core).start()

            @pl.when(d % 2 == 1)
            def _():
                for e in range(2):
                    ob_copy(d - 1, e, 1 - core).wait_recv()
                    ob_copy(d, e, 1 - core).wait_recv()

                def group(g):
                    at = part(g, 2)
                    acc[g] += (nt_dot(a_own[0], rt[(d - 1) % 4, at].reshape(256, seq))
                               + nt_dot(a_own[1], rt[d % 4, at].reshape(256, seq)))
                loop(acc.shape[0], group)

                @pl.when(d < 4)
                def _():
                    pl.semaphore_signal(ob_free, inc=1, device_id=dev(sib), device_id_type=pl.DeviceIdType.MESH)
        loop(8, chunk)
        cnt_e[:] = cnt[:].reshape(rows, 1, res)

        def pair_rows(n):
            for g in range(8):
                t = acc[g, part(n, HALF), :]
                for b in range(2):
                    u0, u1 = t[:HID, b * LANES:b * LANES + LANES], t[HID:, b * LANES:b * LANES + LANES]
                    q = g * 4 + b * 2
                    lo = lane_lo[:HID]
                    o_pair[q * HID:q * HID + HID, :] = jnp.where(lo, u0, pltpu.roll(u1, HALF, 1)).astype(BF)
                    o_pair[q * HID + HID:q * HID + HALF, :] = jnp.where(lo, pltpu.roll(u0, HALF, 1), u1).astype(BF)
            r_own[n] = jnp.dot(wo_e[:], o_pair[:], preferred_element_type=F32)
        loop(rows // 2, pair_rows)
        for d in range(4, 8):
            for e in range(2):
                ob_copy(d, e, core).wait_send()
        load_mask(me)
        mask_et[:] = mask_i[:].astype(F32).T

    pl.run_scoped(
        own_pairs, pltpu.VMEM((res, seq), F32), pltpu.VMEM((rows, res), F32),
        pltpu.VMEM((2, rows * HID, seq), BF), pltpu.VMEM((8, rows * HID, 256), F32), pltpu.VMEM((1024, LANES), BF))

    side = GROUP * 8
    units = 12

    def transpose(yh, narrow, stored, tin, f_in, f_out):
        def i_copy(u):
            return pltpu.make_async_copy(
                e_out.at[part(yh, side), part(u % 4, GROUP), part(u // 4, side)], tin.at[u % 2], t_isem.at[u % 2])

        i_copy(0).start()

        def unit(u):
            @pl.when(u < units - 1)
            def _():
                i_copy(u + 1).start()
            i_copy(u).wait()

            def widen(i):
                f_in[part(i, side)] = tin[u % 2, part(i, 8)].astype(F32).reshape(side, side)
            loop(GROUP, widen)

            def flip(i):
                for v in range(4):
                    at = pl.ds(i * 4 + v, side, stride=GROUP)
                    f_out[at] = f_in[at].T
            loop(4, flip)
            stored(u)
            loop(GROUP, lambda i: narrow(u, i, f_out[part(i, side)].astype(BF).reshape(8, GROUP, side)))
        loop(units, unit)

    def early_half(tout, tin, f_in, f_out):
        def o_copy(u):
            return pltpu.make_async_copy(
                tout.at[u % 2], e_half.at[part(u // 4, side), part(u % 4, GROUP), :], t_osem.at[u % 2])

        def narrow(u, i, value):
            tout[u % 2, part(i, 8)] = value

            @pl.when(i == GROUP - 1)
            def _():
                o_copy(u).start()

        def stored(u):
            @pl.when(u >= 2)
            def _():
                o_copy(u).wait()

        transpose(me // 4, narrow, stored, tin, f_in, f_out)
        o_copy(units - 2).wait()
        o_copy(units - 1).wait()

    def late_half(tin, f_in, f_out):
        yh = 1 - me // 4

        def narrow(u, i, value):
            e_t[part(u // 4 * GROUP + i, 8), part(u % 4, GROUP), part(yh, side)] = value

        transpose(yh, narrow, lambda u: None, tin, f_in, f_out)

    tile = pltpu.VMEM((2, LANES, GROUP, LANES), BF)
    wide_tile = pltpu.VMEM((LANES * GROUP, LANES), F32)

    def b_rows(kk, c):
        return part(kk * 4 + c, HID)

    def k_lane(kk, h):
        return pl.ds(pl.multiple_of(kk * 256 + h * LANES, LANES), LANES)

    def xb_copy(src, kk, h):
        ref = e_t.at[b_rows(kk, src // 2), part(src % 2, rows), part(h, LANES)]
        return remote(ref, ref, xb_ssem.at[src, kk], xb_rsem.at[src, kk], sib)

    def xa_copy(c, kk, h):
        return remote(a_send.at[rblk(c, rows * HID), pl.ds(kk * LANES, LANES)], a_all.at[rblk(c, rows * HID), k_lane(kk, h)],
                      xa_ssem.at[c, kk], xa_rsem.at[c, kk], sib)

    def block(k):
        src = partner(me, k)
        own_half = (src % 2 + core) % 2

        @pl.when(k == 0)
        def _():
            cp = pltpu.make_async_copy(xe.at[:, :, lane(me)], xb, lsem.at[0])
            cp.start()
            cp.wait()
            cp = pltpu.make_async_copy(xb, e_out.at[rblk(me)], lsem.at[0])
            cp.start()
            cp.wait()

        @pl.when(k > 0)
        def _():
            remote(xe.at[:, :, lane(src)], e_out.at[rblk(src)], e_ssem.at[k], e_rsem.at[k], src).wait_recv()
            cp = pltpu.make_async_copy(e_out.at[rblk(src)], xb, lsem.at[0])
            cp.start()
            cp.wait()

        def half(hh):
            r0 = pl.multiple_of(src * rows + hh * GROUP, GROUP)
            right, left = project(hh, mask_et[pl.ds(r0, GROUP), :])
            for kk in range(3):
                r_at = pl.ds(pl.multiple_of(src % 2 * rows + hh * GROUP, GROUP), GROUP)
                e_t[b_rows(kk, src // 2), r_at, part(core, LANES)] = right[:, :, kk * LANES:kk * LANES + LANES]
            at = pl.ds(pl.multiple_of(((src // 2) * rows + hh * GROUP) * HID, GROUP * HID), GROUP * HID)

            @pl.when(own_half == 0)
            def _():
                for kk in range(3):
                    a_all[at, k_lane(kk, core)] = left[:, kk * LANES:kk * LANES + LANES]

            @pl.when(own_half == 1)
            def _():
                a_send[at, :] = left
        loop(rows // GROUP, half)
        for kk in range(3):
            xb_copy(src, kk, core).start()

        @pl.when(own_half == 1)
        def _():
            for kk in range(3):
                xa_copy(src // 2, kk, core).start()

        @pl.when(k == 3)
        def _():
            pl.run_scoped(early_half, tile, tile, wide_tile, wide_tile)
    loop(8, block)

    for k in range(1, 8):
        e_copy(k).wait_send()


    def xwait(s):
        for kk in range(3):
            xb_copy(s, kk, 1 - core).wait_recv()
    loop(8, xwait)

    def xwait_a(c):
        for kk in range(3):
            xa_copy(c, kk, 1 - core).wait_recv()
    loop(4, xwait_a)

    def rs_copy(n):
        t, first, count, k = ((0, 0, 8, 2), (0, 8, 8, 4), (1, 0, 8, 2), (2, 8, 8, 4),
                              (2, 0, 4, 4), (1, 8, 4, 2), (2, 4, 4, 4), (1, 12, 4, 2))[n]
        at = pl.ds(first, count)
        dst = rs_mid.at[first // 8] if t == 0 else rs_recv.at[t - 1, at]
        return remote(rt.at[t, at], dst, rs_ssem.at[n], rs_rsem.at[n], partner(me, k))

    def contract_extra(o_s):
        pairs = GROUP // 2
        low = lax.broadcasted_iota(jnp.int32, (pairs * HID, LANES), 1) < HALF

        def eblk(n):
            t = ((n // 2 + 1) // 2) % 2 * (1 + (n // 2 + n + 1) % 2) + 3 * (n // 6)
            ib = n % 2
            c = partner(me, 2 * (1 - t // 2) + 4 * (1 - t % 2)) // 2
            at = pl.ds(pl.multiple_of((c * rows + ib * GROUP) * HID, GROUP * HID), GROUP * HID)
            away = (1 - c // 2) * 2
            near = c // 2 * 2 + 1 - c % 2

            def right(blocks):
                return jnp.concatenate([jnp.concatenate(
                    [e_t[(kk * 4 + chip_j) * HID + q] for q, chip_j in blocks], axis=0) for kk in range(3)], axis=1)

            def qstep(qq):
                for h in range(2):
                    q = qq * QSTEP + h * 2
                    o = nt_dot(a_all[at, :], right([(q + x, away + y) for x in range(2) for y in range(2)]))
                    o = o.astype(BF).reshape(pairs, 2, HID, 256)
                    for v in range(2):
                        for x in range(2):
                            o_s[:, part(q + x, HID), pl.ds(v * LANES, LANES)] = o[:, v, :, x * LANES:x * LANES + LANES]
                q = qq * QSTEP
                o = nt_dot(a_all[at, :], right([(q + x, near) for x in range(QSTEP)]))
                o = o.reshape(pairs, 2, HID, 256)
                for x in range(2):
                    u0, u1 = (o[:, v, :, x * LANES:x * LANES + LANES].reshape(pairs * HID, LANES) for v in range(2))
                    for y, both in ((0, jnp.where(low, u0, pltpu.roll(u1, HALF, 1))),
                                    (1, jnp.where(low, pltpu.roll(u0, HALF, 1), u1))):
                        o_s[:, part(q + x * 2 + y, HID), pl.ds(2 * LANES, LANES)] = both.astype(BF).reshape(pairs, HID, LANES)
            loop(HID // QSTEP, qstep)

            def rstep(ii):
                for u in range(RSTEP // 2):
                    i = ii * (RSTEP // 2) + u
                    rt[t, ib * pairs + i] = jnp.dot(wo_e[:], o_s[i], preferred_element_type=F32).astype(BF)
            loop(GROUP // RSTEP, rstep)

            for v in range(6):
                @pl.when(n == v)
                def _():
                    if v >= 4:
                        rs_copy(v - 4).wait_recv()
                        for h in range(2):
                            def add(i):
                                i = h * 4 + i
                                at = (t, ib * pairs + i)
                                rt[at] = (rt[at].astype(F32) + rs_mid[v - 4, i].astype(F32)).astype(BF)
                            loop(4, add)
                            rs_copy(v + h * 2).start()
                    else:
                        rs_copy(v).start()
                    if v == 0:
                        for i in range(2):
                            g_wait(i + 1).wait_recv()
                            d_copy(i).start()
                            f_copy(i).start()
                    if v == 1:
                        for k in (3, 5, 6, 7):
                            m_copy(k).start()
        loop(8, eblk)

        for i in range(2):
            d_wait(i).wait_recv()
        f_copy(2).start()
        g_wait(0).wait_recv()
        for i in range(3):
            f_wait(i).wait_recv()

    def contract_main(o_s):
        def mblk(ib):
            at = part(ib, GROUP * HID)

            def qstep(qq):
                for u in range(QSTEP):
                    q = qq * QSTEP + u
                    o_s[:, part(q, HID), :] = nt_dot(am[at, :], bm[q]).astype(BF).reshape(GROUP, HID, res)
            loop(HID // QSTEP, qstep)

            def rstep(ii):
                for u in range(RSTEP):
                    i = ii * RSTEP + u
                    row = ib * GROUP + i
                    r = jnp.dot(wo_m[:], o_s[i], preferred_element_type=F32)
                    pair_out[row] = ((r + bo_m[:]) / (NORM_EPS + cnt_m[row])).T
            loop(GROUP // RSTEP, rstep)
        loop(rows // GROUP, mblk)

    pl.run_scoped(contract_extra, pltpu.VMEM((GROUP // 2, 1024, 3 * LANES), BF))
    def drain(s):
        for kk in range(3):
            xb_copy(s, kk, core).wait_send()
    loop(8, drain)

    def drain_a(c):
        for kk in range(3):
            xa_copy(c, kk, core).wait_send()
    loop(4, drain_a)
    half_copy = pltpu.make_async_copy(e_half, e_t.at[:, :, part(me // 4, side)], lsem.at[2])
    half_copy.start()
    pl.run_scoped(contract_main, pltpu.VMEM((GROUP, 1024, res), BF))
    pl.run_scoped(late_half, tile, wide_tile, wide_tile)
    half_copy.wait()

    def final(zb):
        def z_copy(j):
            return pltpu.make_async_copy(pair.at[part(j, 8)], zb.at[part(j, 8)], lsem.at[3 + j])

        steps = rows // 8
        for j in range(steps):
            z_copy(j).start()
        hi0 = lax.broadcasted_iota(jnp.int32, (LANES, LANES), 0) * 0 + chip // 2 == 0
        odd = lax.broadcasted_iota(jnp.int32, (LANES, LANES), 0) * 0 + chip % 2 == 1

        def row2(n):
            tot = rt[3, n].astype(F32) + rs_recv[0, n].astype(F32) + rs_recv[1, n].astype(F32)
            kept, own = tot[:, 256:], r_own[n]
            rkept, rown = pltpu.roll(kept, HALF, 1), pltpu.roll(own, HALF, 1)
            near0 = jnp.where(lane_lo, jnp.where(odd, kept, own), jnp.where(odd, rown, rkept))
            near1 = jnp.where(lane_lo, jnp.where(odd, rkept, rown), jnp.where(odd, own, kept))
            for v, near in ((0, near0), (1, near1)):
                away = tot[:, v * LANES:v * LANES + LANES]
                row = n * 2 + v
                r = jnp.concatenate([jnp.where(hi0, near, away), jnp.where(hi0, away, near)], axis=1)
                te = (r + bo_e[:]) / (NORM_EPS + cnt_e[row])
                pair_out[row] = (zb[row] + te.T) + pair_out[row]

        for j in range(steps):
            z_copy(j).wait()
        for first, parts in ((0, (2, 4)), (8, (3, 5)), (4, (6,)), (12, (7,))):
            for n in parts:
                rs_copy(n).wait_recv()
            loop(4, lambda i: row2(first + i))

    pl.run_scoped(final, pltpu.VMEM((rows, res, LANES), F32))

    for k in range(1, 8):
        m_copy(k).wait_send()
        to = partner(me, k)
        remote(xm.at[rblk(me, mseq)], m_out.at[:, rblk(to), :], m_ssem.at[k], m_rsem.at[k], to).wait_recv()

    for i in range(3):
        g_copy(i).wait_send()
    for i in range(2):
        d_copy(i).wait_send()
    for i in range(3):
        f_copy(i).wait_send()
    for n in range(8):
        rs_copy(n).wait_send()


def store_kernel(pair_in, e_in, m_in, pair_out, e_out, m_out, sem):
    copies = []
    for src, dst, pieces in ((e_in, e_out, 6), (pair_in, pair_out, 2), (m_in, m_out, 2)):
        n = src.shape[0] // pieces
        for i in range(pieces):
            at = pl.ds(i * n, n)
            copies.append(pltpu.make_async_copy(src.at[at], dst.at[at], sem.at[len(copies)]))
    for copy in copies:
        copy.start()
    for copy in copies:
        copy.wait()


def solution(mesh):
    msa_spec = P('data', 'dap', None)
    mask_spec = P('data', None)
    row_spec = P(('data', 'dap'), None, None)

    def local_program(extra_block, extra_mask, main_block, main_mask, pair_rows,
                      e_gam, e_bet, e_wl, e_bl, e_wr, e_br, e_wo, e_bo,
                      m_gam, m_bet, m_wl, m_bl, m_wr, m_br, m_wo, m_bo):
        seqs, rows, ce = extra_block.shape
        mseqs, _, cm = main_block.shape
        res = extra_mask.shape[1]
        hid = e_wl.shape[1]
        nk = e_wo.shape[1]
        seq = seqs // 8
        args = (
            jnp.transpose(extra_block, (1, 2, 0)), main_block, extra_mask, pair_rows, main_mask,
            e_gam, e_bet, e_wl.T, e_bl, e_wr.T, e_br, e_wo, e_bo, m_gam, m_bet, m_wl.T, m_bl, m_wr.T, m_br, m_wo, m_bo)
        any_spec = pl.BlockSpec(memory_space=pl.ANY)
        vmem = pl.BlockSpec(memory_space=pltpu.VMEM)
        dma = pltpu.SemaphoreType.DMA
        pair_out, e_seq, m_seq, _, _ = pl.pallas_call(
            opm_kernel,
            out_shape=(
                pltpu.VMEM((rows, res, nk), F32),
                pltpu.VMEM((seq, ce, res), BF),
                pltpu.VMEM((mseqs // 8, res, cm), BF),
                jax.ShapeDtypeStruct((res, ce, seq), BF),
                jax.ShapeDtypeStruct((seq, ce, res // 2), BF)),
            in_specs=[any_spec] * 4 + [pl.BlockSpec(memory_space=pltpu.HBM)] * SMALL,
            out_specs=(vmem, vmem, vmem, any_spec, any_spec),
            scratch_shapes=[pltpu.VMEM(x.shape, x.dtype) for x in args[4:]] + [
                pltpu.VMEM((4 * rows * hid, 2 * seq), BF),
                pltpu.VMEM((4 * rows * hid, seq), BF),
                pltpu.VMEM((rows, ce, seq), BF),
                pltpu.VMEM((GROUP * ce, seq), BF),
                pltpu.VMEM((seq, res), jnp.int32),
                pltpu.VMEM((res, seq), F32),
                pltpu.VMEM((rows, 1, mseqs), F32),
                pltpu.VMEM((rows * hid, mseqs), BF),
                pltpu.VMEM((hid, res, mseqs), BF),
                pltpu.VMEM((4, rows // 2, nk, res // 2 * 3), BF),
                pltpu.VMEM((2, GROUP // 2, nk, res // 2 * 3), BF),
                pltpu.VMEM((2, rows // 2, nk, res // 2 * 3), BF),
                pltpu.VMEM((rows // 2, nk, res // 2), F32),
                pltpu.VMEM((hid * RG, ce * RG), BF),
                pltpu.VMEM((hid * LG, ce * LG), BF),
                pltpu.VMEM((2 * hid, cm), BF),
                pltpu.VMEM((nk, hid * hid), BF),
                pltpu.VMEM((nk, hid * hid), BF),
                pltpu.VMEM((ce, 1), F32),
                pltpu.VMEM((ce, 1), F32),
                pltpu.VMEM((hid * RG, 1), F32),
                pltpu.VMEM((hid, 1), F32),
                pltpu.VMEM((nk, 1), F32),
                pltpu.VMEM((2 * hid, 1), F32),
                pltpu.VMEM((nk, 1), F32),
                pltpu.VMEM((rows, 1, res), F32),
                pltpu.VMEM((rows, 1, res), F32),
                dma((8,)), dma((8,)), dma((8,)), dma((8,)), dma((4, 3)), dma((4, 3)), dma((8, 3)), dma((8, 3)),
                dma((2,)), dma((2,)), dma((2,)), dma((2,)),
                dma((3,)), dma((3,)), dma((3,)), dma((3,)), dma((8,)), dma((8,)),
                dma((8,)), dma((8,)), pltpu.SemaphoreType.REGULAR, dma((8,)), dma((SMALL,))],
            compiler_params=pltpu.CompilerParams(
                collective_id=0, has_side_effects=True, vmem_limit_bytes=VMEM_LIMIT),
            name='opm',
        )(*args)
        pair_out, e_seq, m_seq = pl.pallas_call(
            store_kernel,
            out_shape=tuple(jax.ShapeDtypeStruct(x.shape, x.dtype) for x in (pair_out, e_seq, m_seq)),
            in_specs=[vmem] * 3,
            out_specs=(any_spec,) * 3,
            scratch_shapes=[dma((10,))],
            compiler_params=pltpu.CompilerParams(vmem_limit_bytes=2 ** 20),
            name='store',
        )(pair_out, e_seq, m_seq)
        return pair_out, jnp.transpose(e_seq, (0, 2, 1)), m_seq

    in_specs = (msa_spec, mask_spec, msa_spec, mask_spec, row_spec) + (P(),) * 16
    return jax.shard_map(local_program, mesh=mesh, in_specs=in_specs, out_specs=(row_spec,) * 3, check_vma=False)
```

```python
import functools

import jax
import jax.numpy as jnp
from jax import lax
from jax.experimental import pallas as pl
from jax.experimental.pallas import tpu as pltpu
from jax.sharding import PartitionSpec as P

LN_EPS = 1e-5
NORM_EPS = 1e-3
BF = jnp.bfloat16
F32 = jnp.float32
SMALL = 17
GROUP = 16
VMEM_LIMIT = 43 * 2 ** 20
QSTEP = 4
LSTEP = 4
MSTEP = 8
RG, LG = 8, 4
HID, CE, LANES, HALF = 32, 64, 128, 64
RSTEP = 8


def loop(n, body):
    def step(i, carry):
        body(i)
        return carry
    lax.fori_loop(0, n, step, 0)


def part(i, n):
    return pl.ds(pl.multiple_of(i * n, n), n)


def partner(me, k):
    core, cx, cy = me % 2, (me // 2) % 2, me // 4
    k0, k1, k2 = k % 2, (k // 2) % 2, k // 4
    return (core + k0) % 2 + 2 * ((cx + k1) % 2) + 4 * ((cy + k2) % 2)


def nt_dot(lhs, rhs):
    return lax.dot_general(lhs, rhs, (((1,), (1,)), ((), ())), preferred_element_type=F32)


def column(row, n, repeat):
    m = row.shape[1]
    at = lax.broadcasted_iota(jnp.int32, (n, m), 0) // repeat
    return jnp.sum(jnp.where(at == lax.broadcasted_iota(jnp.int32, (n, m), 1), row, 0.0), axis=1, keepdims=True)


def opm_kernel(xe, xm, mask_e, pair, *refs):
    raw, outs, small, scratch = refs[:SMALL], refs[SMALL:SMALL + 5], refs[SMALL + 5:SMALL * 2 + 5], refs[SMALL * 2 + 5:]
    sems = scratch[-1]
    copies = [pltpu.make_async_copy(src, dst, sems.at[i]) for i, (src, dst) in enumerate(zip(raw, small))]
    opm_body(copies, xe, xm, mask_e, small[0], pair, *small[1:], *outs, *scratch[:-1])


def opm_body(
    copies, xe, xm, mask_e, mask_m, pair,
    e_gam, e_bet, e_wl, e_bl, e_wr, e_br, e_wo, e_bo,
    m_gam, m_bet, m_wl, m_bl, m_wr, m_br, m_wo, m_bo,
    pair_out, e_t, m_out, e_out, e_half,
    a_all, a_send, xb, y_s, mask_i, mask_et, mask_mo, am, bm, rt, rs_mid, rs_recv, r_own,
    w_right, w_left, w_m, wo_e, wo_m, gam_e, bet_e, bias_b, bias_a, bo_e, bias_m, bo_m, cnt_e, cnt_m,
    e_ssem, e_rsem, m_ssem, m_rsem, xa_ssem, xa_rsem, xb_ssem, xb_rsem,
    d_ssem, d_rsem, t_isem, t_osem, g_ssem, g_rsem, f_ssem, f_rsem, rs_ssem, rs_rsem, ob_ssem, ob_rsem, ob_free, lsem,
):
    me = lax.axis_index('dap')
    core = me % 2
    chip = me // 2
    sib = partner(me, 1)
    seq = e_out.shape[2]
    mseq = m_out.shape[0]
    rows = xe.shape[0]
    res = e_out.shape[0]

    def dev(d):
        return {'dap': d}

    def lane(h):
        return pl.ds(pl.multiple_of(h * seq, LANES), seq)

    def rblk(d, n=rows):
        return part(d, n)

    for copy in copies:
        copy.start()
    barrier = pltpu.get_barrier_semaphore()
    for k in range(1, 8):
        pl.semaphore_signal(barrier, inc=1, device_id=dev(partner(me, k)), device_id_type=pl.DeviceIdType.MESH)
    pl.semaphore_wait(barrier, 7)

    def remote(src, dst, ssem, rsem, target):
        return pltpu.make_async_remote_copy(
            src_ref=src, dst_ref=dst, send_sem=ssem, recv_sem=rsem,
            device_id=dev(target), device_id_type=pl.DeviceIdType.MESH)

    def e_copy(k):
        to = partner(me, k)
        return remote(xe.at[:, :, lane(to)], e_out.at[rblk(me)], e_ssem.at[k], e_rsem.at[k], to)

    for k in (1, 2, 4, 3, 5, 6, 7):
        e_copy(k).start()

    def m_copy(k):
        to = partner(me, k)
        return remote(xm.at[rblk(to, mseq)], m_out.at[:, rblk(me), :], m_ssem.at[k], m_rsem.at[k], to)

    def row_of(ref):
        v = ref[:].astype(F32)
        return v.reshape(1, v.shape[0])

    for copy in copies:
        copy.wait()

    def weights(wf, wp):
        gam_e[:] = column(row_of(e_gam), HALF, 1)
        bet_e[:] = column(row_of(e_bet), HALF, 1)
        bias_b[:] = column(row_of(e_br), HID * RG, RG)
        bias_a[:] = column(row_of(e_bl), HID, 1)
        bo_e[:] = column(row_of(e_bo), LANES, 1)
        bo_m[:] = column(row_of(m_bo), LANES, 1)
        bias_m[:HID] = column(row_of(m_bl), HID, 1)
        bias_m[HID:] = column(row_of(m_br), HID, 1)
        w_m[:HID] = m_wl[:]
        w_m[HID:] = m_wr[:]

        def wide(ref, n):
            w = ref[:].astype(F32)
            return jnp.concatenate([w] * n, axis=1)

        def place(dst, rep, residue):
            at = lax.broadcasted_iota(jnp.int32, dst.shape, 0)
            dst[:] = jnp.where(residue(at) == lax.broadcasted_iota(jnp.int32, dst.shape, 1) // CE, rep, 0.0).astype(BF)

        w = wide(e_wr, RG)
        place(w_right, jnp.broadcast_to(w[:, None, :], (HID, RG, RG * CE)).reshape(HID * RG, RG * CE), lambda at: at % RG)
        place(w_left, jnp.concatenate([wide(e_wl, LG)] * LG, axis=0), lambda at: at // HID)
        for src, dst in ((e_wo, wo_e), (m_wo, wo_m)):
            wf[:] = src[:].astype(F32)

            def pick(q):
                wp[part(q, HID), :] = wf[pl.ds(q, HID, stride=HID), :]
            loop(HID, pick)
            dst[:] = wp[:].T.astype(BF)

    pl.run_scoped(weights, pltpu.VMEM((1024, LANES), F32), pltpu.VMEM((1024, LANES), F32))

    def masks(mt):
        mt[:] = mask_m[:].astype(F32).T
        own = mt[rblk(me), :]
        mask_mo[:] = own.reshape(rows, 1, mask_m.shape[0])
        cnt_m[:] = jnp.dot(own.astype(BF), mask_m[:].astype(F32).astype(BF),
                             preferred_element_type=F32).reshape(rows, 1, res)

    pl.run_scoped(masks, pltpu.VMEM((res, mask_m.shape[0]), F32))

    def load_mask(d):
        cp = pltpu.make_async_copy(mask_e.at[rblk(d, seq)], mask_i, lsem.at[0])
        cp.start()
        cp.wait()

    def main_proj(xc, xf, bf):
        cp = pltpu.make_async_copy(xm.at[rblk(me, mseq)], xc.at[pl.ds(0, mseq)], lsem.at[1])
        cp.start()
        cp.wait()
        m_out[:, rblk(me), :] = xc[pl.ds(0, mseq)]
        step = xc.shape[0]
        gam_m, bet_m = row_of(m_gam), row_of(m_bet)
        for piece in range(xm.shape[0] // step):
            cp = pltpu.make_async_copy(xm.at[pl.ds(piece * step, step)], xc, lsem.at[2])
            cp.start()
            cp.wait()

            def widen(i):
                s = part(i, 8)
                xf[s] = xc[s].astype(F32)
            loop(step // 8, widen)

            def one(r):
                x = xf[:, r, :]
                mean = jnp.mean(x, axis=1, keepdims=True)
                cen = x - mean
                var = jnp.mean(cen * cen, axis=1, keepdims=True)
                y = (cen * lax.rsqrt(var + LN_EPS) * gam_m + bet_m).astype(BF)
                proj = nt_dot(w_m[:], y) + bias_m[:]
                proj = proj * mask_mo[r, :, pl.ds(piece * step, step)]
                am[part(r, HID), pl.ds(piece * step, step)] = proj[:HID].astype(BF)
                bf[:, r, :] = proj[HID:]
            def some(i):
                for u in range(MSTEP):
                    one(i * MSTEP + u)

            loop(rows // MSTEP, some)
            bm[:, rblk(me), pl.ds(piece * step, step)] = bf[:].astype(BF)

    pl.run_scoped(
        main_proj, pltpu.VMEM((LANES, rows, xm.shape[2]), BF), pltpu.VMEM((LANES, rows, xm.shape[2]), F32),
        pltpu.VMEM((HID, rows, LANES), F32))

    def g_copy(i):
        ref = bm.at[:, rblk(me), :]
        return remote(ref, ref, g_ssem.at[i], g_rsem.at[i], partner(me, (1, 2, 4)[i]))

    def g_wait(i):
        to = partner(me, (1, 2, 4)[i])
        ref = bm.at[:, rblk(to), :]
        return remote(ref, ref, g_ssem.at[i], g_rsem.at[i], to)

    def d_copy(i):
        ref = bm.at[part(i, HID // 2), rblk(partner(me, (2, 4)[i])), :]
        return remote(ref, ref, d_ssem.at[i], d_rsem.at[i], partner(me, (4, 2)[i]))

    def d_wait(i):
        ref = bm.at[part(i, HID // 2), rblk(partner(me, 6)), :]
        return remote(ref, ref, d_ssem.at[i], d_rsem.at[i], partner(me, (4, 2)[i]))

    def f_copy(i):
        ref = bm.at[:, rblk(partner(me, (2, 4, 6)[i])), :]
        return remote(ref, ref, f_ssem.at[i], f_rsem.at[i], sib)

    def f_wait(i):
        ref = bm.at[:, rblk(partner(me, (3, 5, 7)[i])), :]
        return remote(ref, ref, f_ssem.at[i], f_rsem.at[i], sib)

    for i in range(3):
        g_copy(i).start()
    for k in (1, 2, 4, 3, 5):
        m_copy(k).start()

    def project(hh, m16):
        def norm(i):
            for u in range(LSTEP):
                r = i * LSTEP + u
                x = xb[hh * GROUP + r].astype(F32)
                mean = jnp.mean(x, axis=0, keepdims=True)
                cen = x - mean
                var = jnp.mean(cen * cen, axis=0, keepdims=True)
                y = cen * lax.rsqrt(var + LN_EPS) * gam_e[:] + bet_e[:]
                y_s[part(r, CE), :] = y.astype(BF)
        loop(GROUP // LSTEP, norm)

        def dot(w, g):
            return jnp.dot(w[:], y_s[pl.ds(g * w.shape[1], w.shape[1])], preferred_element_type=F32)

        right = jnp.concatenate(
            [(dot(w_right, g) + bias_b[:]).reshape(HID, RG, seq) for g in range(GROUP // RG)], axis=1)
        right = (right * m16[None]).astype(BF)
        left = []
        for g in range(GROUP // LG):
            d = dot(w_left, g)
            for r in range(LG):
                left.append((d[r * HID:r * HID + HID] + bias_a[:]) * m16[g * LG + r:g * LG + r + 1])
        left = jnp.concatenate(left, axis=0).astype(BF)
        return right, left

    lane_lo = lax.broadcasted_iota(jnp.int32, (LANES, LANES), 1) < HALF

    def ob_copy(d, e, h):
        ref = rt.at[d % 4, :, pl.ds(pl.multiple_of(e * HALF + h * rows, rows), rows), :]
        return remote(ref, ref, ob_ssem.at[d % 4 * 2 + e], ob_rsem.at[d % 4 * 2 + e], sib)

    def own_pairs(mt, cnt, a_own, acc, o_pair):
        cnt[:] = jnp.zeros_like(cnt)

        def zero(g):
            acc[g] = jnp.zeros(acc.shape[1:], F32)
        loop(acc.shape[0], zero)

        def chunk(d):
            xcp = pltpu.make_async_copy(xe.at[:, :, lane(d)], xb, lsem.at[1])
            xcp.start()
            load_mask(d)
            m = mask_i[:].astype(F32)
            mt[:] = m.T
            cnt[:] += jnp.dot(mt[rblk(me), :].astype(BF), m.astype(BF), preferred_element_type=F32)

            @pl.when(d >= 4)
            def _():
                for e in range(2):
                    ob_copy(d, e, core).wait_send()
            xcp.wait()

            def half(hh):
                right, left = project(hh, mt[pl.ds(pl.multiple_of(me * rows + hh * GROUP, GROUP), GROUP), :])
                right = right.reshape(16, 2, GROUP, seq)
                for e in range(2):
                    at = pl.ds(pl.multiple_of(e * HALF + core * rows + hh * GROUP, GROUP), GROUP)
                    rt[d % 4, :, at, :] = right[:, e]
                a_own[d % 2, part(hh, GROUP * HID), :] = left
            loop(rows // GROUP, half)

            @pl.when((d // 4) * ((d + 1) % 2) == 1)
            def _():
                pl.semaphore_wait(ob_free, 1)
            for e in range(2):
                ob_copy(d, e, core).start()

            @pl.when(d % 2 == 1)
            def _():
                for e in range(2):
                    ob_copy(d - 1, e, 1 - core).wait_recv()
                    ob_copy(d, e, 1 - core).wait_recv()

                def group(g):
                    at = part(g, 2)
                    acc[g] += (nt_dot(a_own[0], rt[(d - 1) % 4, at].reshape(256, seq))
                               + nt_dot(a_own[1], rt[d % 4, at].reshape(256, seq)))
                loop(acc.shape[0], group)

                @pl.when(d < 4)
                def _():
                    pl.semaphore_signal(ob_free, inc=1, device_id=dev(sib), device_id_type=pl.DeviceIdType.MESH)
        loop(8, chunk)
        cnt_e[:] = cnt[:].reshape(rows, 1, res)

        def pair_rows(n):
            for g in range(8):
                t = acc[g, part(n, HALF), :]
                for b in range(2):
                    u0, u1 = t[:HID, b * LANES:b * LANES + LANES], t[HID:, b * LANES:b * LANES + LANES]
                    q = g * 4 + b * 2
                    lo = lane_lo[:HID]
                    o_pair[q * HID:q * HID + HID, :] = jnp.where(lo, u0, pltpu.roll(u1, HALF, 1)).astype(BF)
                    o_pair[q * HID + HID:q * HID + HALF, :] = jnp.where(lo, pltpu.roll(u0, HALF, 1), u1).astype(BF)
            r_own[n] = jnp.dot(wo_e[:], o_pair[:], preferred_element_type=F32)
        loop(rows // 2, pair_rows)
        for d in range(4, 8):
            for e in range(2):
                ob_copy(d, e, core).wait_send()
        load_mask(me)
        mask_et[:] = mask_i[:].astype(F32).T

    pl.run_scoped(
        own_pairs, pltpu.VMEM((res, seq), F32), pltpu.VMEM((rows, res), F32),
        pltpu.VMEM((2, rows * HID, seq), BF), pltpu.VMEM((8, rows * HID, 256), F32), pltpu.VMEM((1024, LANES), BF))

    side = GROUP * 8
    units = 12

    def transpose(yh, narrow, stored, tin, f_in, f_out):
        def i_copy(u):
            return pltpu.make_async_copy(
                e_out.at[part(yh, side), part(u % 4, GROUP), part(u // 4, side)], tin.at[u % 2], t_isem.at[u % 2])

        i_copy(0).start()

        def unit(u):
            @pl.when(u < units - 1)
            def _():
                i_copy(u + 1).start()
            i_copy(u).wait()

            def widen(i):
                f_in[part(i, side)] = tin[u % 2, part(i, 8)].astype(F32).reshape(side, side)
            loop(GROUP, widen)

            def flip(i):
                for v in range(4):
                    at = pl.ds(i * 4 + v, side, stride=GROUP)
                    f_out[at] = f_in[at].T
            loop(4, flip)
            stored(u)
            loop(GROUP, lambda i: narrow(u, i, f_out[part(i, side)].astype(BF).reshape(8, GROUP, side)))
        loop(units, unit)

    def early_half(tout, tin, f_in, f_out):
        def o_copy(u):
            return pltpu.make_async_copy(
                tout.at[u % 2], e_half.at[part(u // 4, side), part(u % 4, GROUP), :], t_osem.at[u % 2])

        def narrow(u, i, value):
            tout[u % 2, part(i, 8)] = value

            @pl.when(i == GROUP - 1)
            def _():
                o_copy(u).start()

        def stored(u):
            @pl.when(u >= 2)
            def _():
                o_copy(u).wait()

        transpose(me // 4, narrow, stored, tin, f_in, f_out)
        o_copy(units - 2).wait()
        o_copy(units - 1).wait()

    def late_half(tin, f_in, f_out):
        yh = 1 - me // 4

        def narrow(u, i, value):
            e_t[part(u // 4 * GROUP + i, 8), part(u % 4, GROUP), part(yh, side)] = value

        transpose(yh, narrow, lambda u: None, tin, f_in, f_out)

    tile = pltpu.VMEM((2, LANES, GROUP, LANES), BF)
    wide_tile = pltpu.VMEM((LANES * GROUP, LANES), F32)

    def b_rows(kk, c):
        return part(kk * 4 + c, HID)

    def k_lane(kk, h):
        return pl.ds(pl.multiple_of(kk * 256 + h * LANES, LANES), LANES)

    def xb_copy(src, kk, h):
        ref = e_t.at[b_rows(kk, src // 2), part(src % 2, rows), part(h, LANES)]
        return remote(ref, ref, xb_ssem.at[src, kk], xb_rsem.at[src, kk], sib)

    def xa_copy(c, kk, h):
        return remote(a_send.at[rblk(c, rows * HID), pl.ds(kk * LANES, LANES)], a_all.at[rblk(c, rows * HID), k_lane(kk, h)],
                      xa_ssem.at[c, kk], xa_rsem.at[c, kk], sib)

    def block(k):
        src = partner(me, k)
        own_half = (src % 2 + core) % 2

        @pl.when(k == 0)
        def _():
            cp = pltpu.make_async_copy(xe.at[:, :, lane(me)], xb, lsem.at[0])
            cp.start()
            cp.wait()
            cp = pltpu.make_async_copy(xb, e_out.at[rblk(me)], lsem.at[0])
            cp.start()
            cp.wait()

        @pl.when(k > 0)
        def _():
            remote(xe.at[:, :, lane(src)], e_out.at[rblk(src)], e_ssem.at[k], e_rsem.at[k], src).wait_recv()
            cp = pltpu.make_async_copy(e_out.at[rblk(src)], xb, lsem.at[0])
            cp.start()
            cp.wait()

        def half(hh):
            r0 = pl.multiple_of(src * rows + hh * GROUP, GROUP)
            right, left = project(hh, mask_et[pl.ds(r0, GROUP), :])
            for kk in range(3):
                r_at = pl.ds(pl.multiple_of(src % 2 * rows + hh * GROUP, GROUP), GROUP)
                e_t[b_rows(kk, src // 2), r_at, part(core, LANES)] = right[:, :, kk * LANES:kk * LANES + LANES]
            at = pl.ds(pl.multiple_of(((src // 2) * rows + hh * GROUP) * HID, GROUP * HID), GROUP * HID)

            @pl.when(own_half == 0)
            def _():
                for kk in range(3):
                    a_all[at, k_lane(kk, core)] = left[:, kk * LANES:kk * LANES + LANES]

            @pl.when(own_half == 1)
            def _():
                a_send[at, :] = left
        loop(rows // GROUP, half)
        for kk in range(3):
            xb_copy(src, kk, core).start()

        @pl.when(own_half == 1)
        def _():
            for kk in range(3):
                xa_copy(src // 2, kk, core).start()

        @pl.when(k == 3)
        def _():
            pl.run_scoped(early_half, tile, tile, wide_tile, wide_tile)
    loop(8, block)

    for k in range(1, 8):
        e_copy(k).wait_send()


    def xwait(s):
        for kk in range(3):
            xb_copy(s, kk, 1 - core).wait_recv()
    loop(8, xwait)

    def xwait_a(c):
        for kk in range(3):
            xa_copy(c, kk, 1 - core).wait_recv()
    loop(4, xwait_a)

    def rs_copy(n):
        t, first, count, k = ((0, 0, 8, 2), (0, 8, 8, 4), (1, 0, 8, 2), (2, 8, 8, 4),
                              (2, 0, 4, 4), (1, 8, 4, 2), (2, 4, 4, 4), (1, 12, 4, 2))[n]
        at = pl.ds(first, count)
        dst = rs_mid.at[first // 8] if t == 0 else rs_recv.at[t - 1, at]
        return remote(rt.at[t, at], dst, rs_ssem.at[n], rs_rsem.at[n], partner(me, k))

    def contract_extra(o_s):
        pairs = GROUP // 2
        low = lax.broadcasted_iota(jnp.int32, (pairs * HID, LANES), 1) < HALF

        def eblk(n):
            t = ((n // 2 + 1) // 2) % 2 * (1 + (n // 2 + n + 1) % 2) + 3 * (n // 6)
            ib = n % 2
            c = partner(me, 2 * (1 - t // 2) + 4 * (1 - t % 2)) // 2
            at = pl.ds(pl.multiple_of((c * rows + ib * GROUP) * HID, GROUP * HID), GROUP * HID)
            away = (1 - c // 2) * 2
            near = c // 2 * 2 + 1 - c % 2

            def right(blocks):
                return jnp.concatenate([jnp.concatenate(
                    [e_t[(kk * 4 + chip_j) * HID + q] for q, chip_j in blocks], axis=0) for kk in range(3)], axis=1)

            def qstep(qq):
                for h in range(2):
                    q = qq * QSTEP + h * 2
                    o = nt_dot(a_all[at, :], right([(q + x, away + y) for x in range(2) for y in range(2)]))
                    o = o.astype(BF).reshape(pairs, 2, HID, 256)
                    for v in range(2):
                        for x in range(2):
                            o_s[:, part(q + x, HID), pl.ds(v * LANES, LANES)] = o[:, v, :, x * LANES:x * LANES + LANES]
                q = qq * QSTEP
                o = nt_dot(a_all[at, :], right([(q + x, near) for x in range(QSTEP)]))
                o = o.reshape(pairs, 2, HID, 256)
                for x in range(2):
                    u0, u1 = (o[:, v, :, x * LANES:x * LANES + LANES].reshape(pairs * HID, LANES) for v in range(2))
                    for y, both in ((0, jnp.where(low, u0, pltpu.roll(u1, HALF, 1))),
                                    (1, jnp.where(low, pltpu.roll(u0, HALF, 1), u1))):
                        o_s[:, part(q + x * 2 + y, HID), pl.ds(2 * LANES, LANES)] = both.astype(BF).reshape(pairs, HID, LANES)
            loop(HID // QSTEP, qstep)

            def rstep(ii):
                for u in range(RSTEP // 2):
                    i = ii * (RSTEP // 2) + u
                    rt[t, ib * pairs + i] = jnp.dot(wo_e[:], o_s[i], preferred_element_type=F32).astype(BF)
            loop(GROUP // RSTEP, rstep)

            for v in range(6):
                @pl.when(n == v)
                def _():
                    if v >= 4:
                        rs_copy(v - 4).wait_recv()
                        for h in range(2):
                            def add(i):
                                i = h * 4 + i
                                at = (t, ib * pairs + i)
                                rt[at] = (rt[at].astype(F32) + rs_mid[v - 4, i].astype(F32)).astype(BF)
                            loop(4, add)
                            rs_copy(v + h * 2).start()
                    else:
                        rs_copy(v).start()
                    if v == 0:
                        for i in range(2):
                            g_wait(i + 1).wait_recv()
                            d_copy(i).start()
                            f_copy(i).start()
                    if v == 1:
                        for k in (6, 7):
                            m_copy(k).start()
        loop(8, eblk)

        for i in range(2):
            d_wait(i).wait_recv()
        f_copy(2).start()
        g_wait(0).wait_recv()
        for i in range(3):
            f_wait(i).wait_recv()

    def contract_main(o_s):
        def mblk(ib):
            at = part(ib, GROUP * HID)

            def qstep(qq):
                for u in range(QSTEP):
                    q = qq * QSTEP + u
                    o_s[:, part(q, HID), :] = nt_dot(am[at, :], bm[q]).astype(BF).reshape(GROUP, HID, res)
            loop(HID // QSTEP, qstep)

            def rstep(ii):
                for u in range(RSTEP):
                    i = ii * RSTEP + u
                    row = ib * GROUP + i
                    r = jnp.dot(wo_m[:], o_s[i], preferred_element_type=F32)
                    pair_out[row] = ((r + bo_m[:]) / (NORM_EPS + cnt_m[row])).T
            loop(GROUP // RSTEP, rstep)
        loop(rows // GROUP, mblk)

    pl.run_scoped(contract_extra, pltpu.VMEM((GROUP // 2, 1024, 3 * LANES), BF))
    def drain(s):
        for kk in range(3):
            xb_copy(s, kk, core).wait_send()
    loop(8, drain)

    def drain_a(c):
        for kk in range(3):
            xa_copy(c, kk, core).wait_send()
    loop(4, drain_a)
    half_copy = pltpu.make_async_copy(e_half, e_t.at[:, :, part(me // 4, side)], lsem.at[2])
    half_copy.start()
    pl.run_scoped(contract_main, pltpu.VMEM((GROUP, 1024, res), BF))
    pl.run_scoped(late_half, tile, wide_tile, wide_tile)
    half_copy.wait()

    def final(zb):
        def z_copy(j):
            return pltpu.make_async_copy(pair.at[part(j, 8)], zb.at[part(j, 8)], lsem.at[3 + j])

        steps = rows // 8
        for j in range(steps):
            z_copy(j).start()
        hi0 = lax.broadcasted_iota(jnp.int32, (LANES, LANES), 0) * 0 + chip // 2 == 0
        odd = lax.broadcasted_iota(jnp.int32, (LANES, LANES), 0) * 0 + chip % 2 == 1

        def row2(n):
            tot = rt[3, n].astype(F32) + rs_recv[0, n].astype(F32) + rs_recv[1, n].astype(F32)
            kept, own = tot[:, 256:], r_own[n]
            rkept, rown = pltpu.roll(kept, HALF, 1), pltpu.roll(own, HALF, 1)
            near0 = jnp.where(lane_lo, jnp.where(odd, kept, own), jnp.where(odd, rown, rkept))
            near1 = jnp.where(lane_lo, jnp.where(odd, rkept, rown), jnp.where(odd, own, kept))
            for v, near in ((0, near0), (1, near1)):
                away = tot[:, v * LANES:v * LANES + LANES]
                row = n * 2 + v
                r = jnp.concatenate([jnp.where(hi0, near, away), jnp.where(hi0, away, near)], axis=1)
                te = (r + bo_e[:]) / (NORM_EPS + cnt_e[row])
                pair_out[row] = (zb[row] + te.T) + pair_out[row]

        for j in range(steps):
            z_copy(j).wait()
        for first, parts in ((0, (2, 4)), (8, (3, 5)), (4, (6,)), (12, (7,))):
            for n in parts:
                rs_copy(n).wait_recv()
            loop(4, lambda i: row2(first + i))

    pl.run_scoped(final, pltpu.VMEM((rows, res, LANES), F32))

    for k in range(1, 8):
        m_copy(k).wait_send()
        to = partner(me, k)
        remote(xm.at[rblk(me, mseq)], m_out.at[:, rblk(to), :], m_ssem.at[k], m_rsem.at[k], to).wait_recv()

    for i in range(3):
        g_copy(i).wait_send()
    for i in range(2):
        d_copy(i).wait_send()
    for i in range(3):
        f_copy(i).wait_send()
    for n in range(8):
        rs_copy(n).wait_send()


def store_kernel(pair_in, e_in, m_in, pair_out, e_out, m_out, sem):
    copies = []
    for src, dst, pieces in ((e_in, e_out, 6), (pair_in, pair_out, 2), (m_in, m_out, 2)):
        n = src.shape[0] // pieces
        for i in range(pieces):
            at = pl.ds(i * n, n)
            copies.append(pltpu.make_async_copy(src.at[at], dst.at[at], sem.at[len(copies)]))
    for copy in copies:
        copy.start()
    for copy in copies:
        copy.wait()


def solution(mesh):
    msa_spec = P('data', 'dap', None)
    mask_spec = P('data', None)
    row_spec = P(('data', 'dap'), None, None)

    def local_program(extra_block, extra_mask, main_block, main_mask, pair_rows,
                      e_gam, e_bet, e_wl, e_bl, e_wr, e_br, e_wo, e_bo,
                      m_gam, m_bet, m_wl, m_bl, m_wr, m_br, m_wo, m_bo):
        seqs, rows, ce = extra_block.shape
        mseqs, _, cm = main_block.shape
        res = extra_mask.shape[1]
        hid = e_wl.shape[1]
        nk = e_wo.shape[1]
        seq = seqs // 8
        args = (
            jnp.transpose(extra_block, (1, 2, 0)), main_block, extra_mask, pair_rows, main_mask,
            e_gam, e_bet, e_wl.T, e_bl, e_wr.T, e_br, e_wo, e_bo, m_gam, m_bet, m_wl.T, m_bl, m_wr.T, m_br, m_wo, m_bo)
        any_spec = pl.BlockSpec(memory_space=pl.ANY)
        vmem = pl.BlockSpec(memory_space=pltpu.VMEM)
        dma = pltpu.SemaphoreType.DMA
        pair_out, e_seq, m_seq, _, _ = pl.pallas_call(
            opm_kernel,
            out_shape=(
                pltpu.VMEM((rows, res, nk), F32),
                pltpu.VMEM((seq, ce, res), BF),
                pltpu.VMEM((mseqs // 8, res, cm), BF),
                jax.ShapeDtypeStruct((res, ce, seq), BF),
                jax.ShapeDtypeStruct((seq, ce, res // 2), BF)),
            in_specs=[any_spec] * 4 + [pl.BlockSpec(memory_space=pltpu.HBM)] * SMALL,
            out_specs=(vmem, vmem, vmem, any_spec, any_spec),
            scratch_shapes=[pltpu.VMEM(x.shape, x.dtype) for x in args[4:]] + [
                pltpu.VMEM((4 * rows * hid, 2 * seq), BF),
                pltpu.VMEM((4 * rows * hid, seq), BF),
                pltpu.VMEM((rows, ce, seq), BF),
                pltpu.VMEM((GROUP * ce, seq), BF),
                pltpu.VMEM((seq, res), jnp.int32),
                pltpu.VMEM((res, seq), F32),
                pltpu.VMEM((rows, 1, mseqs), F32),
                pltpu.VMEM((rows * hid, mseqs), BF),
                pltpu.VMEM((hid, res, mseqs), BF),
                pltpu.VMEM((4, rows // 2, nk, res // 2 * 3), BF),
                pltpu.VMEM((2, GROUP // 2, nk, res // 2 * 3), BF),
                pltpu.VMEM((2, rows // 2, nk, res // 2 * 3), BF),
                pltpu.VMEM((rows // 2, nk, res // 2), F32),
                pltpu.VMEM((hid * RG, ce * RG), BF),
                pltpu.VMEM((hid * LG, ce * LG), BF),
                pltpu.VMEM((2 * hid, cm), BF),
                pltpu.VMEM((nk, hid * hid), BF),
                pltpu.VMEM((nk, hid * hid), BF),
                pltpu.VMEM((ce, 1), F32),
                pltpu.VMEM((ce, 1), F32),
                pltpu.VMEM((hid * RG, 1), F32),
                pltpu.VMEM((hid, 1), F32),
                pltpu.VMEM((nk, 1), F32),
                pltpu.VMEM((2 * hid, 1), F32),
                pltpu.VMEM((nk, 1), F32),
                pltpu.VMEM((rows, 1, res), F32),
                pltpu.VMEM((rows, 1, res), F32),
                dma((8,)), dma((8,)), dma((8,)), dma((8,)), dma((4, 3)), dma((4, 3)), dma((8, 3)), dma((8, 3)),
                dma((2,)), dma((2,)), dma((2,)), dma((2,)),
                dma((3,)), dma((3,)), dma((3,)), dma((3,)), dma((8,)), dma((8,)),
                dma((8,)), dma((8,)), pltpu.SemaphoreType.REGULAR, dma((8,)), dma((SMALL,))],
            compiler_params=pltpu.CompilerParams(
                collective_id=0, has_side_effects=True, vmem_limit_bytes=VMEM_LIMIT),
            name='opm',
        )(*args)
        pair_out, e_seq, m_seq = pl.pallas_call(
            store_kernel,
            out_shape=tuple(jax.ShapeDtypeStruct(x.shape, x.dtype) for x in (pair_out, e_seq, m_seq)),
            in_specs=[vmem] * 3,
            out_specs=(any_spec,) * 3,
            scratch_shapes=[dma((10,))],
            compiler_params=pltpu.CompilerParams(vmem_limit_bytes=2 ** 20),
            name='store',
        )(pair_out, e_seq, m_seq)
        return pair_out, jnp.transpose(e_seq, (0, 2, 1)), m_seq

    in_specs = (msa_spec, mask_spec, msa_spec, mask_spec, row_spec) + (P(),) * 16
    return jax.shard_map(local_program, mesh=mesh, in_specs=in_specs, out_specs=(row_spec,) * 3, check_vma=False)
```
